32 devices in a mesh: seq: 8 (over z, y), rep: 4 (over x, core).
Axes of the slice: x: 2, y: 2, z: 4, core: 2. Of those that a mesh axis runs over, the one named last changes fastest.
Arguments:
- inputs: bfloat16 [4, 1024, 1024], P('rep', 'seq'), may hold values from -6 to 6
- weight_t: bfloat16 [3072, 1024], P('seq', 'rep'), may hold values from -0.1875 to 0.1875
- states: float32 [4, 1024, 1024], P('rep', 'seq'), may hold values from -0.9 to 0.9
- doc_ids: int32 [4, 1024], P('rep', 'seq'), may hold values from 0 to 3, never falling along the last dimension, each value on 1 to 512 neighbouring positions
- recur: float32 [3, 1024], replicated, may hold values from -1 to 1
- bias: float32 [3, 1024], replicated, may hold values from -8 to 3, as said below
- out_grad: bfloat16 [4, 1024, 1024], P('rep', 'seq'), may hold values from -6 to 6
Outputs:
- input_grad: bfloat16 [4, 1024, 1024], P('rep', 'seq')
- weight_grad: float32 [3072, 1024], P('seq', 'rep')
- param_grad: float32 [6, 1024], replicated
The draws below stay inside these ranges and needn't reach their ends.
Inputs may be any that keep to these rules, and one draw needn't show every extreme that they name: `doc_ids`: within each sequence the numbers never fall; every document has 1 to 512 tokens, and some document has exactly 512. `bias`: row 0 lies between -8 and -1, rows 1 and 2 between -3 and 3.
All inputs are finite; a program needn't handle non-finite values.
Results may differ from the reference program's by a relative error of at most 0.0095.
Values may be sent and summed in bfloat16 or wider, within the bound.
A program may use at most 128 MiB of HBM per device.

```python
import math
import jax
import jax.numpy as jnp
import numpy as np
from jax import lax

DI = 1024
H = 1024
L = 1024
SEQS = 4
SEGS = 4
MOST = 512


def draw_bias(key, part):
    keys = jax.random.split(jax.random.fold_in(key, 17), 4)
    share = 0.5
    others = jnp.clip(jax.random.normal(keys[3], (2, H), jnp.float32), -3.0, 3.0)
    slower = jax.random.uniform(keys[0], (H,), jnp.float32) < share
    slow_value = jax.random.uniform(keys[1], (H,), jnp.float32, -8.0, -6.0)
    fast_value = jax.random.uniform(keys[2], (H,), jnp.float32, -3.0, -1.0)
    first = jnp.where(slower, slow_value, fast_value)
    return jnp.concatenate([first[None, :], others], 0).astype(jnp.float32)


def block_levels(rng, extent, cuts, least, high):
    level = 1.0
    for position, blocks in cuts:
        draws = jax.random.uniform(jax.random.fold_in(jax.random.fold_in(rng, 6), position), (blocks,), jnp.float32, least / len(cuts), high / len(cuts))
        level = level * jnp.repeat(jnp.exp(draws), extent[position] // blocks).reshape((-1,) + (1,) * (len(extent) - 1 - position))
    return level


def profile(amount, total, reach, slope):
    loads = [(1 << 20) // math.isqrt(standing ** slope) + 1 for standing in range(2, amount + 1)]
    spare, counts = total - reach - (amount - 1), [1] * (amount - 1)
    while spare > 0:
        candidates = [i for i in range(amount - 1) if counts[i] < reach]
        pool, budget = sum([loads[i] for i in candidates]), spare
        for i in candidates:
            addition = min(reach - counts[i], max(1, budget * loads[i] // pool), spare)
            counts[i] = counts[i] + addition
            spare = spare - addition
    return np.array([reach] + counts)


def uneven(stream_key, count, total, most, lean):
    if count == 2:
        one = jax.random.randint(stream_key, (), max(1, total - most), min(most, total - 1) + 1)
        return jnp.stack([one, total - one])
    sizes = jnp.asarray(profile(count, total, most, lean), jnp.int32)
    couples = (count - 1) // 2
    giver, receiver = sizes[1:1 + 2 * couples:2], sizes[2:2 + 2 * couples:2]
    room = jnp.minimum(giver - 1, most - receiver)
    moved = jax.random.randint(jax.random.fold_in(stream_key, 1), (couples,), 0, 1 << 20) % (room + 1)
    sizes = sizes.at[1:1 + 2 * couples:2].set(giver - moved).at[2:2 + 2 * couples:2].set(receiver + moved)
    return sizes[jax.random.permutation(jax.random.fold_in(stream_key, 2), count)]


def bell_draw(rng, extent, scale, limit, shards=(), kind=jnp.bfloat16):
    array = scale * jax.random.normal(rng, extent, jnp.float32)
    if shards:
        array = array * block_levels(rng, extent, shards, -0.22, 0.18)
    return jnp.clip(array, -limit, limit).astype(kind)


def setup_inputs(seed: int = 0) -> dict:
    key_of = jax.random.split(jax.random.key(seed), 8)
    return {
        "inputs": bell_draw(key_of[0], (SEQS, L, DI), 1.0, 6.0, ((0, 4), (1, 8))),
        "weight_t": bell_draw(key_of[1], (3 * H, DI), DI ** -0.5, 0.1875, ((0, 8), (1, 4))),
        "states": jnp.clip(jax.random.uniform(key_of[2], (SEQS, L, H), jnp.float32, -0.9, 0.9) * block_levels(key_of[2], (SEQS, L, H), ((0, 4), (1, 8)), -0.4, 0.0), -0.9, 0.9),
        "doc_ids": jax.vmap(lambda own: jnp.searchsorted(jnp.cumsum(uneven(own, SEGS, L, MOST, 1)), jnp.arange(L), side="right"))(jax.random.split(key_of[3], SEQS)).reshape((SEQS, L)).astype(jnp.int32),
        "recur": jnp.clip(jax.random.uniform(key_of[4], (3, H), jnp.float32, -1.0, 1.0), -1.0, 1.0),
        "bias": draw_bias(jax.random.fold_in(key_of[7], 71), 0),
        "out_grad": bell_draw(key_of[6], (SEQS, L, H), 1.0, 6.0, ((0, 4), (1, 8))),
    }


def one_sequence(feats, states, doc_ids, out_grad, weight_t, recur, bias):
    preact = jnp.dot(feats, weight_t.T, preferred_element_type=jnp.float32)
    pz = preact[:, :H]
    pr = preact[:, H:2 * H]
    pc = preact[:, 2 * H:]
    same = jnp.concatenate([jnp.zeros((1,), jnp.float32), (doc_ids[1:] == doc_ids[:-1]).astype(jnp.float32)])
    prior = jnp.concatenate([jnp.zeros((1, H), jnp.float32), states[:-1]], 0) * same[:, None]
    gate_z = jax.nn.sigmoid(pz + recur[0] * prior + bias[0])
    gate_r = jax.nn.sigmoid(pr + recur[1] * prior + bias[1])
    gate_c = jnp.tanh(pc + recur[2] * gate_r * prior + bias[2])
    jacobian = same[:, None] * (1.0 - gate_z + (gate_c - prior) * gate_z * (1.0 - gate_z) * recur[0] + gate_z * (1.0 - gate_c * gate_c) * recur[2] * (gate_r + prior * gate_r * (1.0 - gate_r) * recur[1]))
    factor = jnp.concatenate([jacobian[1:], jnp.zeros((1, H), jnp.float32)], 0)

    def backstep(carry, item):
        upstream, coef = item
        adjoint = upstream + coef * carry
        return (adjoint, adjoint)
    _, adjoint = lax.scan(backstep, jnp.zeros((H,), jnp.float32), (out_grad.astype(jnp.float32), factor), reverse=True)
    grad_z = adjoint * (gate_c - prior) * gate_z * (1.0 - gate_z)
    grad_c = adjoint * gate_z * (1.0 - gate_c * gate_c)
    grad_r = grad_c * recur[2] * prior * gate_r * (1.0 - gate_r)
    grad_pre = jnp.concatenate([grad_z, grad_r, grad_c], 1).astype(jnp.bfloat16)
    input_grad = jnp.dot(grad_pre, weight_t, preferred_element_type=jnp.float32).astype(jnp.bfloat16)
    weight_part = jnp.dot(grad_pre.T, feats, preferred_element_type=jnp.float32)
    stats = jnp.stack([grad_z.sum(0), grad_r.sum(0), grad_c.sum(0), (grad_z * prior).sum(0), (grad_r * prior).sum(0), (grad_c * gate_r * prior).sum(0)])
    return (input_grad, weight_part, stats)

def reference(inputs, weight_t, states, doc_ids, recur, bias, out_grad):

    def single(items):
        return one_sequence(items[0], items[1], items[2], items[3], weight_t, recur, bias)
    input_grad, weight_parts, stats = lax.map(single, (inputs, states, doc_ids, out_grad))
    factor = 1.0 / math.sqrt(SEQS * L)
    return (input_grad, weight_parts.sum(0) * factor, stats.sum(0) * factor)
```

```python
import functools
import math

import jax
import jax.numpy as jnp
from jax import lax
from jax.experimental import pallas as pl
from jax.experimental.pallas import tpu as pltpu
from jax.sharding import PartitionSpec as P

F32 = jnp.float32
BF16 = jnp.bfloat16
GATES = 3


def shifted(block, axis, distance):
    devices = range(lax.axis_size(axis))
    route = [(i - distance, i) for i in devices if i - distance in devices]
    return lax.ppermute(block, axis, route)


def compose(earlier, later):
    return (later[0] * earlier[0], later[1] + later[0] * earlier[1])


def by_tokens(inputs, weight_t, states, doc_ids, recur, bias, out_grad):
    feats = inputs[0]
    hidden_now = states[0]
    ids_float = doc_ids[0].astype(F32)
    count = feats.shape[0]
    width = hidden_now.shape[1]
    columns = lax.all_gather(weight_t, "rep", axis=1, tiled=True)
    contract_last = (((1,), (1,)), ((), ()))
    full_weight = lax.all_gather(columns, "seq", axis=0, tiled=True)
    preact = lax.dot_general(feats, full_weight, contract_last, preferred_element_type=F32)
    tail_state, tail_id = shifted((hidden_now[-1:], ids_float[-1:]), "seq", 1)
    first_same = jnp.where(
        (ids_float[0] == tail_id[0]) & (lax.axis_index("seq") > 0), 1.0, 0.0
    ).astype(F32)
    same = jnp.concatenate([first_same[None], (ids_float[1:] == ids_float[:-1]).astype(F32)])
    prior = jnp.concatenate([tail_state, hidden_now[:-1]], 0) * same[:, None]
    gate_z = jax.nn.sigmoid(preact[:, :width] + recur[0] * prior + bias[0])
    gate_r = jax.nn.sigmoid(preact[:, width : 2 * width] + recur[1] * prior + bias[1])
    gate_c = jnp.tanh(preact[:, 2 * width :] + recur[2] * gate_r * prior + bias[2])
    jacobian = same[:, None] * (
        1.0
        - gate_z
        + (gate_c - prior) * gate_z * (1.0 - gate_z) * recur[0]
        + gate_z
        * (1.0 - gate_c * gate_c)
        * recur[2]
        * (gate_r + prior * gate_r * (1.0 - gate_r) * recur[1])
    )
    upstream = out_grad[0].astype(F32)
    jac_rows, up_rows = (
        lax.all_to_all(jacobian.T, "seq", split_axis=0, concat_axis=1, tiled=True),
        lax.all_to_all(upstream.T, "seq", split_axis=0, concat_axis=1, tiled=True),
    )
    factor = jnp.concatenate([jac_rows[:, 1:], jnp.zeros((jac_rows.shape[0], 1), F32)], 1)
    _, adjoint_rows = lax.associative_scan(compose, (factor, up_rows), reverse=True, axis=1)
    adjoint = lax.all_to_all(adjoint_rows, "seq", split_axis=1, concat_axis=0, tiled=True).T
    grad_z = adjoint * (gate_c - prior) * gate_z * (1.0 - gate_z)
    grad_c = adjoint * gate_z * (1.0 - gate_c * gate_c)
    grad_r = grad_c * recur[2] * prior * gate_r * (1.0 - gate_r)
    grad_pre = jnp.concatenate([grad_z, grad_r, grad_c], 1).astype(BF16)
    input_grad = jnp.dot(grad_pre, full_weight, preferred_element_type=F32)
    tokens_all = count * inputs.shape[0] * lax.axis_size("seq") * lax.axis_size("rep")
    normal_factor = 1.0 / math.sqrt(tokens_all)
    row_share = lax.psum_scatter(
        lax.dot_general(grad_pre, feats, (((0,), (0,)), ((), ())), preferred_element_type=F32),
        "seq",
        scatter_dimension=0,
        tiled=True,
    )
    weight_grad = (
        lax.psum_scatter(row_share.astype(BF16), "rep", scatter_dimension=1, tiled=True).astype(F32)
        * normal_factor
    )
    stats = jnp.stack(
        [
            grad_z.sum(0),
            grad_r.sum(0),
            grad_c.sum(0),
            (grad_z * prior).sum(0),
            (grad_r * prior).sum(0),
            (grad_c * gate_r * prior).sum(0),
        ]
    )
    param_grad = lax.psum(stats, ("seq", "rep")) * normal_factor
    return (input_grad.astype(BF16)[None], weight_grad, param_grad)


def kernel(
    ns, nr, feats, weight, states, ids, recur, bias, upstream,
    out_in, out_w, out_p,
    pay_src, pay, ids_src, ids_all, tail_src, tail_in, x_all, w_all, prev, ids_col, up, jac,
    co_z, co_r, co_c, rprior, prior_all,
    scan_a, scan_b, carry, seg_out, seg_in, lam, grads, part_out, part_in, part_keep, fin_out, fin_in,
    wg_out, wg_in, st_out, st_in,
    x_s0, x_sx, x_sy, x_sd, x_r, w_s, w_r, p_s, p_r, i_s, i_r, e_s, e_r, c_s, c_r, d_s, d_r, f_s, f_r,
    g_s, g_r, t_s, t_r,
):
    T, DI = feats.shape
    H = states.shape[1]
    nh, nz, nx = 2 * nr, ns // 2, nr // 2
    hb, cw = H // nh, DI // nr
    s, r = lax.axis_index("seq"), lax.axis_index("rep")
    z, y, x, c = s // 2, s % 2, r // 2, r % 2
    k = 2 * r + y
    me = s * nr + r
    unsent = []

    def place(a, b):
        return {"seq": a, "rep": b}

    def at(plane, j):
        return place(2 * plane + j % 2, j // 2)

    def send(src, dst, ssem, rsem, where):
        pltpu.make_async_remote_copy(
            src_ref=src, dst_ref=dst, send_sem=ssem, recv_sem=rsem,
            device_id=where, device_id_type=pl.DeviceIdType.MESH,
        ).start()

    def local(src, dst, rsem):
        pltpu.make_async_copy(src, dst, rsem).start()

    def landed(dst, sem):
        pltpu.make_async_copy(dst, dst, sem).wait()

    def send_if(allowed, src, dst, ssem, rsem, where):
        @pl.when(allowed)
        def _():
            send(src, dst, ssem, rsem, where)

        unsent.append((allowed, src, ssem))

    def send_or_local(src, dst, ssem, rsem, where, here):
        send_if(jnp.logical_not(here), src, dst, ssem, rsem, where)

        @pl.when(here)
        def _():
            local(src, dst, rsem)

    def rows(ref, block, count):
        return ref.at[pl.ds(pl.multiple_of(block * count, count), count), :]

    barrier = pltpu.get_barrier_semaphore()

    def greet(d, _):
        @pl.when(d != me)
        def _():
            pl.semaphore_signal(
                barrier, inc=1, device_id=place(d // nr, d % nr), device_id_type=pl.DeviceIdType.MESH
            )

        return 0

    lax.fori_loop(0, ns * nr, greet, 0)
    for j in range(nh):
        pay_src[j, :, :hb] = states[:, j * hb : (j + 1) * hb].astype(BF16)
        pay_src[j, :, hb:] = upstream[:, j * hb : (j + 1) * hb]
        tail_src[j, 0:8, :] = states[T - 8 : T, j * hb : (j + 1) * hb]
        tail_src[j, 8:16, :] = jnp.broadcast_to(ids[0:1, T - 1 : T].astype(F32), (8, hb))
    ids_src[...] = jnp.broadcast_to(ids[...].astype(F32), ids_src.shape)

    pl.semaphore_wait(barrier, ns * nr - 1)

    steps = sorted(range(nz), key=lambda step: -min(step, nz - step))
    for step in steps:
        plane = (z + step) % nz
        for i in range(GATES):
            b = GATES * s + i
            g, j = b // nh, b % nh
            dst = w_all.at[
                pl.ds(pl.multiple_of(g * hb, hb), hb), pl.ds(pl.multiple_of(r * cw, cw), cw)
            ]
            here = jnp.logical_and(step == 0, j == k)
            send_or_local(
                weight.at[i * hb : (i + 1) * hb, :], dst, w_s.at[i * nz + step],
                w_r.at[g * nr + r], at(plane, j), here,
            )
    partner = place(s, r + 1 - 2 * c)
    local(feats, rows(x_all, k, T), x_s0)

    def share(step, src, dx, dy):
        x0, y0 = (x + dx) % nx, (y + dy) % 2
        slot = 2 * (2 * x0 + c) + y0
        dst = rows(x_all, slot, T)
        src = dst if src is None else src
        if dy == 0 or dx == 0:
            for other in range(1, nx):
                if dx == 0:
                    allowed = True if dy == 0 else c == 0
                    send_if(
                        allowed, src, dst, x_sx.at[step * nx + other], x_r.at[slot],
                        place(s, 2 * ((x + other) % nx) + c),
                    )
            if dy == 0:
                allowed = True if dx == 0 else c == 1
                send_if(allowed, src, dst, x_sy.at[step], x_r.at[slot], place(2 * z + 1 - y, r))
        send_if(True, src, dst, x_sd.at[step], x_r.at[slot], partner)

    share(0, feats, 0, 0)

    for j in range(nh):
        send_or_local(ids_src, ids_all.at[k], i_s.at[j], i_r.at[k], at(z, j), k == j)
        send_or_local(pay_src.at[j], pay.at[k], p_s.at[j], p_r.at[k], at(z, j), k == j)
        send_if(
            jnp.logical_and(y == 1, z < nz - 1), tail_src.at[j], tail_in.at[r], e_s.at[j], e_r.at[r],
            at(z + 1, j),
        )

    hops = [(dx, dy) for dx in range(nx) for dy in range(2)]
    hops.sort(key=lambda hop: (hop[0] > 0) + hop[1])
    for step, (dx, dy) in enumerate(hops):
        if step > 0:
            slot = 2 * (2 * ((x + dx) % nx) + c) + (y + dy) % 2
            landed(rows(x_all, slot, T), x_r.at[slot])
            share(step, None, dx, dy)

    stride = T + 8
    for m in range(nh):
        base = m * stride + 8
        landed(ids_all.at[m], i_r.at[m])
        landed(pay.at[m], p_r.at[m])
        prev[base : base + T, :] = pay[m, :, :hb].astype(F32)
        up[m * T : (m + 1) * T, :] = pay[m, :, hb:].astype(F32)
        ids_col[base : base + T, :] = jnp.broadcast_to(ids_all[m, 0:1, :], (hb, T)).T
        if m % 2:
            before = base - stride + T
            prev[base - 8 : base, :] = prev[before - 8 : before, :]
            ids_col[base - 8 : base, :] = ids_col[before - 8 : before, :]
        else:

            @pl.when(z > 0)
            def _():
                landed(tail_in.at[m // 2], e_r.at[m // 2])
                prev[base - 8 : base, :] = tail_in[m // 2, 0:8, :]
                ids_col[base - 8 : base, :] = tail_in[m // 2, 8:16, :]

            @pl.when(z == 0)
            def _():
                prev[base - 8 : base, :] = jnp.zeros((8, hb), F32)
                ids_col[base - 8 : base, :] = jnp.full((8, hb), -1.0, F32)

    for g in range(GATES):
        for col in range(nr):
            landed(
                w_all.at[g * hb : (g + 1) * hb, col * cw : (col + 1) * cw], w_r.at[g * nr + col]
            )
    landed(rows(x_all, k, T), x_s0)
    for x0 in range(nx):
        for y0 in range(2):
            slot = 2 * (2 * x0 + 1 - c) + y0
            landed(rows(x_all, slot, T), x_r.at[slot])

    group = pl.ds(pl.multiple_of(k * hb, hb), hb)
    rz, rr, rc = (recur[i : i + 1, group] for i in range(GATES))
    bz, br, bc = (bias[i : i + 1, group] for i in range(GATES))
    for m in range(nh):
        span = slice(m * T, (m + 1) * T)
        base = m * stride + 8
        pre = lax.dot_general(
            x_all[span, :], w_all[...], (((1,), (1,)), ((), ())), preferred_element_type=F32
        )
        same = jnp.where(
            ids_col[base : base + T, :] == ids_col[base - 1 : base - 1 + T, :], 1.0, 0.0
        )
        prior = prev[base - 1 : base - 1 + T, :] * same
        gz = jax.nn.sigmoid(pre[:, :hb] + rz * prior + bz)
        gr = jax.nn.sigmoid(pre[:, hb : 2 * hb] + rr * prior + br)
        rp = gr * prior
        gc = jnp.tanh(pre[:, 2 * hb :] + rc * rp + bc)
        az = (gc - prior) * gz * (1.0 - gz)
        ac = gz * (1.0 - gc * gc)
        slope = rp * (1.0 - gr)
        acr = ac * rc
        co_z[span, :] = az
        co_c[span, :] = ac
        co_r[span, :] = acr * slope
        rprior[span, :] = rp
        prior_all[span, :] = prior
        jac[span, :] = same * (1.0 - gz + az * rz + acr * (gr + slope * rr))

    def back(i, state):
        a, b = state
        t = T - 1 - i
        f = jac[pl.ds(t, nh, stride=T), :]
        b = b + up[pl.ds(t, nh, stride=T), :]
        scan_a[t] = a
        scan_b[t] = b
        return f * a, f * b

    a, b = lax.fori_loop(0, T, back, (jnp.ones((nh, hb), F32), jnp.zeros((nh, hb), F32)), unroll=8)
    seg_out[...] = jnp.zeros(seg_out.shape, F32)
    for o in range(nr):
        first, second = slice(2 * o, 2 * o + 1), slice(2 * o + 1, 2 * o + 2)
        seg_out[0, o : o + 1, :] = a[first, :] * a[second, :]
        seg_out[1, o : o + 1, :] = b[first, :] + a[first, :] * b[second, :]
    for plane in range(nz - 1):
        send_if(plane < z, seg_out, seg_in.at[z], c_s.at[plane], c_r.at[z], at(plane, k))
    carry[...] = jnp.zeros(carry.shape, F32)
    for plane in reversed(range(1, nz)):

        @pl.when(plane > z)
        def _():
            landed(seg_in.at[plane], c_r.at[plane])
            carry[0:nr, :] = seg_in[plane, 1, 0:nr, :] + seg_in[plane, 0, 0:nr, :] * carry[0:nr, :]

    into = carry[0:nr, :]
    carry_rows = []
    for o in range(nr):
        later = into[o : o + 1, :]
        second = slice(2 * o + 1, 2 * o + 2)
        carry_rows += [b[second, :] + a[second, :] * later, later]
    carried = jnp.concatenate(carry_rows, 0)

    def finish(t, _):
        lam[pl.ds(t, nh, stride=T), :] = scan_b[t] + scan_a[t] * carried
        return 0

    lax.fori_loop(0, T, finish, 0, unroll=8)

    sums = [jnp.zeros((1, hb), F32) for _ in range(6)]
    for m in range(nh):
        span = slice(m * T, (m + 1) * T)
        prior = prior_all[span, :]
        adj = lam[span, :]
        grad_z = adj * co_z[span, :]
        grad_r = adj * co_r[span, :]
        grad_c = adj * co_c[span, :]
        grads[span, :hb] = grad_z.astype(BF16)
        grads[span, hb : 2 * hb] = grad_r.astype(BF16)
        grads[span, 2 * hb :] = grad_c.astype(BF16)
        terms = (grad_z, grad_r, grad_c, grad_z * prior, grad_r * prior, grad_c * rprior[span, :])
        sums = [total + jnp.sum(term, 0, keepdims=True) for total, term in zip(sums, terms)]
    for i in range(6):
        st_out[i : i + 1, :] = sums[i]
    st_out[6:8, :] = jnp.zeros((2, hb), F32)

    slot = k * nz + z
    st_in[slot] = st_out[...]

    def tell(d, _):
        @pl.when(d != me)
        def _():
            send(st_out, st_in.at[slot], t_s.at[d], t_r.at[slot], place(d // nr, d % nr))

        return 0

    lax.fori_loop(0, ns * nr, tell, 0)

    for g in range(GATES):
        wg_out[g] = lax.dot_general(
            grads[:, g * hb : (g + 1) * hb], x_all[...], (((0,), (0,)), ((), ())),
            preferred_element_type=F32,
        ).astype(BF16)
        b = g * nh + k
        owner, i = b // GATES, b % GATES
        for col in range(nr):
            here = jnp.logical_and(owner == s, r == col)
            send_or_local(
                wg_out.at[g, :, col * cw : (col + 1) * cw], wg_in.at[z * GATES + i],
                g_s.at[g * nr + col], g_r.at[z * GATES + i], place(owner, col), here,
            )

    chips = [(x0, y0) for x0 in range(nx) for y0 in range(2)]
    for n, (x0, y0) in enumerate(chips):
        part_out[n] = jnp.dot(
            rows(grads, 2 * (2 * x0 + 1 - c) + y0, T)[...], w_all[...], preferred_element_type=F32
        ).astype(BF16)
        send_if(True, part_out.at[n], part_in.at[n], d_s.at[n], d_r.at[n], partner)
    for n, (x0, y0) in enumerate(chips):
        part_keep[n] = jnp.dot(
            rows(grads, 2 * (2 * x0 + c) + y0, T)[...], w_all[...], preferred_element_type=F32
        )
    chip = 2 * x + y
    for n, (x0, y0) in enumerate(chips):
        landed(part_in.at[n], d_r.at[n])
        fin_out[n] = (part_keep[n] + part_in[n].astype(F32)).astype(BF16)
        send_or_local(
            fin_out.at[n], fin_in.at[chip], f_s.at[n], f_r.at[chip],
            place(2 * z + y0, 2 * x0 + c), chip == n,
        )

    scale = 1.0 / math.sqrt(ns * nr * T)

    def heard(d, _):
        @pl.when(d != slot)
        def _():
            landed(st_in.at[d], t_r.at[d])

        return 0

    lax.fori_loop(0, ns * nr, heard, 0)
    for j in range(nh):
        total = st_in[j * nz]
        for other in range(1, nz):
            total = total + st_in[j * nz + other]
        out_p[:, j * hb : (j + 1) * hb] = total[:6] * scale

    total = None
    for n in range(len(chips)):
        landed(fin_in.at[n], f_r.at[n])
        term = fin_in[n].astype(F32)
        total = term if total is None else total + term
    out_in[...] = total.astype(BF16)

    for i in range(GATES):
        total = None
        for other in range(nz):
            landed(wg_in.at[other * GATES + i], g_r.at[other * GATES + i])
            term = wg_in[other * GATES + i].astype(F32)
            total = term if total is None else total + term
        out_w[i * hb : (i + 1) * hb, :] = total * scale

    def told(d, _):
        @pl.when(d != me)
        def _():
            landed(st_out, t_s.at[d])

        return 0

    lax.fori_loop(0, ns * nr, told, 0)
    for sent, src, sem in unsent:
        if sent is True:
            landed(src, sem)
        else:

            @pl.when(sent)
            def _():
                landed(src, sem)


def flush(in_a, in_b, in_c, out_a, out_b, out_c, sems):
    pairs = [(in_a, out_a), (in_b, out_b), (in_c, out_c)]
    copies = [pltpu.make_async_copy(a, b, sems.at[i]) for i, (a, b) in enumerate(pairs)]
    for copy in copies:
        copy.start()
    for copy in copies:
        copy.wait()


def by_hidden(ns, nr, inputs, weight_t, states, doc_ids, recur, bias, out_grad):
    T, DI = inputs.shape[1:]
    H = states.shape[2]
    nh, nz, nx = 2 * nr, ns // 2, nr // 2
    hb, cw = H // nh, DI // nr
    L = nh * T
    vm = pltpu.VMEM
    scratch = [
        vm((nh, T, 2 * hb), BF16),
        vm((nh, T, 2 * hb), BF16),
        vm((8, T), F32),
        vm((nh, 8, T), F32),
        vm((nh, 16, hb), F32),
        vm((nr, 16, hb), F32),
        vm((L, DI), BF16),
        vm((GATES * hb, DI), BF16),
        vm((L + 8 * nh, hb), F32),
        vm((L + 8 * nh, hb), F32),
        vm((L, hb), F32),
        vm((L, hb), F32),
        vm((L, hb), F32),
        vm((L, hb), F32),
        vm((L, hb), F32),
        vm((L, hb), F32),
        vm((L, hb), F32),
        vm((T, nh, hb), F32),
        vm((T, nh, hb), F32),
        vm((nh, hb), F32),
        vm((2, 8, hb), F32),
        vm((nz, 2, 8, hb), F32),
        vm((L, hb), F32),
        vm((L, GATES * hb), BF16),
        vm((nr, T, DI), BF16),
        vm((nr, T, DI), BF16),
        vm((nr, T, DI), F32),
        vm((nr, T, DI), BF16),
        vm((nr, T, DI), BF16),
        vm((GATES, hb, DI), BF16),
        vm((nz * GATES, hb, cw), BF16),
        vm((8, hb), F32),
        vm((ns * nr, 8, hb), F32),
    ]
    dma = pltpu.SemaphoreType.DMA
    counts = [
        None, nr * nx, nr, nr, nh, GATES * nz, GATES * nr, nh, nh, nh, nh, nh, nr, nz, nz, nr, nr, nr, nr,
        GATES * nr, GATES * nz, ns * nr, ns * nr,
    ]
    sems = [dma if n is None else dma((n,)) for n in counts]
    whole = pl.BlockSpec(memory_space=pltpu.VMEM)
    out_in, out_w, out_p = pl.pallas_call(
        functools.partial(kernel, ns, nr),
        out_shape=(
            pltpu.VMEM((T, DI), BF16),
            pltpu.VMEM(weight_t.shape, F32),
            pltpu.VMEM((6, H), F32),
        ),
        in_specs=[whole] * 7,
        out_specs=(whole,) * 3,
        scratch_shapes=scratch + sems,
        compiler_params=pltpu.CompilerParams(
            collective_id=0, has_side_effects=True, vmem_limit_bytes=56 * 1024 * 1024
        ),
    )(inputs[0], weight_t, states[0], doc_ids, recur, bias, out_grad[0])
    shapes = ((T, DI), BF16), (weight_t.shape, F32), ((6, H), F32)
    out_in, out_w, out_p = pl.pallas_call(
        flush,
        out_shape=tuple(jax.ShapeDtypeStruct(*one) for one in shapes),
        in_specs=[whole] * 3,
        out_specs=(pl.BlockSpec(memory_space=pltpu.HBM),) * 3,
        scratch_shapes=[dma((3,))],
    )(*(pltpu.with_memory_space_constraint(one, pltpu.VMEM) for one in (out_in, out_w, out_p)))
    return out_in[None], out_w, out_p


def fits(ns, nr, inputs, weight_t, states):
    parts, L, DI = inputs.shape
    H = states.shape[2]
    return (
        parts == nr
        and ns == 2 * nr
        and ns % 8 == 0
        and ns == 8
        and H % (ns * 128) == 0
        and DI % (nr * 128) == 0
        and L % (ns * 128) == 0
        and L * DI <= 1 << 21
    )


def solution(mesh):
    ns, nr = mesh.shape["seq"], mesh.shape["rep"]
    placed = (
        P("rep", "seq", None),
        P("seq", "rep"),
        P("rep", "seq", None),
        P("rep", "seq"),
        P(),
        P(),
        P("rep", "seq", None),
    )

    def run(inputs, weight_t, states, doc_ids, recur, bias, out_grad):
        kernelized = fits(ns, nr, inputs, weight_t, states)
        body = functools.partial(by_hidden, ns, nr) if kernelized else by_tokens
        return jax.shard_map(
            body,
            mesh=mesh,
            in_specs=placed,
            out_specs=(P("rep", "seq", None), P("seq", "rep"), P()),
            check_vma=False,
        )(inputs, weight_t, states, doc_ids, recur, bias, out_grad)

    return run
```

```python
import functools
import math

import jax
import jax.numpy as jnp
from jax import lax
from jax.experimental import pallas as pl
from jax.experimental.pallas import tpu as pltpu
from jax.sharding import PartitionSpec as P

F32 = jnp.float32
BF16 = jnp.bfloat16
GATES = 3


def shifted(block, axis, distance):
    devices = range(lax.axis_size(axis))
    route = [(i - distance, i) for i in devices if i - distance in devices]
    return lax.ppermute(block, axis, route)


def compose(earlier, later):
    return (later[0] * earlier[0], later[1] + later[0] * earlier[1])


def by_tokens(inputs, weight_t, states, doc_ids, recur, bias, out_grad):
    feats = inputs[0]
    hidden_now = states[0]
    ids_float = doc_ids[0].astype(F32)
    count = feats.shape[0]
    width = hidden_now.shape[1]
    columns = lax.all_gather(weight_t, "rep", axis=1, tiled=True)
    contract_last = (((1,), (1,)), ((), ()))
    full_weight = lax.all_gather(columns, "seq", axis=0, tiled=True)
    preact = lax.dot_general(feats, full_weight, contract_last, preferred_element_type=F32)
    tail_state, tail_id = shifted((hidden_now[-1:], ids_float[-1:]), "seq", 1)
    first_same = jnp.where(
        (ids_float[0] == tail_id[0]) & (lax.axis_index("seq") > 0), 1.0, 0.0
    ).astype(F32)
    same = jnp.concatenate([first_same[None], (ids_float[1:] == ids_float[:-1]).astype(F32)])
    prior = jnp.concatenate([tail_state, hidden_now[:-1]], 0) * same[:, None]
    gate_z = jax.nn.sigmoid(preact[:, :width] + recur[0] * prior + bias[0])
    gate_r = jax.nn.sigmoid(preact[:, width : 2 * width] + recur[1] * prior + bias[1])
    gate_c = jnp.tanh(preact[:, 2 * width :] + recur[2] * gate_r * prior + bias[2])
    jacobian = same[:, None] * (
        1.0
        - gate_z
        + (gate_c - prior) * gate_z * (1.0 - gate_z) * recur[0]
        + gate_z
        * (1.0 - gate_c * gate_c)
        * recur[2]
        * (gate_r + prior * gate_r * (1.0 - gate_r) * recur[1])
    )
    upstream = out_grad[0].astype(F32)
    jac_rows, up_rows = (
        lax.all_to_all(jacobian.T, "seq", split_axis=0, concat_axis=1, tiled=True),
        lax.all_to_all(upstream.T, "seq", split_axis=0, concat_axis=1, tiled=True),
    )
    factor = jnp.concatenate([jac_rows[:, 1:], jnp.zeros((jac_rows.shape[0], 1), F32)], 1)
    _, adjoint_rows = lax.associative_scan(compose, (factor, up_rows), reverse=True, axis=1)
    adjoint = lax.all_to_all(adjoint_rows, "seq", split_axis=1, concat_axis=0, tiled=True).T
    grad_z = adjoint * (gate_c - prior) * gate_z * (1.0 - gate_z)
    grad_c = adjoint * gate_z * (1.0 - gate_c * gate_c)
    grad_r = grad_c * recur[2] * prior * gate_r * (1.0 - gate_r)
    grad_pre = jnp.concatenate([grad_z, grad_r, grad_c], 1).astype(BF16)
    input_grad = jnp.dot(grad_pre, full_weight, preferred_element_type=F32)
    tokens_all = count * inputs.shape[0] * lax.axis_size("seq") * lax.axis_size("rep")
    normal_factor = 1.0 / math.sqrt(tokens_all)
    row_share = lax.psum_scatter(
        lax.dot_general(grad_pre, feats, (((0,), (0,)), ((), ())), preferred_element_type=F32),
        "seq",
        scatter_dimension=0,
        tiled=True,
    )
    weight_grad = (
        lax.psum_scatter(row_share.astype(BF16), "rep", scatter_dimension=1, tiled=True).astype(F32)
        * normal_factor
    )
    stats = jnp.stack(
        [
            grad_z.sum(0),
            grad_r.sum(0),
            grad_c.sum(0),
            (grad_z * prior).sum(0),
            (grad_r * prior).sum(0),
            (grad_c * gate_r * prior).sum(0),
        ]
    )
    param_grad = lax.psum(stats, ("seq", "rep")) * normal_factor
    return (input_grad.astype(BF16)[None], weight_grad, param_grad)


def kernel(
    ns, nr, feats, weight, states, ids, recur, bias, upstream,
    out_in, out_w, out_p,
    pay_src, pay, ids_src, ids_all, tail_src, tail_in, x_all, w_all, prev, ids_col, up, jac,
    co_z, co_r, co_c, rprior, prior_all,
    scan_a, scan_b, carry, seg_out, seg_in, lam, grads, part_out, part_in, part_keep, fin_out, fin_in,
    wg_own, wg_out, wg_end, wg_mid, wg_fin, wg_in, st_out, st_z, st_sum, st_all,
    x_s0, x_sx, x_sy, x_sd, x_r, w_s, w_f, w_r, p_s, p_r, i_s, i_r, e_s, e_r, c_s, c_r, d_s, d_r, f_s, f_r,
    g_s, g_e, g_m, g_f, g_r, t_s, t_r, u_s, u_r,
):
    T, DI = feats.shape
    H = states.shape[1]
    nh, nz, nx = 2 * nr, ns // 2, nr // 2
    hb, cw = H // nh, DI // nr
    s, r = lax.axis_index("seq"), lax.axis_index("rep")
    z, y, x, c = s // 2, s % 2, r // 2, r % 2
    k = 2 * r + y
    half, per = nz // 2, GATES * nh // nz
    high = z // half
    inner = jnp.logical_or(z == half - 1, z == half)
    end = high * (nz - 1)
    unsent = []

    def place(a, b):
        return {"seq": a, "rep": b}

    def at(plane, j):
        return place(2 * plane + j % 2, j // 2)

    def column(plane):
        return place(2 * plane + y, r)

    def send(src, dst, ssem, rsem, where):
        pltpu.make_async_remote_copy(
            src_ref=src, dst_ref=dst, send_sem=ssem, recv_sem=rsem,
            device_id=where, device_id_type=pl.DeviceIdType.MESH,
        ).start()

    def local(src, dst, rsem):
        pltpu.make_async_copy(src, dst, rsem).start()

    def landed(dst, sem):
        pltpu.make_async_copy(dst, dst, sem).wait()

    def send_if(allowed, src, dst, ssem, rsem, where):
        @pl.when(allowed)
        def _():
            send(src, dst, ssem, rsem, where)

        unsent.append((allowed, src, ssem))

    def send_or_local(src, dst, ssem, rsem, where, here):
        send_if(jnp.logical_not(here), src, dst, ssem, rsem, where)

        @pl.when(here)
        def _():
            local(src, dst, rsem)

    def rows(ref, block, count):
        return ref.at[pl.ds(pl.multiple_of(block * count, count), count), :]

    barrier = pltpu.get_barrier_semaphore()

    def greet(where):
        pl.semaphore_signal(barrier, inc=1, device_id=where, device_id_type=pl.DeviceIdType.MESH)

    for j in range(nh):
        pl.when(j != k)(functools.partial(greet, at(z, j)))
    for plane in range(nz):
        pl.when(plane != z)(functools.partial(greet, column(plane)))
    for j in range(nh):
        pay_src[j, :, :hb] = states[:, j * hb : (j + 1) * hb].astype(BF16)
        pay_src[j, :, hb:] = upstream[:, j * hb : (j + 1) * hb]
    ids_src[...] = jnp.broadcast_to(ids[...].astype(F32), ids_src.shape)

    pl.semaphore_wait(barrier, nh - 1 + nz - 1)

    def piece(g, col):
        return w_all.at[pl.ds(pl.multiple_of(g * hb, hb), hb), col]

    mine = pl.ds(pl.multiple_of(r * cw, cw), cw)
    for i in range(GATES):
        b = GATES * s + i
        g, j = b // nh, b % nh
        send_or_local(
            weight.at[i * hb : (i + 1) * hb, :], piece(g, mine), w_s.at[i], w_r.at[g * nr + r],
            at(z, j), j == k,
        )
    partner = place(s, r + 1 - 2 * c)
    local(feats, rows(x_all, k, T), x_s0)

    def share(step, src, dx, dy):
        x0, y0 = (x + dx) % nx, (y + dy) % 2
        slot = 2 * (2 * x0 + c) + y0
        dst = rows(x_all, slot, T)
        src = dst if src is None else src
        if dy == 0 or dx == 0:
            for other in range(1, nx):
                if dx == 0:
                    allowed = True if dy == 0 else c == 0
                    send_if(
                        allowed, src, dst, x_sx.at[step * nx + other], x_r.at[slot],
                        place(s, 2 * ((x + other) % nx) + c),
                    )
            if dy == 0:
                allowed = True if dx == 0 else c == 1
                send_if(allowed, src, dst, x_sy.at[step], x_r.at[slot], place(2 * z + 1 - y, r))
        send_if(True, src, dst, x_sd.at[step], x_r.at[slot], partner)

    share(0, feats, 0, 0)

    for j in range(nh):
        send_or_local(ids_src, ids_all.at[k], i_s.at[j], i_r.at[k], at(z, j), k == j)
        send_or_local(pay_src.at[j], pay.at[k], p_s.at[j], p_r.at[k], at(z, j), k == j)

    def origin(step):
        plane = (z + (1 - 2 * high) * step + nz) % nz
        g = (per * plane - k + nh - 1) // nh
        return plane, g % GATES, jnp.logical_and(g < GATES, nh * g + k < per * (plane + 1))

    def spread(step):
        plane, g, found = origin(step)
        for col in range(nr):
            cols = slice(col * cw, (col + 1) * cw)
            block, sem = piece(g, cols), w_r.at[g * nr + col]
            if step == 0:
                pl.when(found)(functools.partial(landed, block, sem))
                for n, target in enumerate((half - high, z + 1 - 2 * (z % half))):
                    send_if(found, block, block, w_f.at[n * nr + col], sem, column(target))
            else:
                go = jnp.logical_and(found, inner)
                pl.when(go)(functools.partial(landed, block, sem))
                send_if(go, block, block, w_f.at[(step + 1) * nr + col], sem, column(end))

    hops = [(dx, dy) for dx in range(nx) for dy in range(2)]
    hops.sort(key=lambda hop: (hop[0] > 0) + hop[1])
    spread(0)
    spread(1)
    for step, (dx, dy) in enumerate(hops):
        if step > 0:
            slot = 2 * (2 * ((x + dx) % nx) + c) + (y + dy) % 2
            landed(rows(x_all, slot, T), x_r.at[slot])
            share(step, None, dx, dy)
    spread(2)

    stride = T + 8
    for m in range(nh):
        base = m * stride + 8
        landed(ids_all.at[m], i_r.at[m])
        landed(pay.at[m], p_r.at[m])
        prev[base : base + T, :] = pay[m, :, :hb].astype(F32)
        up[m * T : (m + 1) * T, :] = pay[m, :, hb:].astype(F32)
        ids_col[base : base + T, :] = jnp.broadcast_to(ids_all[m, 0:1, :], (hb, T)).T
        if m % 2:
            before = base - stride + T
            o = m // 2
            prev[base - 8 : base, :] = prev[before - 8 : before, :]
            ids_col[base - 8 : base, :] = ids_col[before - 8 : before, :]
            tail_src[o : o + 1, :] = prev[base + T - 1 : base + T, :]
            tail_src[8 + o : 9 + o, :] = ids_col[base + T - 1 : base + T, :]

    send_if(z < nz - 1, tail_src, tail_in, e_s, e_r, column((z + 1) % nz))

    for step in range(1, nz):
        plane, g, found = origin(step)
        late = found if step == nz - 1 else jnp.logical_and(found, jnp.logical_not(inner))
        for col in range(nr):
            block = piece(g, slice(col * cw, (col + 1) * cw))
            pl.when(late)(functools.partial(landed, block, w_r.at[g * nr + col]))

    @pl.when(z > 0)
    def _():
        landed(tail_in, e_r)
        for o in range(nr):
            base = 2 * o * stride + 8
            prev[base - 1 : base, :] = tail_in[o : o + 1, :]
            ids_col[base - 1 : base, :] = tail_in[8 + o : 9 + o, :]

    @pl.when(z == 0)
    def _():
        for o in range(nr):
            base = 2 * o * stride + 8
            prev[base - 1 : base, :] = jnp.zeros((1, hb), F32)
            ids_col[base - 1 : base, :] = jnp.full((1, hb), -1.0, F32)

    landed(rows(x_all, k, T), x_s0)
    for x0 in range(nx):
        for y0 in range(2):
            slot = 2 * (2 * x0 + 1 - c) + y0
            landed(rows(x_all, slot, T), x_r.at[slot])

    group = pl.ds(pl.multiple_of(k * hb, hb), hb)
    rz, rr, rc = (recur[i : i + 1, group] for i in range(GATES))
    bz, br, bc = (bias[i : i + 1, group] for i in range(GATES))
    for m in range(nh):
        span = slice(m * T, (m + 1) * T)
        base = m * stride + 8
        pre = lax.dot_general(
            x_all[span, :], w_all[...], (((1,), (1,)), ((), ())), preferred_element_type=F32
        )
        same = jnp.where(
            ids_col[base : base + T, :] == ids_col[base - 1 : base - 1 + T, :], 1.0, 0.0
        )
        prior = prev[base - 1 : base - 1 + T, :] * same
        gz = jax.nn.sigmoid(pre[:, :hb] + rz * prior + bz)
        gr = jax.nn.sigmoid(pre[:, hb : 2 * hb] + rr * prior + br)
        rp = gr * prior
        gc = jnp.tanh(pre[:, 2 * hb :] + rc * rp + bc)
        az = (gc - prior) * gz * (1.0 - gz)
        ac = gz * (1.0 - gc * gc)
        slope = rp * (1.0 - gr)
        acr = ac * rc
        co_z[span, :] = az
        co_c[span, :] = ac
        co_r[span, :] = acr * slope
        rprior[span, :] = rp
        prior_all[span, :] = prior
        jac[span, :] = same * (1.0 - gz + az * rz + acr * (gr + slope * rr))

    def back(i, state):
        a, b = state
        t = T - 1 - i
        f = jac[pl.ds(t, nh, stride=T), :]
        b = b + up[pl.ds(t, nh, stride=T), :]
        scan_a[t] = a
        scan_b[t] = b
        return f * a, f * b

    a, b = lax.fori_loop(0, T, back, (jnp.ones((nh, hb), F32), jnp.zeros((nh, hb), F32)), unroll=8)
    seg_out[...] = jnp.zeros(seg_out.shape, F32)
    for o in range(nr):
        first, second = slice(2 * o, 2 * o + 1), slice(2 * o + 1, 2 * o + 2)
        seg_out[0, o : o + 1, :] = a[first, :] * a[second, :]
        seg_out[1, o : o + 1, :] = b[first, :] + a[first, :] * b[second, :]
    for plane in range(nz - 1):
        send_if(plane < z, seg_out, seg_in.at[z], c_s.at[plane], c_r.at[z], at(plane, k))
    carry[...] = jnp.zeros(carry.shape, F32)
    for plane in reversed(range(1, nz)):

        @pl.when(plane > z)
        def _():
            landed(seg_in.at[plane], c_r.at[plane])
            carry[0:nr, :] = seg_in[plane, 1, 0:nr, :] + seg_in[plane, 0, 0:nr, :] * carry[0:nr, :]

    into = carry[0:nr, :]
    carry_rows = []
    for o in range(nr):
        later = into[o : o + 1, :]
        second = slice(2 * o + 1, 2 * o + 2)
        carry_rows += [b[second, :] + a[second, :] * later, later]
    carried = jnp.concatenate(carry_rows, 0)

    def finish(t, _):
        lam[pl.ds(t, nh, stride=T), :] = scan_b[t] + scan_a[t] * carried
        return 0

    lax.fori_loop(0, T, finish, 0, unroll=8)

    sums = [jnp.zeros((1, hb), F32) for _ in range(6)]
    for m in range(nh):
        span = slice(m * T, (m + 1) * T)
        prior = prior_all[span, :]
        adj = lam[span, :]
        grad_z = adj * co_z[span, :]
        grad_r = adj * co_r[span, :]
        grad_c = adj * co_c[span, :]
        grads[span, :hb] = grad_z.astype(BF16)
        grads[span, hb : 2 * hb] = grad_r.astype(BF16)
        grads[span, 2 * hb :] = grad_c.astype(BF16)
        terms = (grad_z, grad_r, grad_c, grad_z * prior, grad_r * prior, grad_c * rprior[span, :])
        sums = [total + jnp.sum(term, 0, keepdims=True) for total, term in zip(sums, terms)]
    for i in range(6):
        st_out[i : i + 1, :] = sums[i]
    st_out[6:8, :] = jnp.zeros((2, hb), F32)
    st_z[z] = st_out[...]
    for plane in range(nz):
        send_if(plane != z, st_out, st_z.at[z], t_s.at[plane], t_r.at[z], column(plane))

    def quarter(col):
        return slice(col * cw, (col + 1) * cw)

    def gate_of(step):
        g = high * step + (1 - high) * (GATES - 1 - step)
        return g, (nh * g + k) // per

    for step in range(GATES):
        g, plane = gate_of(step)
        block = lax.dot_general(
            grads[:, pl.ds(pl.multiple_of(g * hb, hb), hb)], x_all[...], (((0,), (0,)), ((), ())),
            preferred_element_type=F32,
        )
        wg_own[g] = block
        wg_out[g] = block.astype(BF16)
        outward = jnp.logical_and(inner, plane == end)
        inward = jnp.logical_and(jnp.logical_not(inner), plane != z)
        for col in range(nr):
            part = wg_out.at[g, :, quarter(col)]
            send_if(
                inward, part, wg_end.at[g, :, quarter(col)], g_s.at[step * nr + col],
                g_e.at[g * nr + col], column(high + half - 1),
            )
            send_if(
                outward, part, wg_mid.at[0, :, quarter(col)], g_s.at[step * nr + col],
                g_m.at[col], column(end),
            )

    chips = [(x0, y0) for x0 in range(nx) for y0 in range(2)]
    for n, (x0, y0) in enumerate(chips):
        part_out[n] = jnp.dot(
            rows(grads, 2 * (2 * x0 + 1 - c) + y0, T)[...], w_all[...], preferred_element_type=F32
        ).astype(BF16)
        send_if(True, part_out.at[n], part_in.at[n], d_s.at[n], d_r.at[n], partner)
    for n, (x0, y0) in enumerate(chips):
        part_keep[n] = jnp.dot(
            rows(grads, 2 * (2 * x0 + c) + y0, T)[...], w_all[...], preferred_element_type=F32
        )
    chip = 2 * x + y
    for n, (x0, y0) in enumerate(chips):
        landed(part_in.at[n], d_r.at[n])
        fin_out[n] = (part_keep[n] + part_in[n].astype(F32)).astype(BF16)
        send_or_local(
            fin_out.at[n], fin_in.at[chip], f_s.at[n], f_r.at[chip],
            place(2 * z + y0, 2 * x0 + c), chip == n,
        )

    scale = 1.0 / math.sqrt(ns * nr * T)
    for plane in range(nz):
        pl.when(plane != z)(functools.partial(landed, st_z.at[plane], t_r.at[plane]))
    total = st_z[0]
    for plane in range(1, nz):
        total = total + st_z[plane]
    st_sum[...] = total * scale
    st_all[k] = st_sum[...]
    for j in range(nh):
        send_if(j != k, st_sum, st_all.at[k], u_s.at[j], u_r.at[k], at(z, j))

    for step in range(GATES):
        g, plane = gate_of(step)
        passed = jnp.logical_and(inner, jnp.logical_and(plane != z, plane != end))
        far = (plane // half != high) & ((plane == 0) | (plane == nz - 1))
        for col in range(nr):
            cols = quarter(col)

            @pl.when(passed)
            def _():
                landed(wg_end.at[g, :, cols], g_e.at[g * nr + col])
                wg_out[g, :, cols] = (wg_own[g, :, cols] + wg_end[g, :, cols].astype(F32)).astype(BF16)

            for slot, there in enumerate((jnp.logical_not(far), far)):
                send_if(
                    jnp.logical_and(passed, there), wg_out.at[g, :, cols], wg_mid.at[slot, :, cols],
                    g_s.at[step * nr + col], g_m.at[slot * nr + col], column(plane),
                )

    _, g, found = origin(0)
    b = nh * g + k
    owner, i = b // GATES, b % GATES
    for col in range(nr):
        cols = quarter(col)

        @pl.when(found)
        def _():
            landed(wg_mid.at[0, :, cols], g_m.at[col])
            wg_fin[:, cols] = wg_own[g, :, cols] + wg_mid[0, :, cols].astype(F32)

        @pl.when(jnp.logical_and(found, inner))
        def _():
            landed(wg_end.at[g, :, cols], g_e.at[g * nr + col])
            wg_out[g, :, cols] = (wg_fin[:, cols] + wg_end[g, :, cols].astype(F32)).astype(BF16)

        @pl.when(jnp.logical_and(found, jnp.logical_not(inner)))
        def _():
            landed(wg_mid.at[1, :, cols], g_m.at[nr + col])
            wg_out[g, :, cols] = (wg_fin[:, cols] + wg_mid[1, :, cols].astype(F32)).astype(BF16)

        here = jnp.logical_and(owner == s, r == col)

        @pl.when(jnp.logical_and(found, here))
        def _():
            local(wg_out.at[g, :, cols], wg_in.at[i], g_r.at[i])

        send_if(
            jnp.logical_and(found, jnp.logical_not(here)), wg_out.at[g, :, cols], wg_in.at[i],
            g_f.at[col], g_r.at[i], place(owner, col),
        )

    for j in range(nh):
        pl.when(j != k)(functools.partial(landed, st_all.at[j], u_r.at[j]))
        out_p[:, j * hb : (j + 1) * hb] = st_all[j, :6, :]

    total = None
    for n in range(len(chips)):
        landed(fin_in.at[n], f_r.at[n])
        term = fin_in[n].astype(F32)
        total = term if total is None else total + term
    out_in[...] = total.astype(BF16)

    for i in range(GATES):
        landed(wg_in.at[i], g_r.at[i])
        out_w[i * hb : (i + 1) * hb, :] = wg_in[i].astype(F32) * scale

    for sent, src, sem in unsent:
        if sent is True:
            landed(src, sem)
        else:

            @pl.when(sent)
            def _():
                landed(src, sem)


def flush(in_a, in_b, in_c, out_a, out_b, out_c, sems):
    pairs = [(in_a, out_a), (in_b, out_b), (in_c, out_c)]
    copies = [pltpu.make_async_copy(a, b, sems.at[i]) for i, (a, b) in enumerate(pairs)]
    for copy in copies:
        copy.start()
    for copy in copies:
        copy.wait()


def by_hidden(ns, nr, inputs, weight_t, states, doc_ids, recur, bias, out_grad):
    T, DI = inputs.shape[1:]
    H = states.shape[2]
    nh, nz, nx = 2 * nr, ns // 2, nr // 2
    hb, cw = H // nh, DI // nr
    L = nh * T
    vm = pltpu.VMEM
    scratch = [
        vm((nh, T, 2 * hb), BF16),
        vm((nh, T, 2 * hb), BF16),
        vm((8, T), F32),
        vm((nh, 8, T), F32),
        vm((16, hb), F32),
        vm((16, hb), F32),
        vm((L, DI), BF16),
        vm((GATES * hb, DI), BF16),
        vm((L + 8 * nh, hb), F32),
        vm((L + 8 * nh, hb), F32),
        vm((L, hb), F32),
        vm((L, hb), F32),
        vm((L, hb), F32),
        vm((L, hb), F32),
        vm((L, hb), F32),
        vm((L, hb), F32),
        vm((L, hb), F32),
        vm((T, nh, hb), F32),
        vm((T, nh, hb), F32),
        vm((nh, hb), F32),
        vm((2, 8, hb), F32),
        vm((nz, 2, 8, hb), F32),
        vm((L, hb), F32),
        vm((L, GATES * hb), BF16),
        vm((nr, T, DI), BF16),
        vm((nr, T, DI), BF16),
        vm((nr, T, DI), F32),
        vm((nr, T, DI), BF16),
        vm((nr, T, DI), BF16),
        vm((GATES, hb, DI), F32),
        vm((GATES, hb, DI), BF16),
        vm((GATES, hb, DI), BF16),
        vm((2, hb, DI), BF16),
        vm((hb, DI), F32),
        vm((GATES, hb, cw), BF16),
        vm((8, hb), F32),
        vm((nz, 8, hb), F32),
        vm((8, hb), F32),
        vm((nh, 8, hb), F32),
    ]
    dma = pltpu.SemaphoreType.DMA
    counts = [
        None, nr * nx, nr, nr, nh, GATES, nz * nr, GATES * nr, nh, nh, nh, nh, None, None, nz, nz,
        nr, nr, nr, nr, GATES * nr, GATES * nr, 2 * nr, nr, GATES, nz, nz, nh, nh,
    ]
    sems = [dma if n is None else dma((n,)) for n in counts]
    whole = pl.BlockSpec(memory_space=pltpu.VMEM)
    out_in, out_w, out_p = pl.pallas_call(
        functools.partial(kernel, ns, nr),
        out_shape=(
            pltpu.VMEM((T, DI), BF16),
            pltpu.VMEM(weight_t.shape, F32),
            pltpu.VMEM((6, H), F32),
        ),
        in_specs=[whole] * 7,
        out_specs=(whole,) * 3,
        scratch_shapes=scratch + sems,
        compiler_params=pltpu.CompilerParams(
            collective_id=0, has_side_effects=True, vmem_limit_bytes=56 * 1024 * 1024
        ),
    )(inputs[0], weight_t, states[0], doc_ids, recur, bias, out_grad[0])
    shapes = ((T, DI), BF16), (weight_t.shape, F32), ((6, H), F32)
    out_in, out_w, out_p = pl.pallas_call(
        flush,
        out_shape=tuple(jax.ShapeDtypeStruct(*one) for one in shapes),
        in_specs=[whole] * 3,
        out_specs=(pl.BlockSpec(memory_space=pltpu.HBM),) * 3,
        scratch_shapes=[dma((3,))],
    )(*(pltpu.with_memory_space_constraint(one, pltpu.VMEM) for one in (out_in, out_w, out_p)))
    return out_in[None], out_w, out_p


def fits(ns, nr, inputs, weight_t, states):
    parts, L, DI = inputs.shape
    H = states.shape[2]
    return (
        parts == nr
        and ns == 2 * nr
        and ns % 8 == 0
        and ns == 8
        and H % (ns * 128) == 0
        and DI % (nr * 128) == 0
        and L % (ns * 128) == 0
        and L * DI <= 1 << 21
    )


def solution(mesh):
    ns, nr = mesh.shape["seq"], mesh.shape["rep"]
    placed = (
        P("rep", "seq", None),
        P("seq", "rep"),
        P("rep", "seq", None),
        P("rep", "seq"),
        P(),
        P(),
        P("rep", "seq", None),
    )

    def run(inputs, weight_t, states, doc_ids, recur, bias, out_grad):
        kernelized = fits(ns, nr, inputs, weight_t, states)
        body = functools.partial(by_hidden, ns, nr) if kernelized else by_tokens
        return jax.shard_map(
            body,
            mesh=mesh,
            in_specs=placed,
            out_specs=(P("rep", "seq", None), P("seq", "rep"), P()),
            check_vma=False,
        )(inputs, weight_t, states, doc_ids, recur, bias, out_grad)

    return run
```

```python
import functools
import math

import jax
import jax.numpy as jnp
from jax import lax
from jax.experimental import pallas as pl
from jax.experimental.pallas import tpu as pltpu
from jax.sharding import PartitionSpec as P

F32 = jnp.float32
BF16 = jnp.bfloat16
GATES = 3


def shifted(block, axis, distance):
    devices = range(lax.axis_size(axis))
    route = [(i - distance, i) for i in devices if i - distance in devices]
    return lax.ppermute(block, axis, route)


def compose(earlier, later):
    return (later[0] * earlier[0], later[1] + later[0] * earlier[1])


def by_tokens(inputs, weight_t, states, doc_ids, recur, bias, out_grad):
    feats = inputs[0]
    hidden_now = states[0]
    ids_float = doc_ids[0].astype(F32)
    count = feats.shape[0]
    width = hidden_now.shape[1]
    columns = lax.all_gather(weight_t, "rep", axis=1, tiled=True)
    contract_last = (((1,), (1,)), ((), ()))
    full_weight = lax.all_gather(columns, "seq", axis=0, tiled=True)
    preact = lax.dot_general(feats, full_weight, contract_last, preferred_element_type=F32)
    tail_state, tail_id = shifted((hidden_now[-1:], ids_float[-1:]), "seq", 1)
    first_same = jnp.where(
        (ids_float[0] == tail_id[0]) & (lax.axis_index("seq") > 0), 1.0, 0.0
    ).astype(F32)
    same = jnp.concatenate([first_same[None], (ids_float[1:] == ids_float[:-1]).astype(F32)])
    prior = jnp.concatenate([tail_state, hidden_now[:-1]], 0) * same[:, None]
    gate_z = jax.nn.sigmoid(preact[:, :width] + recur[0] * prior + bias[0])
    gate_r = jax.nn.sigmoid(preact[:, width : 2 * width] + recur[1] * prior + bias[1])
    gate_c = jnp.tanh(preact[:, 2 * width :] + recur[2] * gate_r * prior + bias[2])
    jacobian = same[:, None] * (
        1.0
        - gate_z
        + (gate_c - prior) * gate_z * (1.0 - gate_z) * recur[0]
        + gate_z
        * (1.0 - gate_c * gate_c)
        * recur[2]
        * (gate_r + prior * gate_r * (1.0 - gate_r) * recur[1])
    )
    upstream = out_grad[0].astype(F32)
    jac_rows, up_rows = (
        lax.all_to_all(jacobian.T, "seq", split_axis=0, concat_axis=1, tiled=True),
        lax.all_to_all(upstream.T, "seq", split_axis=0, concat_axis=1, tiled=True),
    )
    factor = jnp.concatenate([jac_rows[:, 1:], jnp.zeros((jac_rows.shape[0], 1), F32)], 1)
    _, adjoint_rows = lax.associative_scan(compose, (factor, up_rows), reverse=True, axis=1)
    adjoint = lax.all_to_all(adjoint_rows, "seq", split_axis=1, concat_axis=0, tiled=True).T
    grad_z = adjoint * (gate_c - prior) * gate_z * (1.0 - gate_z)
    grad_c = adjoint * gate_z * (1.0 - gate_c * gate_c)
    grad_r = grad_c * recur[2] * prior * gate_r * (1.0 - gate_r)
    grad_pre = jnp.concatenate([grad_z, grad_r, grad_c], 1).astype(BF16)
    input_grad = jnp.dot(grad_pre, full_weight, preferred_element_type=F32)
    tokens_all = count * inputs.shape[0] * lax.axis_size("seq") * lax.axis_size("rep")
    normal_factor = 1.0 / math.sqrt(tokens_all)
    row_share = lax.psum_scatter(
        lax.dot_general(grad_pre, feats, (((0,), (0,)), ((), ())), preferred_element_type=F32),
        "seq",
        scatter_dimension=0,
        tiled=True,
    )
    weight_grad = (
        lax.psum_scatter(row_share.astype(BF16), "rep", scatter_dimension=1, tiled=True).astype(F32)
        * normal_factor
    )
    stats = jnp.stack(
        [
            grad_z.sum(0),
            grad_r.sum(0),
            grad_c.sum(0),
            (grad_z * prior).sum(0),
            (grad_r * prior).sum(0),
            (grad_c * gate_r * prior).sum(0),
        ]
    )
    param_grad = lax.psum(stats, ("seq", "rep")) * normal_factor
    return (input_grad.astype(BF16)[None], weight_grad, param_grad)


def kernel(
    ns, nr, feats_hbm, weight_hbm, states_hbm, ids_hbm, recur_hbm, bias_hbm, upstream_hbm,
    out_in, out_w, out_p,
    weight, states, ids, recur, bias, upstream,
    pay_src, pay, up_in, ids_src, ids_all, tail_src, tail_mid, tail_in, x_all, w_all, prev, ids_col, same_all, up,
    jac, co_z, co_r, co_c, rprior, prior_all,
    scan_a, scan_b, carry, seg_out, seg_in, lam, grads, part_out, part_in, part_keep, fin_out, fin_in,
    wg_own, wg_out, wg_end, wg_mid, wg_fin, wg_in, st_out, st_z, st_sum, st_all,
    l_s, x_sx, x_sy, x_sd, x_r, w_s, w_f, w_r, p_s, p_r, v_s, v_r, i_s, i_r, e_s, e_r, n_s, n_r, c_s, c_r,
    d_s, d_r, f_s, f_r, g_s, g_e, g_m, g_f, g_r, t_s, t_r, u_s, u_r,
):
    T, DI = feats_hbm.shape
    H = states.shape[1]
    nh, nz, nx = 2 * nr, ns // 2, nr // 2
    hb, cw = H // nh, DI // nr
    s, r = lax.axis_index("seq"), lax.axis_index("rep")
    z, y, x, c = s // 2, s % 2, r // 2, r % 2
    q = 2 * r + y
    k = nx * 2 * c + 2 * x + y
    half, per = nz // 2, GATES * nh // nz
    high = z // half
    inner = jnp.logical_or(z == half - 1, z == half)
    end = high * (nz - 1)
    unsent = []

    def place(a, b):
        return {"seq": a, "rep": b}

    def at(plane, j):
        return place(2 * plane + j % 2, 2 * (j // 2 % nx) + j // (2 * nx))

    def column(plane):
        return place(2 * plane + y, r)

    def send(src, dst, ssem, rsem, where):
        pltpu.make_async_remote_copy(
            src_ref=src, dst_ref=dst, send_sem=ssem, recv_sem=rsem,
            device_id=where, device_id_type=pl.DeviceIdType.MESH,
        ).start()

    def local(src, dst, rsem):
        pltpu.make_async_copy(src, dst, rsem).start()

    def landed(dst, sem):
        pltpu.make_async_copy(dst, dst, sem).wait()

    def send_if(allowed, src, dst, ssem, rsem, where):
        @pl.when(allowed)
        def _():
            send(src, dst, ssem, rsem, where)

        unsent.append((allowed, src, ssem))

    def send_or_local(src, dst, ssem, rsem, where, here):
        send_if(jnp.logical_not(here), src, dst, ssem, rsem, where)

        @pl.when(here)
        def _():
            local(src, dst, rsem)

    def rows(ref, block, count):
        return ref.at[pl.ds(pl.multiple_of(block * count, count), count), :]

    barrier = pltpu.get_barrier_semaphore()

    def greet(where):
        pl.semaphore_signal(barrier, inc=1, device_id=where, device_id_type=pl.DeviceIdType.MESH)

    for j in range(nh):
        pl.when(j != k)(functools.partial(greet, at(z, j)))
    for plane in range(nz):
        pl.when(plane != z)(functools.partial(greet, column(plane)))
    loads = [
        (weight_hbm, weight), (feats_hbm, rows(x_all, q, T)), (states_hbm, states), (ids_hbm, ids),
        (upstream_hbm, upstream), (recur_hbm, recur), (bias_hbm, bias),
    ]
    for n, (src, dst) in enumerate(loads):
        local(src, dst, l_s.at[n])

    def loaded(n):
        landed(loads[n][1], l_s.at[n])

    loaded(2)
    loaded(3)
    for j in range(nh):
        pay_src[j] = states[:, j * hb : (j + 1) * hb].astype(BF16)
    tail_src[0:4, :] = jnp.broadcast_to(states[T - 1 : T, :], (4, H))
    tail_src[4:8, :] = jnp.broadcast_to(ids[0:1, T - 1 : T].astype(F32), (4, H))
    ids_src[...] = jnp.broadcast_to(ids[...].astype(F32), ids_src.shape)
    loaded(0)
    loaded(1)
    loaded(4)
    pl.semaphore_wait(barrier, nh - 1 + nz - 1)

    hands_on = jnp.logical_and(y == 1, z < nz - 1)
    takes_over = jnp.logical_and(y == 1, z > 0)
    send_if(hands_on, tail_src, tail_mid, n_s, n_r, column((z + 1) % nz))

    def piece(g, col):
        return w_all.at[pl.ds(pl.multiple_of(g * hb, hb), hb), col]

    mine = pl.ds(pl.multiple_of(r * cw, cw), cw)
    for i in range(GATES):
        b = GATES * s + i
        g, j = b // nh, b % nh
        send_or_local(
            weight.at[i * hb : (i + 1) * hb, :], piece(g, mine), w_s.at[i], w_r.at[g * nr + r],
            at(z, j), j == k,
        )
    partner = place(s, r + 1 - 2 * c)

    def share(step, src, dx, dy):
        x0, y0 = (x + dx) % nx, (y + dy) % 2
        slot = 2 * (2 * x0 + c) + y0
        dst = rows(x_all, slot, T)
        src = dst if src is None else src
        if dy == 0 or dx == 0:
            for other in range(1, nx):
                if dx == 0:
                    allowed = True if dy == 0 else c == 0
                    send_if(
                        allowed, src, dst, x_sx.at[step * nx + other], x_r.at[slot],
                        place(s, 2 * ((x + other) % nx) + c),
                    )
            if dy == 0:
                allowed = True if dx == 0 else c == 1
                send_if(allowed, src, dst, x_sy.at[step], x_r.at[slot], place(2 * z + 1 - y, r))
        send_if(True, src, dst, x_sd.at[step], x_r.at[slot], partner)

    share(0, None, 0, 0)
    pl.when(takes_over)(functools.partial(landed, tail_mid, n_r))
    for j in range(nh):
        part = tail_mid.at[:, j * hb : (j + 1) * hb]
        send_if(jnp.logical_and(takes_over, j != k), part, tail_in.at[r], e_s.at[j], e_r.at[r], at(z, j))

        @pl.when(jnp.logical_and(takes_over, j == k))
        def _():
            local(part, tail_in.at[r], e_r.at[r])

    for j in range(nh):
        send_or_local(ids_src, ids_all.at[q], i_s.at[j], i_r.at[q], at(z, j), k == j)
        send_or_local(pay_src.at[j], pay.at[q], p_s.at[j], p_r.at[q], at(z, j), k == j)

    def origin(step):
        plane = (z + (1 - 2 * high) * step + nz) % nz
        g = (per * plane - k + nh - 1) // nh
        return plane, g % GATES, jnp.logical_and(g < GATES, nh * g + k < per * (plane + 1))

    order = []
    for n in range(nr):
        chip = (x + n // 2) % nx
        order.append(2 * chip + (c + n) % 2)

    def spread(step):
        plane, g, found = origin(step)
        for n, col in enumerate(order):
            block = piece(g, pl.ds(pl.multiple_of(col * cw, cw), cw))
            sem = w_r.at[g * nr + col]
            if step == 0:
                pl.when(found)(functools.partial(landed, block, sem))
                for i, target in enumerate((half - high, z + 1 - 2 * (z % half))):
                    send_if(found, block, block, w_f.at[i * nr + n], sem, column(target))
            else:
                go = jnp.logical_and(found, inner)
                pl.when(go)(functools.partial(landed, block, sem))
                send_if(go, block, block, w_f.at[(step + 1) * nr + n], sem, column(end))

    hops = [(dx, dy) for dx in range(nx) for dy in range(2)]
    hops.sort(key=lambda hop: (hop[0] > 0) + hop[1])

    def relay(step):
        dx, dy = hops[step]
        slot = 2 * (2 * ((x + dx) % nx) + c) + (y + dy) % 2
        landed(rows(x_all, slot, T), x_r.at[slot])
        share(step, None, dx, dy)

    spread(0)
    spread(1)
    for step in range(1, len(hops) - 1):
        relay(step)
    for j in range(nh):
        part = upstream.at[:, j * hb : (j + 1) * hb]
        send_or_local(part, up_in.at[q], v_s.at[j], v_r.at[q], at(z, j), k == j)
    spread(2)

    stride = T + 8
    for m in range(nh):
        base = m * stride + 8
        span = slice(m * T, (m + 1) * T)
        landed(ids_all.at[m], i_r.at[m])
        landed(pay.at[m], p_r.at[m])
        prev[base : base + T, :] = pay[m].astype(F32)
        ids_col[base : base + T, :] = jnp.broadcast_to(ids_all[m, 0:1, :], (hb, T)).T
        if m % 2:
            before = base - stride + T - 1
            prev[base - 1 : base, :] = prev[before : before + 1, :]
            ids_col[base - 1 : base, :] = ids_col[before : before + 1, :]
        else:

            @pl.when(z > 0)
            def _():
                landed(tail_in.at[m // 2], e_r.at[m // 2])
                prev[base - 1 : base, :] = tail_in[m // 2, 0:1, :]
                ids_col[base - 1 : base, :] = tail_in[m // 2, 4:5, :]

            @pl.when(z == 0)
            def _():
                prev[base - 1 : base, :] = jnp.zeros((1, hb), F32)
                ids_col[base - 1 : base, :] = jnp.full((1, hb), -1.0, F32)

        same = jnp.where(
            ids_col[base : base + T, :] == ids_col[base - 1 : base - 1 + T, :], 1.0, 0.0
        )
        same_all[span, :] = same
        prior_all[span, :] = prev[base - 1 : base - 1 + T, :] * same

    loaded(5)
    loaded(6)
    relay(len(hops) - 1)
    for step in range(1, nz):
        plane, g, found = origin(step)
        late = found if step == nz - 1 else jnp.logical_and(found, jnp.logical_not(inner))
        for col in range(nr):
            block = piece(g, slice(col * cw, (col + 1) * cw))
            pl.when(late)(functools.partial(landed, block, w_r.at[g * nr + col]))

    group = pl.ds(pl.multiple_of(k * hb, hb), hb)
    rz, rr, rc = (recur[i : i + 1, group] for i in range(GATES))
    bz, br, bc = (bias[i : i + 1, group] for i in range(GATES))
    for dx, dy in hops:
        for core in range(2):
            m = 2 * (2 * ((x + dx) % nx) + (c + core) % 2) + (y + dy) % 2
            if core:
                landed(rows(x_all, m, T), x_r.at[m])
            span = pl.ds(pl.multiple_of(m * T, T), T)
            pre = lax.dot_general(
                x_all[span, :], w_all[...], (((1,), (1,)), ((), ())), preferred_element_type=F32
            )
            prior = prior_all[span, :]
            gz = jax.nn.sigmoid(pre[:, :hb] + rz * prior + bz)
            gr = jax.nn.sigmoid(pre[:, hb : 2 * hb] + rr * prior + br)
            rp = gr * prior
            gc = jnp.tanh(pre[:, 2 * hb :] + rc * rp + bc)
            az = (gc - prior) * gz * (1.0 - gz)
            ac = gz * (1.0 - gc * gc)
            slope = rp * (1.0 - gr)
            acr = ac * rc
            co_z[span, :] = az
            co_c[span, :] = ac
            co_r[span, :] = acr * slope
            rprior[span, :] = rp
            jac[span, :] = same_all[span, :] * (1.0 - gz + az * rz + acr * (gr + slope * rr))

    for m in range(nh):
        landed(up_in.at[m], v_r.at[m])
        up[m * T : (m + 1) * T, :] = up_in[m].astype(F32)

    def back(i, state):
        a, b = state
        t = T - 1 - i
        f = jac[pl.ds(t, nh, stride=T), :]
        b = b + up[pl.ds(t, nh, stride=T), :]
        scan_a[t] = a
        scan_b[t] = b
        return f * a, f * b

    a, b = lax.fori_loop(0, T, back, (jnp.ones((nh, hb), F32), jnp.zeros((nh, hb), F32)), unroll=8)
    seg_out[...] = jnp.zeros(seg_out.shape, F32)
    for o in range(nr):
        first, second = slice(2 * o, 2 * o + 1), slice(2 * o + 1, 2 * o + 2)
        seg_out[0, o : o + 1, :] = a[first, :] * a[second, :]
        seg_out[1, o : o + 1, :] = b[first, :] + a[first, :] * b[second, :]
    for plane in range(nz - 1):
        send_if(plane < z, seg_out, seg_in.at[z], c_s.at[plane], c_r.at[z], at(plane, k))
    carry[...] = jnp.zeros(carry.shape, F32)
    for plane in reversed(range(1, nz)):

        @pl.when(plane > z)
        def _():
            landed(seg_in.at[plane], c_r.at[plane])
            carry[0:nr, :] = seg_in[plane, 1, 0:nr, :] + seg_in[plane, 0, 0:nr, :] * carry[0:nr, :]

    into = carry[0:nr, :]
    carry_rows = []
    for o in range(nr):
        later = into[o : o + 1, :]
        second = slice(2 * o + 1, 2 * o + 2)
        carry_rows += [b[second, :] + a[second, :] * later, later]
    carried = jnp.concatenate(carry_rows, 0)

    def finish(t, _):
        lam[pl.ds(t, nh, stride=T), :] = scan_b[t] + scan_a[t] * carried
        return 0

    lax.fori_loop(0, T, finish, 0, unroll=8)

    sums = [jnp.zeros((1, hb), F32) for _ in range(6)]
    for m in range(nh):
        span = slice(m * T, (m + 1) * T)
        prior = prior_all[span, :]
        adj = lam[span, :]
        grad_z = adj * co_z[span, :]
        grad_r = adj * co_r[span, :]
        grad_c = adj * co_c[span, :]
        grads[span, :hb] = grad_z.astype(BF16)
        grads[span, hb : 2 * hb] = grad_r.astype(BF16)
        grads[span, 2 * hb :] = grad_c.astype(BF16)
        terms = (grad_z, grad_r, grad_c, grad_z * prior, grad_r * prior, grad_c * rprior[span, :])
        sums = [total + jnp.sum(term, 0, keepdims=True) for total, term in zip(sums, terms)]
    for i in range(6):
        st_out[i : i + 1, :] = sums[i]
    st_out[6:8, :] = jnp.zeros((2, hb), F32)
    st_z[z] = st_out[...]
    for plane in range(nz):
        send_if(plane != z, st_out, st_z.at[z], t_s.at[plane], t_r.at[z], column(plane))

    def quarter(col):
        return slice(col * cw, (col + 1) * cw)

    def gate_of(step):
        g = high * step + (1 - high) * (GATES - 1 - step)
        return g, (nh * g + k) // per

    for step in range(GATES):
        g, plane = gate_of(step)
        block = lax.dot_general(
            grads[:, pl.ds(pl.multiple_of(g * hb, hb), hb)], x_all[...], (((0,), (0,)), ((), ())),
            preferred_element_type=F32,
        )
        wg_own[g] = block
        wg_out[g] = block.astype(BF16)
        outward = jnp.logical_and(inner, plane == end)
        inward = jnp.logical_and(jnp.logical_not(inner), plane != z)
        for col in range(nr):
            part = wg_out.at[g, :, quarter(col)]
            send_if(
                inward, part, wg_end.at[g, :, quarter(col)], g_s.at[step * nr + col],
                g_e.at[g * nr + col], column(high + half - 1),
            )
            send_if(
                outward, part, wg_mid.at[0, :, quarter(col)], g_s.at[step * nr + col],
                g_m.at[col], column(end),
            )

    chips = [(x + 1, y + 1), (x + 1, y), (x, y + 1), (x, y)]

    def tokens(n, core):
        return rows(grads, 2 * (2 * (chips[n][0] % nx) + core) + chips[n][1] % 2, T)[...]

    for n in range(len(chips)):
        part_out[n] = jnp.dot(tokens(n, 1 - c), w_all[...], preferred_element_type=F32).astype(BF16)
        send_if(True, part_out.at[n], part_in.at[n], d_s.at[n], d_r.at[n], partner)
    for n in range(len(chips)):
        part_keep[n] = jnp.dot(tokens(n, c), w_all[...], preferred_element_type=F32)

    first = place(2 * z + (y + c) % 2, 2 * ((x + 1 - c) % nx) + c)
    second = place(2 * z + (y + 1 - c) % 2, 2 * ((x + c) % nx) + c)

    def both(n):
        landed(part_in.at[n], d_r.at[n])
        return part_keep[n] + part_in[n].astype(F32)

    fin_out[0] = both(0).astype(BF16)
    send_if(True, fin_out.at[0], fin_in.at[0], f_s.at[0], f_r.at[0], first)
    fin_out[1] = both(1 + c).astype(BF16)
    send_if(True, fin_out.at[1], fin_in.at[1], f_s.at[1], f_r.at[1], first)

    scale = 1.0 / math.sqrt(ns * nr * T)
    for plane in range(nz):
        pl.when(plane != z)(functools.partial(landed, st_z.at[plane], t_r.at[plane]))
    total = st_z[0]
    for plane in range(1, nz):
        total = total + st_z[plane]
    st_sum[...] = total * scale
    st_all[k] = st_sum[...]
    for j in range(nh):
        send_if(j != k, st_sum, st_all.at[k], u_s.at[j], u_r.at[k], at(z, j))

    def turn():
        total = both(2 - c)
        landed(fin_in.at[0], f_r.at[0])
        fin_out[2] = (total + fin_in[0].astype(F32)).astype(BF16)
        send_if(True, fin_out.at[2], fin_in.at[2], f_s.at[2], f_r.at[2], second)

    for step in range(GATES):
        if step == 1:
            turn()
        g, plane = gate_of(step)
        passed = jnp.logical_and(inner, jnp.logical_and(plane != z, plane != end))
        far = (plane // half != high) & ((plane == 0) | (plane == nz - 1))
        for col in range(nr):
            cols = quarter(col)

            @pl.when(passed)
            def _():
                landed(wg_end.at[g, :, cols], g_e.at[g * nr + col])
                wg_out[g, :, cols] = (wg_own[g, :, cols] + wg_end[g, :, cols].astype(F32)).astype(BF16)

            for slot, there in enumerate((jnp.logical_not(far), far)):
                send_if(
                    jnp.logical_and(passed, there), wg_out.at[g, :, cols], wg_mid.at[slot, :, cols],
                    g_s.at[step * nr + col], g_m.at[slot * nr + col], column(plane),
                )

    _, g, found = origin(0)
    b = nh * g + k
    owner, i = b // GATES, b % GATES
    for col in range(nr):
        cols = quarter(col)

        @pl.when(found)
        def _():
            landed(wg_mid.at[0, :, cols], g_m.at[col])
            wg_fin[:, cols] = wg_own[g, :, cols] + wg_mid[0, :, cols].astype(F32)

        @pl.when(jnp.logical_and(found, inner))
        def _():
            landed(wg_end.at[g, :, cols], g_e.at[g * nr + col])
            wg_out[g, :, cols] = (wg_fin[:, cols] + wg_end[g, :, cols].astype(F32)).astype(BF16)

        @pl.when(jnp.logical_and(found, jnp.logical_not(inner)))
        def _():
            landed(wg_mid.at[1, :, cols], g_m.at[nr + col])
            wg_out[g, :, cols] = (wg_fin[:, cols] + wg_mid[1, :, cols].astype(F32)).astype(BF16)

        here = jnp.logical_and(owner == s, r == col)

        @pl.when(jnp.logical_and(found, here))
        def _():
            local(wg_out.at[g, :, cols], wg_in.at[i], g_r.at[i])

        send_if(
            jnp.logical_and(found, jnp.logical_not(here)), wg_out.at[g, :, cols], wg_in.at[i],
            g_f.at[col], g_r.at[i], place(owner, col),
        )

    for j in range(nh):
        pl.when(j != k)(functools.partial(landed, st_all.at[j], u_r.at[j]))
        out_p[:, j * hb : (j + 1) * hb] = st_all[j, :6, :]

    total = both(3)
    for n in (1, 2):
        landed(fin_in.at[n], f_r.at[n])
        total = total + fin_in[n].astype(F32)
    out_in[...] = total.astype(BF16)

    for i in range(GATES):
        landed(wg_in.at[i], g_r.at[i])
        out_w[i * hb : (i + 1) * hb, :] = wg_in[i].astype(F32) * scale

    for sent, src, sem in unsent:
        if sent is True:
            landed(src, sem)
        else:

            @pl.when(sent)
            def _():
                landed(src, sem)


def flush(in_a, in_b, in_c, out_a, out_b, out_c, sems):
    pairs = [(in_a, out_a), (in_b, out_b), (in_c, out_c)]
    copies = [pltpu.make_async_copy(a, b, sems.at[i]) for i, (a, b) in enumerate(pairs)]
    for copy in copies:
        copy.start()
    for copy in copies:
        copy.wait()


def by_hidden(ns, nr, inputs, weight_t, states, doc_ids, recur, bias, out_grad):
    T, DI = inputs.shape[1:]
    H = states.shape[2]
    nh, nz, nx = 2 * nr, ns // 2, nr // 2
    hb, cw = H // nh, DI // nr
    L = nh * T
    vm = pltpu.VMEM
    scratch = [
        vm(weight_t.shape, BF16),
        vm((T, H), F32),
        vm((1, T), jnp.int32),
        vm((GATES, H), F32),
        vm((GATES, H), F32),
        vm((T, H), BF16),
        vm((nh, T, hb), BF16),
        vm((nh, T, hb), BF16),
        vm((nh, T, hb), BF16),
        vm((8, T), F32),
        vm((nh, 8, T), F32),
        vm((8, H), F32),
        vm((8, H), F32),
        vm((nr, 8, hb), F32),
        vm((L, DI), BF16),
        vm((GATES * hb, DI), BF16),
        vm((L + 8 * nh, hb), F32),
        vm((L + 8 * nh, hb), F32),
        vm((L, hb), F32),
        vm((L, hb), F32),
        vm((L, hb), F32),
        vm((L, hb), F32),
        vm((L, hb), F32),
        vm((L, hb), F32),
        vm((L, hb), F32),
        vm((L, hb), F32),
        vm((T, nh, hb), F32),
        vm((T, nh, hb), F32),
        vm((nh, hb), F32),
        vm((2, 8, hb), F32),
        vm((nz, 2, 8, hb), F32),
        vm((L, hb), F32),
        vm((L, GATES * hb), BF16),
        vm((nr, T, DI), BF16),
        vm((nr, T, DI), BF16),
        vm((nr, T, DI), F32),
        vm((3, T, DI), BF16),
        vm((3, T, DI), BF16),
        vm((GATES, hb, DI), F32),
        vm((GATES, hb, DI), BF16),
        vm((GATES, hb, DI), BF16),
        vm((2, hb, DI), BF16),
        vm((hb, DI), F32),
        vm((GATES, hb, cw), BF16),
        vm((8, hb), F32),
        vm((nz, 8, hb), F32),
        vm((8, hb), F32),
        vm((nh, 8, hb), F32),
    ]
    dma = pltpu.SemaphoreType.DMA
    counts = [
        7, nr * nx, nr, nr, nh, GATES, nz * nr, GATES * nr, nh, nh, nh, nh, nh, nh, nh, nr, None, None,
        nz, nz, nr, nr, 3, 3, GATES * nr, GATES * nr, 2 * nr, nr, GATES, nz, nz, nh, nh,
    ]
    sems = [dma if n is None else dma((n,)) for n in counts]
    whole = pl.BlockSpec(memory_space=pltpu.VMEM)
    out_in, out_w, out_p = pl.pallas_call(
        functools.partial(kernel, ns, nr),
        out_shape=(
            pltpu.VMEM((T, DI), BF16),
            pltpu.VMEM(weight_t.shape, F32),
            pltpu.VMEM((6, H), F32),
        ),
        in_specs=[pl.BlockSpec(memory_space=pltpu.HBM)] * 7,
        out_specs=(whole,) * 3,
        scratch_shapes=scratch + sems,
        compiler_params=pltpu.CompilerParams(
            collective_id=0, has_side_effects=True, vmem_limit_bytes=56 * 1024 * 1024
        ),
    )(inputs[0], weight_t, states[0], doc_ids, recur, bias, out_grad[0])
    shapes = ((T, DI), BF16), (weight_t.shape, F32), ((6, H), F32)
    out_in, out_w, out_p = pl.pallas_call(
        flush,
        out_shape=tuple(jax.ShapeDtypeStruct(*one) for one in shapes),
        in_specs=[whole] * 3,
        out_specs=(pl.BlockSpec(memory_space=pltpu.HBM),) * 3,
        scratch_shapes=[dma((3,))],
    )(*(pltpu.with_memory_space_constraint(one, pltpu.VMEM) for one in (out_in, out_w, out_p)))
    return out_in[None], out_w, out_p


def fits(ns, nr, inputs, weight_t, states):
    parts, L, DI = inputs.shape
    H = states.shape[2]
    return (
        parts == nr
        and ns == 2 * nr
        and ns % 8 == 0
        and ns == 8
        and H % (ns * 128) == 0
        and DI % (nr * 128) == 0
        and L % (ns * 128) == 0
        and L * DI <= 1 << 21
    )


def solution(mesh):
    ns, nr = mesh.shape["seq"], mesh.shape["rep"]
    placed = (
        P("rep", "seq", None),
        P("seq", "rep"),
        P("rep", "seq", None),
        P("rep", "seq"),
        P(),
        P(),
        P("rep", "seq", None),
    )

    def run(inputs, weight_t, states, doc_ids, recur, bias, out_grad):
        kernelized = fits(ns, nr, inputs, weight_t, states)
        body = functools.partial(by_hidden, ns, nr) if kernelized else by_tokens
        return jax.shard_map(
            body,
            mesh=mesh,
            in_specs=placed,
            out_specs=(P("rep", "seq", None), P("seq", "rep"), P()),
            check_vma=False,
        )(inputs, weight_t, states, doc_ids, recur, bias, out_grad)

    return run
```

```python
import functools
import math

import jax
import jax.numpy as jnp
from jax import lax
from jax.experimental import pallas as pl
from jax.experimental.pallas import tpu as pltpu
from jax.sharding import PartitionSpec as P

F32 = jnp.float32
BF16 = jnp.bfloat16
GATES = 3


def shifted(block, axis, distance):
    devices = range(lax.axis_size(axis))
    route = [(i - distance, i) for i in devices if i - distance in devices]
    return lax.ppermute(block, axis, route)


def compose(earlier, later):
    return (later[0] * earlier[0], later[1] + later[0] * earlier[1])


def by_tokens(inputs, weight_t, states, doc_ids, recur, bias, out_grad):
    feats = inputs[0]
    hidden_now = states[0]
    ids_float = doc_ids[0].astype(F32)
    count = feats.shape[0]
    width = hidden_now.shape[1]
    columns = lax.all_gather(weight_t, "rep", axis=1, tiled=True)
    contract_last = (((1,), (1,)), ((), ()))
    full_weight = lax.all_gather(columns, "seq", axis=0, tiled=True)
    preact = lax.dot_general(feats, full_weight, contract_last, preferred_element_type=F32)
    tail_state, tail_id = shifted((hidden_now[-1:], ids_float[-1:]), "seq", 1)
    first_same = jnp.where(
        (ids_float[0] == tail_id[0]) & (lax.axis_index("seq") > 0), 1.0, 0.0
    ).astype(F32)
    same = jnp.concatenate([first_same[None], (ids_float[1:] == ids_float[:-1]).astype(F32)])
    prior = jnp.concatenate([tail_state, hidden_now[:-1]], 0) * same[:, None]
    gate_z = jax.nn.sigmoid(preact[:, :width] + recur[0] * prior + bias[0])
    gate_r = jax.nn.sigmoid(preact[:, width : 2 * width] + recur[1] * prior + bias[1])
    gate_c = jnp.tanh(preact[:, 2 * width :] + recur[2] * gate_r * prior + bias[2])
    jacobian = same[:, None] * (
        1.0
        - gate_z
        + (gate_c - prior) * gate_z * (1.0 - gate_z) * recur[0]
        + gate_z
        * (1.0 - gate_c * gate_c)
        * recur[2]
        * (gate_r + prior * gate_r * (1.0 - gate_r) * recur[1])
    )
    upstream = out_grad[0].astype(F32)
    jac_rows, up_rows = (
        lax.all_to_all(jacobian.T, "seq", split_axis=0, concat_axis=1, tiled=True),
        lax.all_to_all(upstream.T, "seq", split_axis=0, concat_axis=1, tiled=True),
    )
    factor = jnp.concatenate([jac_rows[:, 1:], jnp.zeros((jac_rows.shape[0], 1), F32)], 1)
    _, adjoint_rows = lax.associative_scan(compose, (factor, up_rows), reverse=True, axis=1)
    adjoint = lax.all_to_all(adjoint_rows, "seq", split_axis=1, concat_axis=0, tiled=True).T
    grad_z = adjoint * (gate_c - prior) * gate_z * (1.0 - gate_z)
    grad_c = adjoint * gate_z * (1.0 - gate_c * gate_c)
    grad_r = grad_c * recur[2] * prior * gate_r * (1.0 - gate_r)
    grad_pre = jnp.concatenate([grad_z, grad_r, grad_c], 1).astype(BF16)
    input_grad = jnp.dot(grad_pre, full_weight, preferred_element_type=F32)
    tokens_all = count * inputs.shape[0] * lax.axis_size("seq") * lax.axis_size("rep")
    normal_factor = 1.0 / math.sqrt(tokens_all)
    row_share = lax.psum_scatter(
        lax.dot_general(grad_pre, feats, (((0,), (0,)), ((), ())), preferred_element_type=F32),
        "seq",
        scatter_dimension=0,
        tiled=True,
    )
    weight_grad = (
        lax.psum_scatter(row_share.astype(BF16), "rep", scatter_dimension=1, tiled=True).astype(F32)
        * normal_factor
    )
    stats = jnp.stack(
        [
            grad_z.sum(0),
            grad_r.sum(0),
            grad_c.sum(0),
            (grad_z * prior).sum(0),
            (grad_r * prior).sum(0),
            (grad_c * gate_r * prior).sum(0),
        ]
    )
    param_grad = lax.psum(stats, ("seq", "rep")) * normal_factor
    return (input_grad.astype(BF16)[None], weight_grad, param_grad)


def kernel(
    ns, nr, feats_hbm, weight_hbm, states_hbm, ids_hbm, recur_hbm, bias_hbm, upstream_hbm,
    out_in, out_w, out_p,
    weight, states, ids, recur, bias, upstream,
    pay_src, pay, up_in, tail_src, tail_mid, tail_in, x_all, w_all, prev, ids_col, same_all, up,
    pre, jac, co_z, co_r, co_c, rprior, prior_all,
    scan_a, scan_b, carry, seg_out, seg_in, lam, grads, part_out, part_in, part_keep, fin_out, fin_in,
    wg_own, wg_out, wg_end, wg_mid, wg_fin, wg_in, st_out, st_z, st_sum, st_all,
    l_s, x_s, x_r, w_s, w_f, w_r, p_s, p_r, v_s, v_r, e_s, e_r, n_s, n_r, c_s, c_r,
    d_s, d_r, f_s, f_r, g_s, g_e, g_m, g_f, g_r, t_s, t_r, u_s, u_r,
):
    T, DI = feats_hbm.shape
    H = states.shape[1]
    nh, nz, nx = 2 * nr, ns // 2, nr // 2
    hb, cw = H // nh, DI // nr
    s, r = lax.axis_index("seq"), lax.axis_index("rep")
    z, y, x, c = s // 2, s % 2, r // 2, r % 2
    q = 2 * r + y
    k = nx * 2 * c + 2 * x + y
    half, per = nz // 2, GATES * nh // nz
    high = z // half
    inner = jnp.logical_or(z == half - 1, z == half)
    end = high * (nz - 1)
    unsent = []

    def place(a, b):
        return {"seq": a, "rep": b}

    def at(plane, j):
        return place(2 * plane + j % 2, 2 * (j // 2 % nx) + j // (2 * nx))

    def column(plane):
        return place(2 * plane + y, r)

    def send(src, dst, ssem, rsem, where):
        pltpu.make_async_remote_copy(
            src_ref=src, dst_ref=dst, send_sem=ssem, recv_sem=rsem,
            device_id=where, device_id_type=pl.DeviceIdType.MESH,
        ).start()

    def local(src, dst, rsem):
        pltpu.make_async_copy(src, dst, rsem).start()

    def landed(dst, sem):
        pltpu.make_async_copy(dst, dst, sem).wait()

    def send_if(allowed, *args):
        pl.when(allowed)(functools.partial(send, *args))

    def send_or_local(src, dst, ssem, rsem, where, here):
        send_if(jnp.logical_not(here), src, dst, ssem, rsem, where)
        pl.when(here)(functools.partial(local, src, dst, rsem))

    def rows(ref, block, count):
        return ref.at[pl.ds(pl.multiple_of(block * count, count), count), :]

    barrier = pltpu.get_barrier_semaphore()

    def greet(where):
        pl.semaphore_signal(barrier, inc=1, device_id=where, device_id_type=pl.DeviceIdType.MESH)

    for j in range(nh):
        pl.when(j != k)(functools.partial(greet, at(z, j)))
    for plane in range(nz):
        pl.when(plane != z)(functools.partial(greet, column(plane)))
    loads = [
        (weight_hbm, weight), (feats_hbm, rows(x_all, q, T)), (states_hbm, states), (ids_hbm, ids),
        (upstream_hbm, upstream), (recur_hbm, recur), (bias_hbm, bias),
    ]
    for n, (src, dst) in enumerate(loads):
        local(src, dst, l_s.at[n])

    def loaded(n):
        landed(loads[n][1], l_s.at[n])

    def piece(g, col):
        return w_all.at[pl.ds(pl.multiple_of(g * hb, hb), hb), col]

    loaded(0)
    pl.semaphore_wait(barrier, nh - 1 + nz - 1)

    mine = pl.ds(pl.multiple_of(r * cw, cw), cw)
    for i in range(GATES):
        b = GATES * s + i
        g, j = b // nh, b % nh
        part = weight.at[i * hb : (i + 1) * hb, :]
        send_or_local(part, piece(g, mine), w_s.at[i], w_r.at[g * nr + r], at(z, j), j == k)
        unsent.append((j != k, part, w_s.at[i]))

    partner = place(s, r + 1 - 2 * c)
    nearest = place(2 * z + (y + c) % 2, 2 * ((x + 1 - c) % nx) + c)
    across = place(2 * z + (y + 1 - c) % 2, 2 * ((x + c) % nx) + c)

    def features(dx, dy, core):
        return 2 * (2 * ((x + dx) % nx) + (c + core) % 2) + (y + dy) % 2

    def share(dx, dy, targets):
        slot = features(dx, dy, 0)
        block = rows(x_all, slot, T)
        for where in targets:
            send(block, block, x_s, x_r.at[slot], where)

    loaded(1)
    share(0, 0, (nearest, across, partner))
    unsent.append((True, x_all.at[0 : (nh - 1) * T, :], x_s))

    loaded(2)
    loaded(3)
    tail_src[0:4, :] = jnp.broadcast_to(states[T - 1 : T, :], (4, H))
    tail_src[4:8, :] = jnp.broadcast_to(ids[0:1, T - 1 : T].astype(F32), (4, H))
    hands_on = jnp.logical_and(y == 1, z < nz - 1)
    takes_over = jnp.logical_and(y == 1, z > 0)
    send_if(hands_on, tail_src, tail_mid, n_s, n_r, column((z + 1) % nz))
    unsent.append((hands_on, tail_src, n_s))
    for j in range(nh):
        pay_src[j, 0:T, :] = states[:, j * hb : (j + 1) * hb].astype(BF16)
        pay_src[j, T:, :] = jnp.broadcast_to(ids[...].astype(F32), (16, hb)).astype(BF16)
    for j in range(nh):
        send_or_local(pay_src.at[j], pay.at[q], p_s, p_r, at(z, j), k == j)
    unsent.append((True, pay.at[0 : nh - 1], p_s))

    def origin(step):
        plane = (z + (1 - 2 * high) * step + nz) % nz
        g = (per * plane - k + nh - 1) // nh
        return plane, g % GATES, jnp.logical_and(g < GATES, nh * g + k < per * (plane + 1))

    order = []
    for n in range(nr):
        chip = (x + n // 2) % nx
        order.append(2 * chip + (c + n) % 2)

    def spread(step, numbers):
        plane, g, found = origin(step)
        outer = jnp.logical_and(found, jnp.logical_not(inner))
        within = jnp.logical_and(found, inner)
        far, near = column(half - high), column(z + 1 - 2 * (z % half))
        for n in numbers:
            block = piece(g, pl.ds(pl.multiple_of(order[n] * cw, cw), cw))
            sem = w_r.at[g * nr + order[n]]
            if step == 0:
                pl.when(found)(functools.partial(landed, block, sem))
                send_if(found, block, block, w_f.at[0], sem, far)
                send_if(within, block, block, w_f.at[0], sem, near)
            else:
                pl.when(within)(functools.partial(landed, block, sem))
                send_if(within, block, block, w_f.at[step], sem, column(end))
        if step == 0:
            for n in numbers:
                block = piece(g, pl.ds(pl.multiple_of(order[n] * cw, cw), cw))
                send_if(outer, block, block, w_f.at[0], w_r.at[g * nr + order[n]], near)
            unsent.append((found, w_all.at[0 : 2 * hb, :], w_f.at[0]))
        elif numbers[-1] == nr - 1:
            unsent.append((within, w_all.at[0:hb, :], w_f.at[step]))

    def relay(dx, dy, targets):
        slot = features(dx, dy, 0)
        landed(rows(x_all, slot, T), x_r.at[slot])
        share(dx, dy, targets)

    spread(0, range(nr))
    pl.when(takes_over)(functools.partial(landed, tail_mid, n_r))
    for j in range(nh):
        part = tail_mid.at[:, j * hb : (j + 1) * hb]
        here = j == k
        send_if(jnp.logical_and(takes_over, j != k), part, tail_in.at[r], e_s, e_r, at(z, j))
        pl.when(jnp.logical_and(takes_over, here))(functools.partial(local, part, tail_in.at[r], e_r))
    unsent.append((takes_over, st_all.at[0 : nh - 1], e_s))
    spread(1, range(nr // 2))
    relay(c, 1 - c, (nearest, partner))
    spread(1, range(nr // 2, nr))
    relay(1 - c, c, (partner,))
    loaded(4)
    for j in range(nh):
        part = upstream.at[:, j * hb : (j + 1) * hb]
        send_or_local(part, up_in.at[q], v_s, v_r, at(z, j), k == j)
    unsent.append((True, up_in.at[0 : nh - 1], v_s))
    spread(2, range(nr))

    stride = T + 8
    landed(pay, p_r)
    pl.when(z > 0)(functools.partial(landed, tail_in, e_r))
    for m in range(nh):
        base = m * stride + 8
        span = slice(m * T, (m + 1) * T)
        prev[base : base + T, :] = pay[m, 0:T, :].astype(F32)
        ids_row = pay[m, T:, :].astype(F32)[0:1, :]
        ids_col[base : base + T, :] = jnp.broadcast_to(ids_row, (hb, T)).T
        if m % 2:
            before = base - stride + T - 1
            prev[base - 1 : base, :] = prev[before : before + 1, :]
            ids_col[base - 1 : base, :] = ids_col[before : before + 1, :]
        else:

            @pl.when(z > 0)
            def _():
                prev[base - 1 : base, :] = tail_in[m // 2, 0:1, :]
                ids_col[base - 1 : base, :] = tail_in[m // 2, 4:5, :]

            @pl.when(z == 0)
            def _():
                prev[base - 1 : base, :] = jnp.zeros((1, hb), F32)
                ids_col[base - 1 : base, :] = jnp.full((1, hb), -1.0, F32)

        same = jnp.where(
            ids_col[base : base + T, :] == ids_col[base - 1 : base - 1 + T, :], 1.0, 0.0
        )
        same_all[span, :] = same
        prior_all[span, :] = prev[base - 1 : base - 1 + T, :] * same

    loaded(5)
    loaded(6)
    (_, g0, found0), (_, g1, _), (_, g2, _), (_, g3, found3) = (origin(step) for step in range(nz))
    own, wide = found0.astype(jnp.int32), found3.astype(jnp.int32)
    early = own * g0 + (1 - own) * g1
    late = wide * g3 + (1 - wide) * g2
    middle = (GATES - early - late) % GATES
    outer = jnp.logical_not(inner)

    def arrived(g, unseen):
        for col in range(nr):
            block = piece(g, slice(col * cw, (col + 1) * cw))
            pl.when(unseen)(functools.partial(landed, block, w_r.at[g * nr + col]))

    def project(span, g):
        return lax.dot_general(
            x_all[span, :], piece(g, slice(None))[...], (((1,), (1,)), ((), ())),
            preferred_element_type=F32,
        )

    def ahead(blocks):
        for m in blocks:
            span = pl.ds(pl.multiple_of(m * T, T), T)
            for g in (early, middle):
                pre[g, span, :] = project(span, g)

    hops = [(0, 0), (0, 1), (1, 0), (1, 1)]
    for dx, dy in hops[:3]:
        m = features(dx, dy, 1)
        landed(rows(x_all, m, T), x_r.at[m])
    arrived(early, jnp.logical_and(jnp.logical_not(found0), outer))
    arrived(middle, outer)
    ahead([features(dx, dy, core) for dx, dy in hops[:3] for core in range(2)])
    relay(1, 1, (partner,))
    m = features(1, 1, 1)
    landed(rows(x_all, m, T), x_r.at[m])
    ahead([features(1, 1, core) for core in range(2)])
    arrived(late, jnp.logical_or(found3, outer))

    group = pl.ds(pl.multiple_of(k * hb, hb), hb)
    rz, rr, rc = (recur[i : i + 1, group] for i in range(GATES))
    bz, br, bc = (bias[i : i + 1, group] for i in range(GATES))
    for m in range(nh):
        span = slice(m * T, (m + 1) * T)
        last = project(span, late)
        pz, pr, pc = (jnp.where(late == i, last, pre[i, span, :]) for i in range(GATES))
        prior = prior_all[span, :]
        gz = jax.nn.sigmoid(pz + rz * prior + bz)
        gr = jax.nn.sigmoid(pr + rr * prior + br)
        rp = gr * prior
        gc = jnp.tanh(pc + rc * rp + bc)
        az = (gc - prior) * gz * (1.0 - gz)
        ac = gz * (1.0 - gc * gc)
        slope = rp * (1.0 - gr)
        acr = ac * rc
        co_z[span, :] = az
        co_c[span, :] = ac
        co_r[span, :] = acr * slope
        rprior[span, :] = rp
        jac[m * stride : m * stride + T, :] = same_all[span, :] * (
            1.0 - gz + az * rz + acr * (gr + slope * rr)
        )

    landed(up_in, v_r)
    for m in range(nh):
        up[m * stride : m * stride + T, :] = up_in[m].astype(F32)

    def back(i, state):
        a, b = state
        t = T - 1 - i
        f = jac[pl.ds(t, nh, stride=stride), :]
        b = b + up[pl.ds(t, nh, stride=stride), :]
        scan_a[t] = a
        scan_b[t] = b
        return f * a, f * b

    a, b = lax.fori_loop(0, T, back, (jnp.ones((nh, hb), F32), jnp.zeros((nh, hb), F32)), unroll=8)
    seg_out[...] = jnp.zeros(seg_out.shape, F32)
    for o in range(nr):
        first, second = slice(2 * o, 2 * o + 1), slice(2 * o + 1, 2 * o + 2)
        seg_out[0, o : o + 1, :] = a[first, :] * a[second, :]
        seg_out[1, o : o + 1, :] = b[first, :] + a[first, :] * b[second, :]
    for plane in range(nz - 1):
        send_if(plane < z, seg_out, seg_in.at[z], c_s, c_r.at[z], at(plane, k))
        unsent.append((z == plane + 1, seg_in.at[0 : plane + 1], c_s))
    carry[...] = jnp.zeros(carry.shape, F32)
    for plane in reversed(range(1, nz)):

        @pl.when(plane > z)
        def _():
            landed(seg_in.at[plane], c_r.at[plane])
            carry[0:nr, :] = seg_in[plane, 1, 0:nr, :] + seg_in[plane, 0, 0:nr, :] * carry[0:nr, :]

    into = carry[0:nr, :]
    carry_rows = []
    for o in range(nr):
        later = into[o : o + 1, :]
        second = slice(2 * o + 1, 2 * o + 2)
        carry_rows += [b[second, :] + a[second, :] * later, later]
    carried = jnp.concatenate(carry_rows, 0)

    def finish(t, _):
        lam[pl.ds(t, nh, stride=stride), :] = scan_b[t] + scan_a[t] * carried
        return 0

    lax.fori_loop(0, T, finish, 0, unroll=8)

    sums = [jnp.zeros((1, hb), F32) for _ in range(6)]
    for m in range(nh):
        span = slice(m * T, (m + 1) * T)
        prior = prior_all[span, :]
        adj = lam[m * stride : m * stride + T, :]
        grad_z = adj * co_z[span, :]
        grad_r = adj * co_r[span, :]
        grad_c = adj * co_c[span, :]
        grads[span, :hb] = grad_z.astype(BF16)
        grads[span, hb : 2 * hb] = grad_r.astype(BF16)
        grads[span, 2 * hb :] = grad_c.astype(BF16)
        terms = (grad_z, grad_r, grad_c, grad_z * prior, grad_r * prior, grad_c * rprior[span, :])
        sums = [total + jnp.sum(term, 0, keepdims=True) for total, term in zip(sums, terms)]
    for i in range(6):
        st_out[i : i + 1, :] = sums[i]
    st_out[6:8, :] = jnp.zeros((2, hb), F32)
    st_z[z] = st_out[...]
    for plane in range(nz):
        send_if(plane != z, st_out, st_z.at[z], t_s, t_r, column(plane))
    unsent.append((True, st_z.at[0 : nz - 1], t_s))

    def quarter(col):
        return slice(col * cw, (col + 1) * cw)

    def gate_of(step):
        g = high * step + (1 - high) * (GATES - 1 - step)
        return g, (nh * g + k) // per

    for step in range(GATES):
        g, plane = gate_of(step)
        block = lax.dot_general(
            grads[:, pl.ds(pl.multiple_of(g * hb, hb), hb)], x_all[...], (((0,), (0,)), ((), ())),
            preferred_element_type=F32,
        )
        wg_own[g] = block
        wg_out[g] = block.astype(BF16)
        outward = jnp.logical_and(inner, plane == end)
        inward = jnp.logical_and(jnp.logical_not(inner), plane != z)
        for col in range(nr):
            part = wg_out.at[g, :, quarter(col)]
            send_if(
                inward, part, wg_end.at[g, :, quarter(col)], g_s.at[step],
                g_e.at[g * nr + col], column(high + half - 1),
            )
            send_if(
                outward, part, wg_mid.at[0, :, quarter(col)], g_s.at[step], g_m.at[col], column(end),
            )
        unsent.append((plane != z, wg_out.at[step], g_s.at[step]))

    chips = [(x + 1, y + 1), (x + 1, y), (x, y + 1), (x, y)]

    def tokens(n, core):
        return rows(grads, 2 * (2 * (chips[n][0] % nx) + core) + chips[n][1] % 2, T)[...]

    for n in range(len(chips)):
        part_out[n] = jnp.dot(tokens(n, 1 - c), w_all[...], preferred_element_type=F32).astype(BF16)
        send(part_out.at[n], part_in.at[n], d_s, d_r, partner)
    for n in range(len(chips)):
        part_keep[n] = jnp.dot(tokens(n, c), w_all[...], preferred_element_type=F32)

    unsent.append((True, part_out, d_s))
    unsent.append((True, fin_out, f_s))

    def both(n):
        return part_keep[n] + part_in[n].astype(F32)

    landed(part_in, d_r)
    fin_out[0] = both(0).astype(BF16)
    send(fin_out.at[0], fin_in.at[0], f_s, f_r.at[0], nearest)
    fin_out[1] = both(1 + c).astype(BF16)
    send(fin_out.at[1], fin_in.at[1], f_s, f_r.at[1], nearest)

    scale = 1.0 / math.sqrt(ns * nr * T)
    landed(st_z.at[0 : nz - 1], t_r)
    total = st_z[0]
    for plane in range(1, nz):
        total = total + st_z[plane]
    st_sum[...] = total * scale
    st_all[k] = st_sum[...]
    for j in range(nh):
        send_if(j != k, st_sum, st_all.at[k], u_s, u_r, at(z, j))
    unsent.append((True, st_all.at[0 : nh - 1], u_s))

    def turn():
        total = both(2 - c)
        landed(fin_in.at[0], f_r.at[0])
        fin_out[2] = (total + fin_in[0].astype(F32)).astype(BF16)
        send(fin_out.at[2], fin_in.at[2], f_s, f_r.at[2], across)

    for step in range(GATES):
        if step == 1:
            turn()
        g, plane = gate_of(step)
        passed = jnp.logical_and(inner, jnp.logical_and(plane != z, plane != end))
        far = (plane // half != high) & ((plane == 0) | (plane == nz - 1))
        for col in range(nr):
            cols = quarter(col)

            @pl.when(passed)
            def _():
                landed(wg_end.at[g, :, cols], g_e.at[g * nr + col])
                wg_out[g, :, cols] = (wg_own[g, :, cols] + wg_end[g, :, cols].astype(F32)).astype(BF16)

            for slot, there in enumerate((jnp.logical_not(far), far)):
                send_if(
                    jnp.logical_and(passed, there), wg_out.at[g, :, cols], wg_mid.at[slot, :, cols],
                    g_s.at[step], g_m.at[slot * nr + col], column(plane),
                )

    _, g, found = origin(0)
    b = nh * g + k
    owner, i = b // GATES, b % GATES
    for col in range(nr):
        cols = quarter(col)

        @pl.when(found)
        def _():
            landed(wg_mid.at[0, :, cols], g_m.at[col])
            wg_fin[:, cols] = wg_own[g, :, cols] + wg_mid[0, :, cols].astype(F32)

        @pl.when(jnp.logical_and(found, inner))
        def _():
            landed(wg_end.at[g, :, cols], g_e.at[g * nr + col])
            wg_out[g, :, cols] = (wg_fin[:, cols] + wg_end[g, :, cols].astype(F32)).astype(BF16)

        @pl.when(jnp.logical_and(found, jnp.logical_not(inner)))
        def _():
            landed(wg_mid.at[1, :, cols], g_m.at[nr + col])
            wg_out[g, :, cols] = (wg_fin[:, cols] + wg_mid[1, :, cols].astype(F32)).astype(BF16)

        here = jnp.logical_and(owner == s, r == col)

        @pl.when(jnp.logical_and(found, here))
        def _():
            local(wg_out.at[g, :, cols], wg_in.at[i], g_r.at[i])

        send_if(
            jnp.logical_and(found, jnp.logical_not(here)), wg_out.at[g, :, cols], wg_in.at[i],
            g_f, g_r.at[i], place(owner, col),
        )
    unsent.append((jnp.logical_and(found, owner != s), wg_out.at[0], g_f))
    unsent.append((jnp.logical_and(found, owner == s), wg_out.at[0, :, 0 : (nr - 1) * cw], g_f))

    landed(st_all.at[0 : nh - 1], u_r)
    for j in range(nh):
        out_p[:, j * hb : (j + 1) * hb] = st_all[j, :6, :]

    total = both(3)
    for n in (1, 2):
        landed(fin_in.at[n], f_r.at[n])
        total = total + fin_in[n].astype(F32)
    out_in[...] = total.astype(BF16)

    for i in range(GATES):
        landed(wg_in.at[i], g_r.at[i])
        out_w[i * hb : (i + 1) * hb, :] = wg_in[i].astype(F32) * scale

    for sent, src, sem in unsent:
        if sent is True:
            landed(src, sem)
        else:

            @pl.when(sent)
            def _():
                landed(src, sem)


def flush(in_a, in_b, in_c, out_a, out_b, out_c, sems):
    pairs = [(in_a, out_a), (in_b, out_b), (in_c, out_c)]
    copies = [pltpu.make_async_copy(a, b, sems.at[i]) for i, (a, b) in enumerate(pairs)]
    for copy in copies:
        copy.start()
    for copy in copies:
        copy.wait()


def by_hidden(ns, nr, inputs, weight_t, states, doc_ids, recur, bias, out_grad):
    T, DI = inputs.shape[1:]
    H = states.shape[2]
    nh, nz, nx = 2 * nr, ns // 2, nr // 2
    hb, cw = H // nh, DI // nr
    L = nh * T
    vm = pltpu.VMEM
    scratch = [
        vm(weight_t.shape, BF16),
        vm((T, H), F32),
        vm((1, T), jnp.int32),
        vm((GATES, H), F32),
        vm((GATES, H), F32),
        vm((T, H), BF16),
        vm((nh, T + 16, hb), BF16),
        vm((nh, T + 16, hb), BF16),
        vm((nh, T, hb), BF16),
        vm((8, H), F32),
        vm((8, H), F32),
        vm((nr, 8, hb), F32),
        vm((L, DI), BF16),
        vm((GATES * hb, DI), BF16),
        vm((L + 8 * nh, hb), F32),
        vm((L + 8 * nh, hb), F32),
        vm((L, hb), F32),
        vm((L + 8 * nh, hb), F32),
        vm((GATES, L, hb), F32),
        vm((L + 8 * nh, hb), F32),
        vm((L, hb), F32),
        vm((L, hb), F32),
        vm((L, hb), F32),
        vm((L, hb), F32),
        vm((L, hb), F32),
        vm((T, nh, hb), F32),
        vm((T, nh, hb), F32),
        vm((nh, hb), F32),
        vm((2, 8, hb), F32),
        vm((nz, 2, 8, hb), F32),
        vm((L + 8 * nh, hb), F32),
        vm((L, GATES * hb), BF16),
        vm((nr, T, DI), BF16),
        vm((nr, T, DI), BF16),
        vm((nr, T, DI), F32),
        vm((3, T, DI), BF16),
        vm((3, T, DI), BF16),
        vm((GATES, hb, DI), F32),
        vm((GATES, hb, DI), BF16),
        vm((GATES, hb, DI), BF16),
        vm((2, hb, DI), BF16),
        vm((hb, DI), F32),
        vm((GATES, hb, cw), BF16),
        vm((8, hb), F32),
        vm((nz, 8, hb), F32),
        vm((8, hb), F32),
        vm((nh, 8, hb), F32),
    ]
    dma = pltpu.SemaphoreType.DMA
    counts = [
        7, None, nh, GATES, nz - 1, GATES * nr, None, None, None, None, None, None, None, None, None, nz,
        None, None, None, 3, GATES, GATES * nr, 2 * nr, None, GATES, None, None, None, None,
    ]
    sems = [dma if n is None else dma((n,)) for n in counts]
    whole = pl.BlockSpec(memory_space=pltpu.VMEM)
    out_in, out_w, out_p = pl.pallas_call(
        functools.partial(kernel, ns, nr),
        out_shape=(
            pltpu.VMEM((T, DI), BF16),
            pltpu.VMEM(weight_t.shape, F32),
            pltpu.VMEM((6, H), F32),
        ),
        in_specs=[pl.BlockSpec(memory_space=pltpu.HBM)] * 7,
        out_specs=(whole,) * 3,
        scratch_shapes=scratch + sems,
        compiler_params=pltpu.CompilerParams(
            collective_id=0, has_side_effects=True, vmem_limit_bytes=56 * 1024 * 1024
        ),
    )(inputs[0], weight_t, states[0], doc_ids, recur, bias, out_grad[0])
    shapes = ((T, DI), BF16), (weight_t.shape, F32), ((6, H), F32)
    out_in, out_w, out_p = pl.pallas_call(
        flush,
        out_shape=tuple(jax.ShapeDtypeStruct(*one) for one in shapes),
        in_specs=[whole] * 3,
        out_specs=(pl.BlockSpec(memory_space=pltpu.HBM),) * 3,
        scratch_shapes=[dma((3,))],
    )(*(pltpu.with_memory_space_constraint(one, pltpu.VMEM) for one in (out_in, out_w, out_p)))
    return out_in[None], out_w, out_p


def fits(ns, nr, inputs, weight_t, states):
    parts, L, DI = inputs.shape
    H = states.shape[2]
    return (
        parts == nr
        and ns == 2 * nr
        and ns % 8 == 0
        and ns == 8
        and L * 2 * nr == H * ns
        and H % (ns * 128) == 0
        and DI % (nr * 128) == 0
        and L % (ns * 128) == 0
        and L * DI <= 1 << 21
    )


def solution(mesh):
    ns, nr = mesh.shape["seq"], mesh.shape["rep"]
    placed = (
        P("rep", "seq", None),
        P("seq", "rep"),
        P("rep", "seq", None),
        P("rep", "seq"),
        P(),
        P(),
        P("rep", "seq", None),
    )

    def run(inputs, weight_t, states, doc_ids, recur, bias, out_grad):
        kernelized = fits(ns, nr, inputs, weight_t, states)
        body = functools.partial(by_hidden, ns, nr) if kernelized else by_tokens
        return jax.shard_map(
            body,
            mesh=mesh,
            in_specs=placed,
            out_specs=(P("rep", "seq", None), P("seq", "rep"), P()),
            check_vma=False,
        )(inputs, weight_t, states, doc_ids, recur, bias, out_grad)

    return run
```

```python
import functools
import math

import jax
import jax.numpy as jnp
from jax import lax
from jax.experimental import pallas as pl
from jax.experimental.pallas import tpu as pltpu
from jax.sharding import PartitionSpec as P

F32 = jnp.float32
BF16 = jnp.bfloat16
GATES = 3


def shifted(block, axis, distance):
    devices = range(lax.axis_size(axis))
    route = [(i - distance, i) for i in devices if i - distance in devices]
    return lax.ppermute(block, axis, route)


def compose(earlier, later):
    return (later[0] * earlier[0], later[1] + later[0] * earlier[1])


def by_tokens(inputs, weight_t, states, doc_ids, recur, bias, out_grad):
    feats = inputs[0]
    hidden_now = states[0]
    ids_float = doc_ids[0].astype(F32)
    count = feats.shape[0]
    width = hidden_now.shape[1]
    columns = lax.all_gather(weight_t, "rep", axis=1, tiled=True)
    contract_last = (((1,), (1,)), ((), ()))
    full_weight = lax.all_gather(columns, "seq", axis=0, tiled=True)
    preact = lax.dot_general(feats, full_weight, contract_last, preferred_element_type=F32)
    tail_state, tail_id = shifted((hidden_now[-1:], ids_float[-1:]), "seq", 1)
    first_same = jnp.where(
        (ids_float[0] == tail_id[0]) & (lax.axis_index("seq") > 0), 1.0, 0.0
    ).astype(F32)
    same = jnp.concatenate([first_same[None], (ids_float[1:] == ids_float[:-1]).astype(F32)])
    prior = jnp.concatenate([tail_state, hidden_now[:-1]], 0) * same[:, None]
    gate_z = jax.nn.sigmoid(preact[:, :width] + recur[0] * prior + bias[0])
    gate_r = jax.nn.sigmoid(preact[:, width : 2 * width] + recur[1] * prior + bias[1])
    gate_c = jnp.tanh(preact[:, 2 * width :] + recur[2] * gate_r * prior + bias[2])
    jacobian = same[:, None] * (
        1.0
        - gate_z
        + (gate_c - prior) * gate_z * (1.0 - gate_z) * recur[0]
        + gate_z
        * (1.0 - gate_c * gate_c)
        * recur[2]
        * (gate_r + prior * gate_r * (1.0 - gate_r) * recur[1])
    )
    upstream = out_grad[0].astype(F32)
    jac_rows, up_rows = (
        lax.all_to_all(jacobian.T, "seq", split_axis=0, concat_axis=1, tiled=True),
        lax.all_to_all(upstream.T, "seq", split_axis=0, concat_axis=1, tiled=True),
    )
    factor = jnp.concatenate([jac_rows[:, 1:], jnp.zeros((jac_rows.shape[0], 1), F32)], 1)
    _, adjoint_rows = lax.associative_scan(compose, (factor, up_rows), reverse=True, axis=1)
    adjoint = lax.all_to_all(adjoint_rows, "seq", split_axis=1, concat_axis=0, tiled=True).T
    grad_z = adjoint * (gate_c - prior) * gate_z * (1.0 - gate_z)
    grad_c = adjoint * gate_z * (1.0 - gate_c * gate_c)
    grad_r = grad_c * recur[2] * prior * gate_r * (1.0 - gate_r)
    grad_pre = jnp.concatenate([grad_z, grad_r, grad_c], 1).astype(BF16)
    input_grad = jnp.dot(grad_pre, full_weight, preferred_element_type=F32)
    tokens_all = count * inputs.shape[0] * lax.axis_size("seq") * lax.axis_size("rep")
    normal_factor = 1.0 / math.sqrt(tokens_all)
    row_share = lax.psum_scatter(
        lax.dot_general(grad_pre, feats, (((0,), (0,)), ((), ())), preferred_element_type=F32),
        "seq",
        scatter_dimension=0,
        tiled=True,
    )
    weight_grad = (
        lax.psum_scatter(row_share.astype(BF16), "rep", scatter_dimension=1, tiled=True).astype(F32)
        * normal_factor
    )
    stats = jnp.stack(
        [
            grad_z.sum(0),
            grad_r.sum(0),
            grad_c.sum(0),
            (grad_z * prior).sum(0),
            (grad_r * prior).sum(0),
            (grad_c * gate_r * prior).sum(0),
        ]
    )
    param_grad = lax.psum(stats, ("seq", "rep")) * normal_factor
    return (input_grad.astype(BF16)[None], weight_grad, param_grad)


def kernel(
    ns, nr, feats_hbm, weight_hbm, states_hbm, ids_hbm, recur_hbm, bias_hbm, upstream_hbm,
    out_in, out_w, out_p,
    weight, states, ids, recur, bias, upstream,
    pay_src, pay, up_in, tail_src, tail_mid, tail_in, x_all, w_all, prev, ids_col, same_all, up,
    pre, jac, co_z, co_r, co_c, rprior, prior_all,
    scan_a, scan_b, carry, seg_out, seg_in, lam, grads, wg_via, part_out, part_in, part_keep, fin_out, fin_in,
    wg_own, wg_out, wg_end, wg_mid, wg_fin, wg_in, st_out, st_z, st_sum, st_all,
    l_s, x_s, x_r, w_s, w_f, w_r, p_s, p_r, v_s, v_r, e_s, e_r, n_s, n_r, c_s, c_r,
    d_s, d_r, f_s, f_r, g_s, g_e, g_m, g_f, g_r, t_s, t_r, u_s, u_r, h_s, h_r,
):
    T, DI = feats_hbm.shape
    H = states.shape[1]
    nh, nz, nx = 2 * nr, ns // 2, nr // 2
    hb, cw = H // nh, DI // nr
    s, r = lax.axis_index("seq"), lax.axis_index("rep")
    z, y, x, c = s // 2, s % 2, r // 2, r % 2
    q = 2 * r + y
    k = nx * 2 * c + 2 * x + y
    half, per = nz // 2, GATES * nh // nz
    high = z // half
    inner = jnp.logical_or(z == half - 1, z == half)
    end = high * (nz - 1)
    unsent = []

    def place(a, b):
        return {"seq": a, "rep": b}

    def at(plane, j):
        return place(2 * plane + j % 2, 2 * (j // 2 % nx) + j // (2 * nx))

    def column(plane):
        return place(2 * plane + y, r)

    def send(src, dst, ssem, rsem, where):
        pltpu.make_async_remote_copy(
            src_ref=src, dst_ref=dst, send_sem=ssem, recv_sem=rsem,
            device_id=where, device_id_type=pl.DeviceIdType.MESH,
        ).start()

    def local(src, dst, rsem):
        pltpu.make_async_copy(src, dst, rsem).start()

    def landed(dst, sem):
        pltpu.make_async_copy(dst, dst, sem).wait()

    def send_if(allowed, *args):
        pl.when(allowed)(functools.partial(send, *args))

    def send_or_local(src, dst, ssem, rsem, where, here):
        send_if(jnp.logical_not(here), src, dst, ssem, rsem, where)
        pl.when(here)(functools.partial(local, src, dst, rsem))

    def rows(ref, block, count):
        return ref.at[pl.ds(pl.multiple_of(block * count, count), count), :]

    barrier = pltpu.get_barrier_semaphore()

    def greet(where):
        pl.semaphore_signal(barrier, inc=1, device_id=where, device_id_type=pl.DeviceIdType.MESH)

    for j in range(nh):
        pl.when(j != k)(functools.partial(greet, at(z, j)))
    for plane in range(nz):
        pl.when(plane != z)(functools.partial(greet, column(plane)))
    loads = [
        (weight_hbm, weight), (feats_hbm, rows(x_all, q, T)), (states_hbm, states), (ids_hbm, ids),
        (upstream_hbm, upstream), (recur_hbm, recur), (bias_hbm, bias),
    ]
    for n, (src, dst) in enumerate(loads):
        local(src, dst, l_s.at[n])

    def loaded(n):
        landed(loads[n][1], l_s.at[n])

    def piece(g, col):
        return w_all.at[pl.ds(pl.multiple_of(g * hb, hb), hb), col]

    loaded(0)
    pl.semaphore_wait(barrier, nh - 1 + nz - 1)

    mine = pl.ds(pl.multiple_of(r * cw, cw), cw)
    for i in range(GATES):
        b = GATES * s + i
        g, j = b // nh, b % nh
        part = weight.at[i * hb : (i + 1) * hb, :]
        send_or_local(part, piece(g, mine), w_s.at[i], w_r.at[g * nr + r], at(z, j), j == k)
        unsent.append((j != k, part, w_s.at[i]))

    partner = place(s, r + 1 - 2 * c)
    nearest = place(2 * z + (y + c) % 2, 2 * ((x + 1 - c) % nx) + c)
    across = place(2 * z + (y + 1 - c) % 2, 2 * ((x + c) % nx) + c)

    def features(dx, dy, core):
        return 2 * (2 * ((x + dx) % nx) + (c + core) % 2) + (y + dy) % 2

    def share(dx, dy, targets):
        slot = features(dx, dy, 0)
        block = rows(x_all, slot, T)
        for where in targets:
            send(block, block, x_s, x_r.at[slot], where)

    loaded(1)
    share(0, 0, (nearest, across, partner))
    unsent.append((True, x_all.at[0 : (nh - 1) * T, :], x_s))

    loaded(2)
    loaded(3)
    tail_src[0:4, :] = jnp.broadcast_to(states[T - 1 : T, :], (4, H))
    tail_src[4:8, :] = jnp.broadcast_to(ids[0:1, T - 1 : T].astype(F32), (4, H))
    hands_on = jnp.logical_and(y == 1, z < nz - 1)
    takes_over = jnp.logical_and(y == 1, z > 0)
    send_if(hands_on, tail_src, tail_mid, n_s, n_r, column((z + 1) % nz))
    unsent.append((hands_on, tail_src, n_s))
    for j in range(nh):
        pay_src[j, 0:T, :] = states[:, j * hb : (j + 1) * hb].astype(BF16)
        pay_src[j, T:, :] = jnp.broadcast_to(ids[...].astype(F32), (16, hb)).astype(BF16)
    for j in range(nh):
        send_or_local(pay_src.at[j], pay.at[q], p_s, p_r, at(z, j), k == j)
    unsent.append((True, pay.at[0 : nh - 1], p_s))

    def origin(step):
        plane = (z + (1 - 2 * high) * step + nz) % nz
        g = (per * plane - k + nh - 1) // nh
        return plane, g % GATES, jnp.logical_and(g < GATES, nh * g + k < per * (plane + 1))

    order = []
    for n in range(nr):
        chip = (x + n // 2) % nx
        order.append(2 * chip + (c + n) % 2)

    def spread(step, numbers):
        plane, g, found = origin(step)
        outer = jnp.logical_and(found, jnp.logical_not(inner))
        within = jnp.logical_and(found, inner)
        far, near = column(half - high), column(z + 1 - 2 * (z % half))
        for n in numbers:
            block = piece(g, pl.ds(pl.multiple_of(order[n] * cw, cw), cw))
            sem = w_r.at[g * nr + order[n]]
            if step == 0:
                pl.when(found)(functools.partial(landed, block, sem))
                send_if(found, block, block, w_f.at[0], sem, far)
                send_if(within, block, block, w_f.at[0], sem, near)
            else:
                pl.when(within)(functools.partial(landed, block, sem))
                send_if(within, block, block, w_f.at[step], sem, column(end))
        if step == 0:
            for n in numbers:
                block = piece(g, pl.ds(pl.multiple_of(order[n] * cw, cw), cw))
                send_if(outer, block, block, w_f.at[0], w_r.at[g * nr + order[n]], near)
            unsent.append((found, w_all.at[0 : 2 * hb, :], w_f.at[0]))
        elif numbers[-1] == nr - 1:
            unsent.append((within, w_all.at[0:hb, :], w_f.at[step]))

    def relay(dx, dy, targets):
        slot = features(dx, dy, 0)
        landed(rows(x_all, slot, T), x_r.at[slot])
        share(dx, dy, targets)

    spread(0, range(nr))
    pl.when(takes_over)(functools.partial(landed, tail_mid, n_r))
    for j in range(nh):
        part = tail_mid.at[:, j * hb : (j + 1) * hb]
        here = j == k
        send_if(jnp.logical_and(takes_over, j != k), part, tail_in.at[r], e_s, e_r, at(z, j))
        pl.when(jnp.logical_and(takes_over, here))(functools.partial(local, part, tail_in.at[r], e_r))
    unsent.append((takes_over, st_all.at[0 : nh - 1], e_s))
    spread(1, range(nr // 2))
    relay(c, 1 - c, (nearest, partner))
    spread(1, range(nr // 2, nr))
    relay(1 - c, c, (partner,))
    spread(2, range(nr))

    stride = T + 8
    landed(pay, p_r)
    pl.when(z > 0)(functools.partial(landed, tail_in, e_r))
    for m in range(nh):
        base = m * stride + 8
        span = slice(m * T, (m + 1) * T)
        prev[base : base + T, :] = pay[m, 0:T, :].astype(F32)
        ids_row = pay[m, T:, :].astype(F32)[0:1, :]
        ids_col[base : base + T, :] = jnp.broadcast_to(ids_row, (hb, T)).T
        if m % 2:
            before = base - stride + T - 1
            prev[base - 1 : base, :] = prev[before : before + 1, :]
            ids_col[base - 1 : base, :] = ids_col[before : before + 1, :]
        else:

            @pl.when(z > 0)
            def _():
                prev[base - 1 : base, :] = tail_in[m // 2, 0:1, :]
                ids_col[base - 1 : base, :] = tail_in[m // 2, 4:5, :]

            @pl.when(z == 0)
            def _():
                prev[base - 1 : base, :] = jnp.zeros((1, hb), F32)
                ids_col[base - 1 : base, :] = jnp.full((1, hb), -1.0, F32)

        same = jnp.where(
            ids_col[base : base + T, :] == ids_col[base - 1 : base - 1 + T, :], 1.0, 0.0
        )
        same_all[span, :] = same
        prior_all[span, :] = prev[base - 1 : base - 1 + T, :] * same

    loaded(5)
    loaded(6)
    (_, g0, found0), (_, g1, _), (_, g2, _), (_, g3, found3) = (origin(step) for step in range(nz))
    own, wide = found0.astype(jnp.int32), found3.astype(jnp.int32)
    early = own * g0 + (1 - own) * g1
    late = wide * g3 + (1 - wide) * g2
    middle = (GATES - early - late) % GATES
    outer = jnp.logical_not(inner)

    def arrived(g, unseen):
        for col in range(nr):
            block = piece(g, slice(col * cw, (col + 1) * cw))
            pl.when(unseen)(functools.partial(landed, block, w_r.at[g * nr + col]))

    def project(span, g):
        return lax.dot_general(
            x_all[span, :], piece(g, slice(None))[...], (((1,), (1,)), ((), ())),
            preferred_element_type=F32,
        )

    def ahead(blocks):
        for m in blocks:
            span = pl.ds(pl.multiple_of(m * T, T), T)
            for g in (early, middle):
                pre[g, span, :] = project(span, g)

    hops = [(0, 0), (0, 1), (1, 0), (1, 1)]
    for dx, dy in hops[:3]:
        m = features(dx, dy, 1)
        landed(rows(x_all, m, T), x_r.at[m])
    arrived(early, jnp.logical_and(jnp.logical_not(found0), outer))
    arrived(middle, outer)
    ahead([features(dx, dy, core) for dx, dy in hops[:3] for core in range(2)])
    loaded(4)
    for j in range(nh):
        part = upstream.at[:, j * hb : (j + 1) * hb]
        send_or_local(part, up_in.at[q], v_s, v_r, at(z, j), k == j)
    unsent.append((True, up_in.at[0 : nh - 1], v_s))
    relay(1, 1, (partner,))
    m = features(1, 1, 1)
    landed(rows(x_all, m, T), x_r.at[m])
    ahead([features(1, 1, core) for core in range(2)])
    arrived(late, jnp.logical_or(found3, outer))

    group = pl.ds(pl.multiple_of(k * hb, hb), hb)
    rz, rr, rc = (recur[i : i + 1, group] for i in range(GATES))
    bz, br, bc = (bias[i : i + 1, group] for i in range(GATES))
    for m in range(nh):
        span = slice(m * T, (m + 1) * T)
        last = project(span, late)
        pz, pr, pc = (jnp.where(late == i, last, pre[i, span, :]) for i in range(GATES))
        prior = prior_all[span, :]
        gz = jax.nn.sigmoid(pz + rz * prior + bz)
        gr = jax.nn.sigmoid(pr + rr * prior + br)
        rp = gr * prior
        gc = jnp.tanh(pc + rc * rp + bc)
        az = (gc - prior) * gz * (1.0 - gz)
        ac = gz * (1.0 - gc * gc)
        slope = rp * (1.0 - gr)
        acr = ac * rc
        co_z[span, :] = az
        co_c[span, :] = ac
        co_r[span, :] = acr * slope
        rprior[span, :] = rp
        jac[m * stride : m * stride + T, :] = same_all[span, :] * (
            1.0 - gz + az * rz + acr * (gr + slope * rr)
        )

    landed(up_in, v_r)
    for m in range(nh):
        up[m * stride : m * stride + T, :] = up_in[m].astype(F32)

    def back(i, state):
        a, b = state
        t = T - 1 - i
        f = jac[pl.ds(t, nh, stride=stride), :]
        b = b + up[pl.ds(t, nh, stride=stride), :]
        scan_a[pl.ds(t, nh, stride=stride), :] = a
        scan_b[pl.ds(t, nh, stride=stride), :] = b
        return f * a, f * b

    a, b = lax.fori_loop(0, T, back, (jnp.ones((nh, hb), F32), jnp.zeros((nh, hb), F32)), unroll=8)
    seg_out[...] = jnp.zeros(seg_out.shape, F32)
    for o in range(nr):
        first, second = slice(2 * o, 2 * o + 1), slice(2 * o + 1, 2 * o + 2)
        seg_out[0, o : o + 1, :] = a[first, :] * a[second, :]
        seg_out[1, o : o + 1, :] = b[first, :] + a[first, :] * b[second, :]
    for plane in range(nz - 1):
        send_if(plane < z, seg_out, seg_in.at[z], c_s, c_r.at[z], at(plane, k))
        unsent.append((z == plane + 1, seg_in.at[0 : plane + 1], c_s))
    carry[...] = jnp.zeros(carry.shape, F32)
    for plane in reversed(range(1, nz)):

        @pl.when(plane > z)
        def _():
            landed(seg_in.at[plane], c_r.at[plane])
            carry[0:nr, :] = seg_in[plane, 1, 0:nr, :] + seg_in[plane, 0, 0:nr, :] * carry[0:nr, :]

    into = carry[0:nr, :]
    carry_rows = []
    for o in range(nr):
        later = into[o : o + 1, :]
        second = slice(2 * o + 1, 2 * o + 2)
        carry_rows += [b[second, :] + a[second, :] * later, later]
    carried = jnp.concatenate(carry_rows, 0)

    for m in range(nh):
        span = slice(m * T, (m + 1) * T)
        padded = slice(m * stride, m * stride + T)
        adj = scan_b[padded, :] + scan_a[padded, :] * carried[m : m + 1, :]
        lam[span, :] = adj
        for g, slope in enumerate((co_z, co_r, co_c)):
            grads[span, g * hb : (g + 1) * hb] = (adj * slope[span, :]).astype(BF16)

    def quarter(col):
        return slice(col * cw, (col + 1) * cw)

    def gate_of(step):
        g = high * step + (1 - high) * (GATES - 1 - step)
        return g, (nh * g + k) // per

    def short(hidden):
        g = (per * z - hidden + nh - 1) // nh
        have = jnp.logical_and(g < GATES, nh * g + hidden < per * (z + 1))
        return jnp.logical_and(outer, jnp.logical_not(have))

    lacks, helps = short(k), short(2 * nx * c + 2 * ((x + 1) % nx) + y)
    beside = place(s, 2 * ((x + 1) % nx) + c)
    hub = high + half - 1
    halves = slice(nr // 2 * cw, DI)

    near = inner.astype(jnp.int32)
    turns = (
        (GATES - 1) * (high * near + (1 - high) * (1 - near)),
        (GATES - 1) * (1 - high) * near + 1 - near,
        near + (GATES - 1) * high * (1 - near),
    )

    def statistics():
        sums = [jnp.zeros((1, hb), F32) for _ in range(6)]
        for m in range(nh):
            span = slice(m * T, (m + 1) * T)
            prior = prior_all[span, :]
            adj = lam[span, :]
            grad_z = adj * co_z[span, :]
            grad_r = adj * co_r[span, :]
            grad_c = adj * co_c[span, :]
            terms = (grad_z, grad_r, grad_c, grad_z * prior, grad_r * prior, grad_c * rprior[span, :])
            sums = [total + jnp.sum(term, 0, keepdims=True) for total, term in zip(sums, terms)]
        for i in range(6):
            st_out[i : i + 1, :] = sums[i]
        st_out[6:8, :] = jnp.zeros((2, hb), F32)
        st_z[z] = st_out[...]
        for plane in range(nz):
            send_if(plane != z, st_out, st_z.at[z], t_s, t_r, column(plane))
        unsent.append((True, st_z.at[0 : nz - 1], t_s))

    def weigh(step):
        g = turns[step]
        plane = (nh * g + k) // per
        block = lax.dot_general(
            grads[:, pl.ds(pl.multiple_of(g * hb, hb), hb)], x_all[...], (((0,), (0,)), ((), ())),
            preferred_element_type=F32,
        )
        wg_own[g] = block
        wg_out[g] = block.astype(BF16)
        outward = jnp.logical_and(inner, plane == end)
        inward = jnp.logical_and(outer, plane != z)
        for col in range(nr):
            if step == 0 and col == nr // 2:
                statistics()
            part = wg_out.at[g, :, quarter(col)]
            send_if(
                jnp.logical_and(inward, plane != hub), part, wg_end.at[g, :, quarter(col)], g_s.at[g],
                g_e.at[g * nr + col], column(hub),
            )
            send_if(
                outward, part, wg_mid.at[0, :, quarter(col)], g_s.at[g], g_m.at[col], column(end),
            )
        if step == GATES - 1:
            send_if(lacks, wg_out.at[g, :, halves], wg_via, g_s.at[g], h_r, beside)
        unsent.append((plane != z, wg_out.at[g], g_s.at[g]))

    def nearby(step):
        g, plane = gate_of(step)
        for col in range(nr):
            go = jnp.logical_and(outer, plane == hub)
            if step == GATES - 1 and col >= nr // 2:
                go = jnp.logical_and(go, jnp.logical_not(lacks))
            send_if(
                go, wg_out.at[g, :, quarter(col)], wg_end.at[g, :, quarter(col)], g_s.at[g],
                g_e.at[g * nr + col], column(hub),
            )

    def assist():
        g, _ = gate_of(GATES - 1)
        pl.when(helps)(functools.partial(landed, wg_via, h_r))
        for col in range(nr // 2, nr):
            part = wg_via.at[:, (col - nr // 2) * cw : (col - nr // 2 + 1) * cw]
            where = place(2 * hub + y, 2 * ((x + 1) % nx) + c)
            send_if(helps, part, wg_end.at[g, :, quarter(col)], h_s, g_e.at[g * nr + col], where)
        unsent.append((helps, wg_via, h_s))

    chips = [(x + 1, y + 1), (x + 1, y), (x, y + 1), (x, y)]
    lot = (0, 1, 1, 2)

    def tokens(n, core):
        return rows(grads, 2 * (2 * (chips[n][0] % nx) + core) + chips[n][1] % 2, T)[...]

    def give(n):
        part_out[n] = jnp.dot(tokens(n, 1 - c), w_all[...], preferred_element_type=F32).astype(BF16)
        send(part_out.at[n], part_in.at[n], d_s, d_r.at[lot[n]], partner)

    def keep(n):
        part_keep[n] = jnp.dot(tokens(n, c), w_all[...], preferred_element_type=F32)

    def both(n):
        return part_keep[n] + part_in[n].astype(F32)

    weigh(0)
    give(0)
    keep(0)
    weigh(1)
    give(1)
    give(2)
    landed(part_in.at[0], d_r.at[0])
    fin_out[0] = both(0).astype(BF16)
    send(fin_out.at[0], fin_in.at[0], f_s, f_r.at[0], nearest)
    weigh(2)
    keep(1)
    keep(2)
    landed(part_in.at[1:3], d_r.at[1])
    fin_out[1] = both(1 + c).astype(BF16)
    send(fin_out.at[1], fin_in.at[1], f_s, f_r.at[1], nearest)
    give(3)
    keep(3)
    unsent.append((True, part_out, d_s))
    unsent.append((True, fin_out, f_s))

    scale = 1.0 / math.sqrt(ns * nr * T)
    def gather_stats():
        landed(st_z.at[0 : nz - 1], t_r)
        total = st_z[0]
        for plane in range(1, nz):
            total = total + st_z[plane]
        st_sum[...] = total * scale
        st_all[k] = st_sum[...]
        for j in range(nh):
            send_if(j != k, st_sum, st_all.at[k], u_s, u_r, at(z, j))
        unsent.append((True, st_all.at[0 : nh - 1], u_s))

    def turn():
        total = both(2 - c)
        landed(fin_in.at[0], f_r.at[0])
        fin_out[2] = (total + fin_in[0].astype(F32)).astype(BF16)
        send(fin_out.at[2], fin_in.at[2], f_s, f_r.at[2], across)

    for step in range(GATES):
        if step == 1:
            turn()
            for other in range(GATES):
                nearby(other)
            assist()
        g, plane = gate_of(step)
        passed = jnp.logical_and(inner, jnp.logical_and(plane != z, plane != end))
        far = (plane // half != high) & ((plane == 0) | (plane == nz - 1))
        for col in range(nr):
            cols = quarter(col)

            @pl.when(passed)
            def _():
                landed(wg_end.at[g, :, cols], g_e.at[g * nr + col])
                wg_out[g, :, cols] = (wg_own[g, :, cols] + wg_end[g, :, cols].astype(F32)).astype(BF16)

            for slot, there in enumerate((jnp.logical_not(far), far)):
                send_if(
                    jnp.logical_and(passed, there), wg_out.at[g, :, cols], wg_mid.at[slot, :, cols],
                    g_s.at[g], g_m.at[slot * nr + col], column(plane),
                )

    gather_stats()
    _, g, found = origin(0)
    b = nh * g + k
    owner, i = b // GATES, b % GATES
    for col in range(nr):
        cols = quarter(col)

        @pl.when(found)
        def _():
            landed(wg_mid.at[0, :, cols], g_m.at[col])
            wg_fin[:, cols] = wg_own[g, :, cols] + wg_mid[0, :, cols].astype(F32)

        @pl.when(jnp.logical_and(found, inner))
        def _():
            landed(wg_end.at[g, :, cols], g_e.at[g * nr + col])
            wg_out[g, :, cols] = (wg_fin[:, cols] + wg_end[g, :, cols].astype(F32)).astype(BF16)

        @pl.when(jnp.logical_and(found, jnp.logical_not(inner)))
        def _():
            landed(wg_mid.at[1, :, cols], g_m.at[nr + col])
            wg_out[g, :, cols] = (wg_fin[:, cols] + wg_mid[1, :, cols].astype(F32)).astype(BF16)

        here = jnp.logical_and(owner == s, r == col)

        @pl.when(jnp.logical_and(found, here))
        def _():
            local(wg_out.at[g, :, cols], wg_in.at[i], g_r.at[i])

        send_if(
            jnp.logical_and(found, jnp.logical_not(here)), wg_out.at[g, :, cols], wg_in.at[i],
            g_f, g_r.at[i], place(owner, col),
        )
    unsent.append((jnp.logical_and(found, owner != s), wg_out.at[0], g_f))
    unsent.append((jnp.logical_and(found, owner == s), wg_out.at[0, :, 0 : (nr - 1) * cw], g_f))

    landed(st_all.at[0 : nh - 1], u_r)
    for j in range(nh):
        out_p[:, j * hb : (j + 1) * hb] = st_all[j, :6, :]

    landed(part_in.at[3], d_r.at[2])
    total = both(3)
    for n in (1, 2):
        landed(fin_in.at[n], f_r.at[n])
        total = total + fin_in[n].astype(F32)
    out_in[...] = total.astype(BF16)

    for i in range(GATES):
        landed(wg_in.at[i], g_r.at[i])
        out_w[i * hb : (i + 1) * hb, :] = wg_in[i].astype(F32) * scale

    for sent, src, sem in unsent:
        if sent is True:
            landed(src, sem)
        else:

            @pl.when(sent)
            def _():
                landed(src, sem)


def flush(in_a, in_b, in_c, out_a, out_b, out_c, sems):
    pairs = [(in_a, out_a), (in_b, out_b), (in_c, out_c)]
    copies = [pltpu.make_async_copy(a, b, sems.at[i]) for i, (a, b) in enumerate(pairs)]
    for copy in copies:
        copy.start()
    for copy in copies:
        copy.wait()


def by_hidden(ns, nr, inputs, weight_t, states, doc_ids, recur, bias, out_grad):
    T, DI = inputs.shape[1:]
    H = states.shape[2]
    nh, nz, nx = 2 * nr, ns // 2, nr // 2
    hb, cw = H // nh, DI // nr
    L = nh * T
    vm = pltpu.VMEM
    scratch = [
        vm(weight_t.shape, BF16),
        vm((T, H), F32),
        vm((1, T), jnp.int32),
        vm((GATES, H), F32),
        vm((GATES, H), F32),
        vm((T, H), BF16),
        vm((nh, T + 16, hb), BF16),
        vm((nh, T + 16, hb), BF16),
        vm((nh, T, hb), BF16),
        vm((8, H), F32),
        vm((8, H), F32),
        vm((nr, 8, hb), F32),
        vm((L, DI), BF16),
        vm((GATES * hb, DI), BF16),
        vm((L + 8 * nh, hb), F32),
        vm((L + 8 * nh, hb), F32),
        vm((L, hb), F32),
        vm((L + 8 * nh, hb), F32),
        vm((GATES, L, hb), F32),
        vm((L + 8 * nh, hb), F32),
        vm((L, hb), F32),
        vm((L, hb), F32),
        vm((L, hb), F32),
        vm((L, hb), F32),
        vm((L, hb), F32),
        vm((L + 8 * nh, hb), F32),
        vm((L + 8 * nh, hb), F32),
        vm((nh, hb), F32),
        vm((2, 8, hb), F32),
        vm((nz, 2, 8, hb), F32),
        vm((L, hb), F32),
        vm((L, GATES * hb), BF16),
        vm((hb, DI // 2), BF16),
        vm((nr, T, DI), BF16),
        vm((nr, T, DI), BF16),
        vm((nr, T, DI), F32),
        vm((3, T, DI), BF16),
        vm((3, T, DI), BF16),
        vm((GATES, hb, DI), F32),
        vm((GATES, hb, DI), BF16),
        vm((GATES, hb, DI), BF16),
        vm((2, hb, DI), BF16),
        vm((hb, DI), F32),
        vm((GATES, hb, cw), BF16),
        vm((8, hb), F32),
        vm((nz, 8, hb), F32),
        vm((8, hb), F32),
        vm((nh, 8, hb), F32),
    ]
    dma = pltpu.SemaphoreType.DMA
    counts = [
        7, None, nh, GATES, nz - 1, GATES * nr, None, None, None, None, None, None, None, None, None, nz,
        None, 3, None, 3, GATES, GATES * nr, 2 * nr, None, GATES, None, None, None, None, None, None,
    ]
    sems = [dma if n is None else dma((n,)) for n in counts]
    whole = pl.BlockSpec(memory_space=pltpu.VMEM)
    out_in, out_w, out_p = pl.pallas_call(
        functools.partial(kernel, ns, nr),
        out_shape=(
            pltpu.VMEM((T, DI), BF16),
            pltpu.VMEM(weight_t.shape, F32),
            pltpu.VMEM((6, H), F32),
        ),
        in_specs=[pl.BlockSpec(memory_space=pltpu.HBM)] * 7,
        out_specs=(whole,) * 3,
        scratch_shapes=scratch + sems,
        compiler_params=pltpu.CompilerParams(
            collective_id=0, has_side_effects=True, vmem_limit_bytes=56 * 1024 * 1024
        ),
    )(inputs[0], weight_t, states[0], doc_ids, recur, bias, out_grad[0])
    shapes = ((T, DI), BF16), (weight_t.shape, F32), ((6, H), F32)
    out_in, out_w, out_p = pl.pallas_call(
        flush,
        out_shape=tuple(jax.ShapeDtypeStruct(*one) for one in shapes),
        in_specs=[whole] * 3,
        out_specs=(pl.BlockSpec(memory_space=pltpu.HBM),) * 3,
        scratch_shapes=[dma((3,))],
    )(*(pltpu.with_memory_space_constraint(one, pltpu.VMEM) for one in (out_in, out_w, out_p)))
    return out_in[None], out_w, out_p


def fits(ns, nr, inputs, weight_t, states):
    parts, L, DI = inputs.shape
    H = states.shape[2]
    return (
        parts == nr
        and ns == 2 * nr
        and ns % 8 == 0
        and ns == 8
        and L * 2 * nr == H * ns
        and H % (ns * 128) == 0
        and DI % (nr * 128) == 0
        and L % (ns * 128) == 0
        and L * DI <= 1 << 21
    )


def solution(mesh):
    ns, nr = mesh.shape["seq"], mesh.shape["rep"]
    placed = (
        P("rep", "seq", None),
        P("seq", "rep"),
        P("rep", "seq", None),
        P("rep", "seq"),
        P(),
        P(),
        P("rep", "seq", None),
    )

    def run(inputs, weight_t, states, doc_ids, recur, bias, out_grad):
        kernelized = fits(ns, nr, inputs, weight_t, states)
        body = functools.partial(by_hidden, ns, nr) if kernelized else by_tokens
        return jax.shard_map(
            body,
            mesh=mesh,
            in_specs=placed,
            out_specs=(P("rep", "seq", None), P("seq", "rep"), P()),
            check_vma=False,
        )(inputs, weight_t, states, doc_ids, recur, bias, out_grad)

    return run
```

```python
import functools
import math

import jax
import jax.numpy as jnp
from jax import lax
from jax.experimental import pallas as pl
from jax.experimental.pallas import tpu as pltpu
from jax.sharding import PartitionSpec as P

F32 = jnp.float32
BF16 = jnp.bfloat16
GATES = 3


def shifted(block, axis, distance):
    devices = range(lax.axis_size(axis))
    route = [(i - distance, i) for i in devices if i - distance in devices]
    return lax.ppermute(block, axis, route)


def compose(earlier, later):
    return (later[0] * earlier[0], later[1] + later[0] * earlier[1])


def by_tokens(inputs, weight_t, states, doc_ids, recur, bias, out_grad):
    feats = inputs[0]
    hidden_now = states[0]
    ids_float = doc_ids[0].astype(F32)
    count = feats.shape[0]
    width = hidden_now.shape[1]
    columns = lax.all_gather(weight_t, "rep", axis=1, tiled=True)
    contract_last = (((1,), (1,)), ((), ()))
    full_weight = lax.all_gather(columns, "seq", axis=0, tiled=True)
    preact = lax.dot_general(feats, full_weight, contract_last, preferred_element_type=F32)
    tail_state, tail_id = shifted((hidden_now[-1:], ids_float[-1:]), "seq", 1)
    first_same = jnp.where(
        (ids_float[0] == tail_id[0]) & (lax.axis_index("seq") > 0), 1.0, 0.0
    ).astype(F32)
    same = jnp.concatenate([first_same[None], (ids_float[1:] == ids_float[:-1]).astype(F32)])
    prior = jnp.concatenate([tail_state, hidden_now[:-1]], 0) * same[:, None]
    gate_z = jax.nn.sigmoid(preact[:, :width] + recur[0] * prior + bias[0])
    gate_r = jax.nn.sigmoid(preact[:, width : 2 * width] + recur[1] * prior + bias[1])
    gate_c = jnp.tanh(preact[:, 2 * width :] + recur[2] * gate_r * prior + bias[2])
    jacobian = same[:, None] * (
        1.0
        - gate_z
        + (gate_c - prior) * gate_z * (1.0 - gate_z) * recur[0]
        + gate_z
        * (1.0 - gate_c * gate_c)
        * recur[2]
        * (gate_r + prior * gate_r * (1.0 - gate_r) * recur[1])
    )
    upstream = out_grad[0].astype(F32)
    jac_rows, up_rows = (
        lax.all_to_all(jacobian.T, "seq", split_axis=0, concat_axis=1, tiled=True),
        lax.all_to_all(upstream.T, "seq", split_axis=0, concat_axis=1, tiled=True),
    )
    factor = jnp.concatenate([jac_rows[:, 1:], jnp.zeros((jac_rows.shape[0], 1), F32)], 1)
    _, adjoint_rows = lax.associative_scan(compose, (factor, up_rows), reverse=True, axis=1)
    adjoint = lax.all_to_all(adjoint_rows, "seq", split_axis=1, concat_axis=0, tiled=True).T
    grad_z = adjoint * (gate_c - prior) * gate_z * (1.0 - gate_z)
    grad_c = adjoint * gate_z * (1.0 - gate_c * gate_c)
    grad_r = grad_c * recur[2] * prior * gate_r * (1.0 - gate_r)
    grad_pre = jnp.concatenate([grad_z, grad_r, grad_c], 1).astype(BF16)
    input_grad = jnp.dot(grad_pre, full_weight, preferred_element_type=F32)
    tokens_all = count * inputs.shape[0] * lax.axis_size("seq") * lax.axis_size("rep")
    normal_factor = 1.0 / math.sqrt(tokens_all)
    row_share = lax.psum_scatter(
        lax.dot_general(grad_pre, feats, (((0,), (0,)), ((), ())), preferred_element_type=F32),
        "seq",
        scatter_dimension=0,
        tiled=True,
    )
    weight_grad = (
        lax.psum_scatter(row_share.astype(BF16), "rep", scatter_dimension=1, tiled=True).astype(F32)
        * normal_factor
    )
    stats = jnp.stack(
        [
            grad_z.sum(0),
            grad_r.sum(0),
            grad_c.sum(0),
            (grad_z * prior).sum(0),
            (grad_r * prior).sum(0),
            (grad_c * gate_r * prior).sum(0),
        ]
    )
    param_grad = lax.psum(stats, ("seq", "rep")) * normal_factor
    return (input_grad.astype(BF16)[None], weight_grad, param_grad)


def kernel(
    ns, nr, feats_hbm, weight_hbm, states_hbm, ids_hbm, recur_hbm, bias_hbm, upstream_hbm,
    out_in, out_w, out_p,
    weight, states, ids, recur, bias, upstream,
    pay_src, pay, up_in, tail_src, tail_mid, tail_in, x_all, w_all, prev, ids_col, same_all, up,
    pre, jac, co_z, co_r, co_c, rprior, prior_all,
    scan_a, scan_b, carry, seg_out, seg_in, lam, grads, wg_via, part_out, part_in, part_keep, fin_out, fin_in,
    wg_own, wg_out, wg_end, wg_mid, wg_in, st_out, st_z, st_sum, st_all,
    l_s, x_s, x_r, w_s, w_f, w_r, p_s, p_r, v_s, v_r, e_s, e_r, n_s, n_r, c_s, c_r,
    d_s, d_r, f_s, f_r, g_s, g_e, g_m, g_f, g_r, t_s, t_r, u_s, u_r, h_s, h_r,
):
    T, DI = feats_hbm.shape
    H = states.shape[1]
    nh, nz, nx = 2 * nr, ns // 2, nr // 2
    hb, cw = H // nh, DI // nr
    s, r = lax.axis_index("seq"), lax.axis_index("rep")
    z, y, x, c = s // 2, s % 2, r // 2, r % 2
    q = 2 * r + y
    k = nx * 2 * c + 2 * x + y
    half, per = nz // 2, GATES * nh // nz
    high = z // half
    inner = jnp.logical_or(z == half - 1, z == half)
    end = high * (nz - 1)
    unsent = []

    def place(a, b):
        return {"seq": a, "rep": b}

    def at(plane, j):
        return place(2 * plane + j % 2, 2 * (j // 2 % nx) + j // (2 * nx))

    def column(plane):
        return place(2 * plane + y, r)

    def send(src, dst, ssem, rsem, where):
        pltpu.make_async_remote_copy(
            src_ref=src, dst_ref=dst, send_sem=ssem, recv_sem=rsem,
            device_id=where, device_id_type=pl.DeviceIdType.MESH,
        ).start()

    def local(src, dst, rsem):
        pltpu.make_async_copy(src, dst, rsem).start()

    def landed(dst, sem):
        pltpu.make_async_copy(dst, dst, sem).wait()

    def send_if(allowed, *args):
        pl.when(allowed)(functools.partial(send, *args))

    def send_or_local(src, dst, ssem, rsem, where, here):
        send_if(jnp.logical_not(here), src, dst, ssem, rsem, where)
        pl.when(here)(functools.partial(local, src, dst, rsem))

    def rows(ref, block, count):
        return ref.at[pl.ds(pl.multiple_of(block * count, count), count), :]

    barrier = pltpu.get_barrier_semaphore()

    def greet(where):
        pl.semaphore_signal(barrier, inc=1, device_id=where, device_id_type=pl.DeviceIdType.MESH)

    for j in range(nh):
        pl.when(j != k)(functools.partial(greet, at(z, j)))
    for plane in range(nz):
        pl.when(plane != z)(functools.partial(greet, column(plane)))
    loads = [
        (weight_hbm, weight), (feats_hbm, rows(x_all, q, T)), (states_hbm, states), (ids_hbm, ids),
        (upstream_hbm, upstream), (recur_hbm, recur), (bias_hbm, bias),
    ]
    for n, (src, dst) in enumerate(loads):
        local(src, dst, l_s.at[n])

    def loaded(n):
        landed(loads[n][1], l_s.at[n])

    def piece(g, col):
        return w_all.at[pl.ds(pl.multiple_of(g * hb, hb), hb), col]

    loaded(0)
    pl.semaphore_wait(barrier, nh - 1 + nz - 1)

    mine = pl.ds(pl.multiple_of(r * cw, cw), cw)
    for i in range(GATES):
        b = GATES * s + i
        g, j = b // nh, b % nh
        part = weight.at[i * hb : (i + 1) * hb, :]
        send_or_local(part, piece(g, mine), w_s.at[i], w_r.at[g * nr + r], at(z, j), j == k)
        unsent.append((j != k, part, w_s.at[i]))

    partner = place(s, r + 1 - 2 * c)
    nearest = place(2 * z + (y + c) % 2, 2 * ((x + 1 - c) % nx) + c)
    across = place(2 * z + (y + 1 - c) % 2, 2 * ((x + c) % nx) + c)

    def features(dx, dy, core):
        return 2 * (2 * ((x + dx) % nx) + (c + core) % 2) + (y + dy) % 2

    def share(dx, dy, targets):
        slot = features(dx, dy, 0)
        block = rows(x_all, slot, T)
        for where in targets:
            send(block, block, x_s, x_r.at[slot], where)

    loaded(1)
    share(0, 0, (nearest, across, partner))
    unsent.append((True, x_all.at[0 : (nh - 1) * T, :], x_s))

    loaded(2)
    loaded(3)
    tail_src[0:4, :] = jnp.broadcast_to(states[T - 1 : T, :], (4, H))
    tail_src[4:8, :] = jnp.broadcast_to(ids[0:1, T - 1 : T].astype(F32), (4, H))
    hands_on = jnp.logical_and(y == 1, z < nz - 1)
    takes_over = jnp.logical_and(y == 1, z > 0)
    send_if(hands_on, tail_src, tail_mid, n_s, n_r, column((z + 1) % nz))
    unsent.append((hands_on, tail_src, n_s))
    for j in range(nh):
        pay_src[j, 0:T, :] = states[:, j * hb : (j + 1) * hb].astype(BF16)
        pay_src[j, T:, :] = jnp.broadcast_to(ids[...].astype(F32), (16, hb)).astype(BF16)
    for j in range(nh):
        send_or_local(pay_src.at[j], pay.at[q], p_s, p_r, at(z, j), k == j)
    unsent.append((True, pay.at[0 : nh - 1], p_s))

    def origin(step):
        plane = (z + (1 - 2 * high) * step + nz) % nz
        g = (per * plane - k + nh - 1) // nh
        return plane, g % GATES, jnp.logical_and(g < GATES, nh * g + k < per * (plane + 1))

    order = []
    for n in range(nr):
        chip = (x + n // 2) % nx
        order.append(2 * chip + (c + n) % 2)

    def spread(step, numbers):
        plane, g, found = origin(step)
        outer = jnp.logical_and(found, jnp.logical_not(inner))
        within = jnp.logical_and(found, inner)
        far, near = column(half - high), column(z + 1 - 2 * (z % half))
        for n in numbers:
            block = piece(g, pl.ds(pl.multiple_of(order[n] * cw, cw), cw))
            sem = w_r.at[g * nr + order[n]]
            if step == 0:
                pl.when(found)(functools.partial(landed, block, sem))
                send_if(found, block, block, w_f.at[0], sem, far)
                send_if(within, block, block, w_f.at[0], sem, near)
            else:
                pl.when(within)(functools.partial(landed, block, sem))
                send_if(within, block, block, w_f.at[step], sem, column(end))
        if step == 0:
            for n in numbers:
                block = piece(g, pl.ds(pl.multiple_of(order[n] * cw, cw), cw))
                send_if(outer, block, block, w_f.at[0], w_r.at[g * nr + order[n]], near)
            unsent.append((found, w_all.at[0 : 2 * hb, :], w_f.at[0]))
        elif numbers[-1] == nr - 1:
            unsent.append((within, w_all.at[0:hb, :], w_f.at[step]))

    def relay(dx, dy, targets):
        slot = features(dx, dy, 0)
        landed(rows(x_all, slot, T), x_r.at[slot])
        share(dx, dy, targets)

    spread(0, range(nr))
    pl.when(takes_over)(functools.partial(landed, tail_mid, n_r))
    for j in range(nh):
        part = tail_mid.at[:, j * hb : (j + 1) * hb]
        here = j == k
        send_if(jnp.logical_and(takes_over, j != k), part, tail_in.at[r], e_s, e_r, at(z, j))
        pl.when(jnp.logical_and(takes_over, here))(functools.partial(local, part, tail_in.at[r], e_r))
    unsent.append((takes_over, st_all.at[0 : nh - 1], e_s))
    spread(1, range(nr // 2))
    relay(c, 1 - c, (nearest, partner))
    spread(1, range(nr // 2, nr))
    relay(1 - c, c, (partner,))
    loaded(4)

    def send_upstream(early):
        for j in range(nh):
            part = upstream.at[:, j * hb : (j + 1) * hb]
            over_x, over_y = j // 2 % nx != x, j % 2 != y
            other_link = jnp.where(c == 0, jnp.logical_and(over_y, jnp.logical_not(over_x)), over_x)
            now = jnp.logical_not(other_link) if early else other_link
            send_if(jnp.logical_and(now, j != k), part, up_in.at[q], v_s, v_r, at(z, j))
            if early:
                pl.when(j == k)(functools.partial(local, part, up_in.at[q], v_r))

    unsent.append((True, up_in.at[0 : nh - 1], v_s))
    send_upstream(True)
    spread(2, range(nr))

    stride = T + 8
    landed(pay, p_r)
    pl.when(z > 0)(functools.partial(landed, tail_in, e_r))
    for m in range(nh):
        base = m * stride + 8
        span = slice(m * T, (m + 1) * T)
        prev[base : base + T, :] = pay[m, 0:T, :].astype(F32)
        ids_row = pay[m, T:, :].astype(F32)[0:1, :]
        ids_col[base : base + T, :] = jnp.broadcast_to(ids_row, (hb, T)).T
        if m % 2:
            before = base - stride + T - 1
            prev[base - 1 : base, :] = prev[before : before + 1, :]
            ids_col[base - 1 : base, :] = ids_col[before : before + 1, :]
        else:

            @pl.when(z > 0)
            def _():
                prev[base - 1 : base, :] = tail_in[m // 2, 0:1, :]
                ids_col[base - 1 : base, :] = tail_in[m // 2, 4:5, :]

            @pl.when(z == 0)
            def _():
                prev[base - 1 : base, :] = jnp.zeros((1, hb), F32)
                ids_col[base - 1 : base, :] = jnp.full((1, hb), -1.0, F32)

        same = jnp.where(
            ids_col[base : base + T, :] == ids_col[base - 1 : base - 1 + T, :], 1.0, 0.0
        )
        same_all[span, :] = same
        prior_all[span, :] = prev[base - 1 : base - 1 + T, :] * same

    loaded(5)
    loaded(6)
    (_, g0, found0), (_, g1, _), (_, g2, _), (_, g3, found3) = (origin(step) for step in range(nz))
    own, wide = found0.astype(jnp.int32), found3.astype(jnp.int32)
    early = own * g0 + (1 - own) * g1
    late = wide * g3 + (1 - wide) * g2
    middle = (GATES - early - late) % GATES
    outer = jnp.logical_not(inner)

    def arrived(g, unseen):
        for col in range(nr):
            block = piece(g, slice(col * cw, (col + 1) * cw))
            pl.when(unseen)(functools.partial(landed, block, w_r.at[g * nr + col]))

    def project(span, g):
        return lax.dot_general(
            x_all[span, :], piece(g, slice(None))[...], (((1,), (1,)), ((), ())),
            preferred_element_type=F32,
        )

    def ahead(blocks):
        for m in blocks:
            span = pl.ds(pl.multiple_of(m * T, T), T)
            for g in (early, middle):
                pre[g, span, :] = project(span, g)

    hops = [(0, 0), (0, 1), (1, 0), (1, 1)]
    for dx, dy in hops[:3]:
        m = features(dx, dy, 1)
        landed(rows(x_all, m, T), x_r.at[m])
    arrived(early, jnp.logical_and(jnp.logical_not(found0), outer))
    arrived(middle, outer)
    ahead([features(dx, dy, core) for dx, dy in hops[:3] for core in range(2)])
    send_upstream(False)
    relay(1, 1, (partner,))
    ahead([features(1, 1, 0)])
    m = features(1, 1, 1)
    landed(rows(x_all, m, T), x_r.at[m])
    ahead([m])
    arrived(late, jnp.logical_or(found3, outer))

    group = pl.ds(pl.multiple_of(k * hb, hb), hb)
    rz, rr, rc = (recur[i : i + 1, group] for i in range(GATES))
    bz, br, bc = (bias[i : i + 1, group] for i in range(GATES))
    for m in range(nh):
        span = slice(m * T, (m + 1) * T)
        last = project(span, late)
        pz, pr, pc = (jnp.where(late == i, last, pre[i, span, :]) for i in range(GATES))
        prior = prior_all[span, :]
        gz = jax.nn.sigmoid(pz + rz * prior + bz)
        gr = jax.nn.sigmoid(pr + rr * prior + br)
        rp = gr * prior
        gc = jnp.tanh(pc + rc * rp + bc)
        az = (gc - prior) * gz * (1.0 - gz)
        ac = gz * (1.0 - gc * gc)
        slope = rp * (1.0 - gr)
        acr = ac * rc
        co_z[span, :] = az
        co_c[span, :] = ac
        co_r[span, :] = acr * slope
        rprior[span, :] = rp
        jac[m * stride : m * stride + T, :] = same_all[span, :] * (
            1.0 - gz + az * rz + acr * (gr + slope * rr)
        )

    landed(up_in, v_r)
    for m in range(nh):
        up[m * stride : m * stride + T, :] = up_in[m].astype(F32)

    def back(i, state):
        a, b = state
        t = T - 1 - i
        f = jac[pl.ds(t, nh, stride=stride), :]
        b = b + up[pl.ds(t, nh, stride=stride), :]
        scan_a[pl.ds(t, nh, stride=stride), :] = a
        scan_b[pl.ds(t, nh, stride=stride), :] = b
        return f * a, f * b

    a, b = lax.fori_loop(0, T, back, (jnp.ones((nh, hb), F32), jnp.zeros((nh, hb), F32)), unroll=8)
    seg_out[...] = jnp.zeros(seg_out.shape, F32)
    for o in range(nr):
        first, second = slice(2 * o, 2 * o + 1), slice(2 * o + 1, 2 * o + 2)
        seg_out[0, o : o + 1, :] = a[first, :] * a[second, :]
        seg_out[1, o : o + 1, :] = b[first, :] + a[first, :] * b[second, :]
    for plane in range(nz - 1):
        send_if(plane < z, seg_out, seg_in.at[z], c_s, c_r.at[z], at(plane, k))
        unsent.append((z == plane + 1, seg_in.at[0 : plane + 1], c_s))
    carry[...] = jnp.zeros(carry.shape, F32)
    for plane in reversed(range(1, nz)):

        @pl.when(plane > z)
        def _():
            landed(seg_in.at[plane], c_r.at[plane])
            carry[0:nr, :] = seg_in[plane, 1, 0:nr, :] + seg_in[plane, 0, 0:nr, :] * carry[0:nr, :]

    into = carry[0:nr, :]
    carry_rows = []
    for o in range(nr):
        later = into[o : o + 1, :]
        second = slice(2 * o + 1, 2 * o + 2)
        carry_rows += [b[second, :] + a[second, :] * later, later]
    carried = jnp.concatenate(carry_rows, 0)

    for m in range(nh):
        span = slice(m * T, (m + 1) * T)
        padded = slice(m * stride, m * stride + T)
        adj = scan_b[padded, :] + scan_a[padded, :] * carried[m : m + 1, :]
        lam[span, :] = adj
        for g, slope in enumerate((co_z, co_r, co_c)):
            grads[span, g * hb : (g + 1) * hb] = (adj * slope[span, :]).astype(BF16)

    def quarter(col):
        return slice(col * cw, (col + 1) * cw)

    def gate_of(step):
        g = high * step + (1 - high) * (GATES - 1 - step)
        return g, (nh * g + k) // per

    def short(hidden):
        g = (per * z - hidden + nh - 1) // nh
        have = jnp.logical_and(g < GATES, nh * g + hidden < per * (z + 1))
        return jnp.logical_and(outer, jnp.logical_not(have))

    other = 2 * nx * c + 2 * ((x + 1) % nx) + y
    lacks, helps = short(k), short(other)
    beside = place(s, 2 * ((x + 1) % nx) + c)
    hub = high + half - 1
    halves = slice(nr // 2 * cw, DI)

    near = inner.astype(jnp.int32)
    turns = (
        (GATES - 1) * (high * near + (1 - high) * (1 - near)),
        (GATES - 1) * (1 - high) * near + 1 - near,
        near + (GATES - 1) * high * (1 - near),
    )

    def statistics():
        sums = [jnp.zeros((1, hb), F32) for _ in range(6)]
        for m in range(nh):
            span = slice(m * T, (m + 1) * T)
            prior = prior_all[span, :]
            adj = lam[span, :]
            grad_z = adj * co_z[span, :]
            grad_r = adj * co_r[span, :]
            grad_c = adj * co_c[span, :]
            terms = (grad_z, grad_r, grad_c, grad_z * prior, grad_r * prior, grad_c * rprior[span, :])
            sums = [total + jnp.sum(term, 0, keepdims=True) for total, term in zip(sums, terms)]
        for i in range(6):
            st_out[i : i + 1, :] = sums[i]
        st_out[6:8, :] = jnp.zeros((2, hb), F32)
        st_z[z] = st_out[...]
        for plane in range(nz):
            send_if(plane != z, st_out, st_z.at[z], t_s, t_r, column(plane))
        unsent.append((True, st_z.at[0 : nz - 1], t_s))

    def weigh(step):
        g = turns[step]
        plane = (nh * g + k) // per
        spans = (slice(0, DI // 2), slice(DI // 2, DI)) if step == 0 else (slice(0, DI),)

        def product(span):
            block = lax.dot_general(
                grads[:, pl.ds(pl.multiple_of(g * hb, hb), hb)], x_all[:, span], (((0,), (0,)), ((), ())),
                preferred_element_type=F32,
            )
            wg_own[g, :, span] = block
            wg_out[g, :, span] = block.astype(BF16)

        product(spans[0])
        outward = jnp.logical_and(inner, plane == end)
        inward = jnp.logical_and(outer, plane != z)
        for col in range(nr):
            if step == 0 and col == 1:
                give(0)
                statistics()
                product(spans[1])
            part = wg_out.at[g, :, quarter(col)]
            send_if(
                jnp.logical_and(inward, plane != hub), part, wg_end.at[g, :, quarter(col)], g_s.at[g],
                g_e.at[g * nr + col], column(hub),
            )
            send_if(
                outward, part, wg_mid.at[0, :, quarter(col)], g_s.at[g], g_m.at[col], column(end),
            )
        if step == GATES - 1:
            send_if(lacks, wg_out.at[g, :, halves], wg_via, g_s.at[g], h_r, beside)
        unsent.append((plane != z, wg_out.at[g], g_s.at[g]))

    def nearby(step):
        g, plane = gate_of(step)
        for col in range(nr):
            go = jnp.logical_and(outer, plane == hub)
            if step == GATES - 1 and col >= nr // 2:
                go = jnp.logical_and(go, jnp.logical_not(lacks))
            send_if(
                go, wg_out.at[g, :, quarter(col)], wg_end.at[g, :, quarter(col)], g_s.at[g],
                g_e.at[g * nr + col], column(hub),
            )

    def assist():
        g, _ = gate_of(GATES - 1)
        pl.when(helps)(functools.partial(landed, wg_via, h_r))
        for col in range(nr // 2, nr):
            part = wg_via.at[:, (col - nr // 2) * cw : (col - nr // 2 + 1) * cw]
            where = place(2 * hub + y, 2 * ((x + 1) % nx) + c)
            send_if(helps, part, wg_end.at[g, :, quarter(col)], h_s, g_e.at[g * nr + col], where)
        unsent.append((helps, wg_via, h_s))

    chips = [(x + 1, y + 1), (x + 1, y), (x, y + 1), (x, y)]
    lot = (0, 1, 1, 2)

    def tokens(n, core):
        return rows(grads, 2 * (2 * (chips[n][0] % nx) + core) + chips[n][1] % 2, T)[...]

    def give(n):
        part_out[n] = jnp.dot(tokens(n, 1 - c), w_all[...], preferred_element_type=F32).astype(BF16)
        send(part_out.at[n], part_in.at[n], d_s, d_r.at[lot[n]], partner)

    def keep(n):
        part_keep[n] = jnp.dot(tokens(n, c), w_all[...], preferred_element_type=F32)

    def both(n):
        return part_keep[n] + part_in[n].astype(F32)

    parts = [slice(n * T // 2, (n + 1) * T // 2) for n in range(2)]
    scale = 1.0 / math.sqrt(ns * nr * T)

    def gather_stats():
        landed(st_z.at[0 : nz - 1], t_r)
        total = st_z[0]
        for plane in range(1, nz):
            total = total + st_z[plane]
        st_sum[...] = total * scale
        st_all[k] = st_sum[...]
        for j in range(nh):
            send_if(j != k, st_sum, st_all.at[k], u_s, u_r, at(z, j))
        unsent.append((True, st_all.at[0 : nh - 1], u_s))

    def turn(n):
        part = parts[n]
        landed(fin_in.at[0, part], f_r.at[n])
        total = part_keep[2 - c, part] + part_in[2 - c, part].astype(F32) + fin_in[0, part].astype(F32)
        fin_out[2, part] = total.astype(BF16)
        send(fin_out.at[2, part], fin_in.at[2, part], f_s, f_r.at[3 + n], across)

    def hand_on(step, numbers):
        g, plane = gate_of(step)
        passed = jnp.logical_and(inner, jnp.logical_and(plane != z, plane != end))
        far = (plane // half != high) & ((plane == 0) | (plane == nz - 1))
        for col in numbers:
            cols = quarter(col)

            @pl.when(passed)
            def _():
                landed(wg_end.at[g, :, cols], g_e.at[g * nr + col])
                wg_out[g, :, cols] = (wg_own[g, :, cols] + wg_end[g, :, cols].astype(F32)).astype(BF16)

            for slot, there in enumerate((jnp.logical_not(far), far)):
                send_if(
                    jnp.logical_and(passed, there), wg_out.at[g, :, cols], wg_mid.at[slot, :, cols],
                    g_s.at[g], g_m.at[slot * nr + col], column(plane),
                )

    weigh(0)
    keep(0)
    weigh(1)
    landed(part_in.at[0], d_r.at[0])
    fin_out[0] = both(0).astype(BF16)
    for n, part in enumerate(parts):
        send(fin_out.at[0, part], fin_in.at[0, part], f_s, f_r.at[n], nearest)
    give(1)
    give(2)
    weigh(2)
    hand_on(0, (0,))
    keep(1)
    keep(2)
    landed(part_in.at[1:3], d_r.at[1])
    fin_out[1] = both(1 + c).astype(BF16)
    send(fin_out.at[1], fin_in.at[1], f_s, f_r.at[2], nearest)
    hand_on(0, (1,))
    give(3)
    keep(3)
    hand_on(0, (2,))
    turn(0)
    hand_on(0, (3,))
    for n in range(GATES):
        nearby(n)
    gather_stats()
    turn(1)
    assist()
    for step in range(1, GATES):
        hand_on(step, range(nr))
    unsent.append((True, part_out, d_s))
    unsent.append((True, fin_out, f_s))

    _, g, found = origin(0)
    b = nh * g + k
    owner, i = b // GATES, b % GATES
    for col in range(nr):
        cols = quarter(col)

        @pl.when(found)
        def _():
            landed(wg_mid.at[0, :, cols], g_m.at[col])
            wg_own[g, :, cols] = wg_own[g, :, cols] + wg_mid[0, :, cols].astype(F32)

        @pl.when(jnp.logical_and(found, inner))
        def _():
            landed(wg_end.at[g, :, cols], g_e.at[g * nr + col])
            wg_own[g, :, cols] = wg_own[g, :, cols] + wg_end[g, :, cols].astype(F32)

        @pl.when(jnp.logical_and(found, outer))
        def _():
            landed(wg_mid.at[1, :, cols], g_m.at[nr + col])
            wg_own[g, :, cols] = wg_own[g, :, cols] + wg_mid[1, :, cols].astype(F32)

        @pl.when(found)
        def _():
            wg_out[g, :, cols] = wg_own[g, :, cols].astype(BF16)

        here = jnp.logical_and(owner == s, r == col)

        @pl.when(jnp.logical_and(found, here))
        def _():
            local(wg_out.at[g, :, cols], wg_in.at[i], g_r.at[i])

        send_if(
            jnp.logical_and(found, jnp.logical_not(here)), wg_out.at[g, :, cols], wg_in.at[i],
            g_f, g_r.at[i], place(owner, col),
        )
    unsent.append((jnp.logical_and(found, owner != s), wg_out.at[0], g_f))
    unsent.append((jnp.logical_and(found, owner == s), wg_out.at[0, :, 0 : (nr - 1) * cw], g_f))

    landed(st_all.at[0 : nh - 1], u_r)
    for j in range(nh):
        out_p[:, j * hb : (j + 1) * hb] = st_all[j, :6, :]

    landed(part_in.at[3], d_r.at[2])
    total = both(3)
    landed(fin_in.at[1], f_r.at[2])
    for n, part in enumerate(parts):
        landed(fin_in.at[2, part], f_r.at[3 + n])
    total = total + fin_in[1].astype(F32) + fin_in[2].astype(F32)
    out_in[...] = total.astype(BF16)

    for i in range(GATES):
        landed(wg_in.at[i], g_r.at[i])
        block = slice(i * hb, (i + 1) * hb)
        out_w[block, :] = wg_in[i].astype(F32) * scale

    for sent, src, sem in unsent:
        if sent is True:
            landed(src, sem)
        else:

            @pl.when(sent)
            def _():
                landed(src, sem)


def flush(in_a, in_b, in_c, out_a, out_b, out_c, sems):
    pairs = [(in_a, out_a), (in_b, out_b), (in_c, out_c)]
    copies = [pltpu.make_async_copy(a, b, sems.at[i]) for i, (a, b) in enumerate(pairs)]
    for copy in copies:
        copy.start()
    for copy in copies:
        copy.wait()


def by_hidden(ns, nr, inputs, weight_t, states, doc_ids, recur, bias, out_grad):
    T, DI = inputs.shape[1:]
    H = states.shape[2]
    nh, nz, nx = 2 * nr, ns // 2, nr // 2
    hb, cw = H // nh, DI // nr
    L = nh * T
    vm = pltpu.VMEM
    scratch = [
        vm(weight_t.shape, BF16),
        vm((T, H), F32),
        vm((1, T), jnp.int32),
        vm((GATES, H), F32),
        vm((GATES, H), F32),
        vm((T, H), BF16),
        vm((nh, T + 16, hb), BF16),
        vm((nh, T + 16, hb), BF16),
        vm((nh, T, hb), BF16),
        vm((8, H), F32),
        vm((8, H), F32),
        vm((nr, 8, hb), F32),
        vm((L, DI), BF16),
        vm((GATES * hb, DI), BF16),
        vm((L + 8 * nh, hb), F32),
        vm((L + 8 * nh, hb), F32),
        vm((L, hb), F32),
        vm((L + 8 * nh, hb), F32),
        vm((GATES, L, hb), F32),
        vm((L + 8 * nh, hb), F32),
        vm((L, hb), F32),
        vm((L, hb), F32),
        vm((L, hb), F32),
        vm((L, hb), F32),
        vm((L, hb), F32),
        vm((L + 8 * nh, hb), F32),
        vm((L + 8 * nh, hb), F32),
        vm((nh, hb), F32),
        vm((2, 8, hb), F32),
        vm((nz, 2, 8, hb), F32),
        vm((L, hb), F32),
        vm((L, GATES * hb), BF16),
        vm((hb, DI // 2), BF16),
        vm((nr, T, DI), BF16),
        vm((nr, T, DI), BF16),
        vm((nr, T, DI), F32),
        vm((3, T, DI), BF16),
        vm((3, T, DI), BF16),
        vm((GATES, hb, DI), F32),
        vm((GATES, hb, DI), BF16),
        vm((GATES, hb, DI), BF16),
        vm((2, hb, DI), BF16),
        vm((GATES, hb, cw), BF16),
        vm((8, hb), F32),
        vm((nz, 8, hb), F32),
        vm((8, hb), F32),
        vm((nh, 8, hb), F32),
    ]
    dma = pltpu.SemaphoreType.DMA
    counts = [
        7, None, nh, GATES, nz - 1, GATES * nr, None, None, None, None, None, None, None, None, None, nz,
        None, 3, None, 5, GATES, GATES * nr, 2 * nr, None, GATES, None, None, None, None, None, None,
    ]
    sems = [dma if n is None else dma((n,)) for n in counts]
    whole = pl.BlockSpec(memory_space=pltpu.VMEM)
    out_in, out_w, out_p = pl.pallas_call(
        functools.partial(kernel, ns, nr),
        out_shape=(
            pltpu.VMEM((T, DI), BF16),
            pltpu.VMEM(weight_t.shape, F32),
            pltpu.VMEM((6, H), F32),
        ),
        in_specs=[pl.BlockSpec(memory_space=pltpu.HBM)] * 7,
        out_specs=(whole,) * 3,
        scratch_shapes=scratch + sems,
        compiler_params=pltpu.CompilerParams(
            collective_id=0, has_side_effects=True, vmem_limit_bytes=56 * 1024 * 1024
        ),
    )(inputs[0], weight_t, states[0], doc_ids, recur, bias, out_grad[0])
    shapes = ((T, DI), BF16), (weight_t.shape, F32), ((6, H), F32)
    out_in, out_w, out_p = pl.pallas_call(
        flush,
        out_shape=tuple(jax.ShapeDtypeStruct(*one) for one in shapes),
        in_specs=[whole] * 3,
        out_specs=(pl.BlockSpec(memory_space=pltpu.HBM),) * 3,
        scratch_shapes=[dma((3,))],
    )(*(pltpu.with_memory_space_constraint(one, pltpu.VMEM) for one in (out_in, out_w, out_p)))
    return out_in[None], out_w, out_p


def fits(ns, nr, inputs, weight_t, states):
    parts, L, DI = inputs.shape
    H = states.shape[2]
    return (
        parts == nr
        and ns == 2 * nr
        and ns % 8 == 0
        and ns == 8
        and L * 2 * nr == H * ns
        and H % (ns * 128) == 0
        and DI % (nr * 128) == 0
        and L % (ns * 128) == 0
        and L * DI <= 1 << 21
    )


def solution(mesh):
    ns, nr = mesh.shape["seq"], mesh.shape["rep"]
    placed = (
        P("rep", "seq", None),
        P("seq", "rep"),
        P("rep", "seq", None),
        P("rep", "seq"),
        P(),
        P(),
        P("rep", "seq", None),
    )

    def run(inputs, weight_t, states, doc_ids, recur, bias, out_grad):
        kernelized = fits(ns, nr, inputs, weight_t, states)
        body = functools.partial(by_hidden, ns, nr) if kernelized else by_tokens
        return jax.shard_map(
            body,
            mesh=mesh,
            in_specs=placed,
            out_specs=(P("rep", "seq", None), P("seq", "rep"), P()),
            check_vma=False,
        )(inputs, weight_t, states, doc_ids, recur, bias, out_grad)

    return run
```

```python
import functools
import math

import jax
import jax.numpy as jnp
from jax import lax
from jax.experimental import pallas as pl
from jax.experimental.pallas import tpu as pltpu
from jax.sharding import PartitionSpec as P

F32 = jnp.float32
BF16 = jnp.bfloat16
GATES = 3


def shifted(block, axis, distance):
    devices = range(lax.axis_size(axis))
    route = [(i - distance, i) for i in devices if i - distance in devices]
    return lax.ppermute(block, axis, route)


def compose(earlier, later):
    return (later[0] * earlier[0], later[1] + later[0] * earlier[1])


def by_tokens(inputs, weight_t, states, doc_ids, recur, bias, out_grad):
    feats = inputs[0]
    hidden_now = states[0]
    ids_float = doc_ids[0].astype(F32)
    count = feats.shape[0]
    width = hidden_now.shape[1]
    columns = lax.all_gather(weight_t, "rep", axis=1, tiled=True)
    contract_last = (((1,), (1,)), ((), ()))
    full_weight = lax.all_gather(columns, "seq", axis=0, tiled=True)
    preact = lax.dot_general(feats, full_weight, contract_last, preferred_element_type=F32)
    tail_state, tail_id = shifted((hidden_now[-1:], ids_float[-1:]), "seq", 1)
    first_same = jnp.where(
        (ids_float[0] == tail_id[0]) & (lax.axis_index("seq") > 0), 1.0, 0.0
    ).astype(F32)
    same = jnp.concatenate([first_same[None], (ids_float[1:] == ids_float[:-1]).astype(F32)])
    prior = jnp.concatenate([tail_state, hidden_now[:-1]], 0) * same[:, None]
    gate_z = jax.nn.sigmoid(preact[:, :width] + recur[0] * prior + bias[0])
    gate_r = jax.nn.sigmoid(preact[:, width : 2 * width] + recur[1] * prior + bias[1])
    gate_c = jnp.tanh(preact[:, 2 * width :] + recur[2] * gate_r * prior + bias[2])
    jacobian = same[:, None] * (
        1.0
        - gate_z
        + (gate_c - prior) * gate_z * (1.0 - gate_z) * recur[0]
        + gate_z
        * (1.0 - gate_c * gate_c)
        * recur[2]
        * (gate_r + prior * gate_r * (1.0 - gate_r) * recur[1])
    )
    upstream = out_grad[0].astype(F32)
    jac_rows, up_rows = (
        lax.all_to_all(jacobian.T, "seq", split_axis=0, concat_axis=1, tiled=True),
        lax.all_to_all(upstream.T, "seq", split_axis=0, concat_axis=1, tiled=True),
    )
    factor = jnp.concatenate([jac_rows[:, 1:], jnp.zeros((jac_rows.shape[0], 1), F32)], 1)
    _, adjoint_rows = lax.associative_scan(compose, (factor, up_rows), reverse=True, axis=1)
    adjoint = lax.all_to_all(adjoint_rows, "seq", split_axis=1, concat_axis=0, tiled=True).T
    grad_z = adjoint * (gate_c - prior) * gate_z * (1.0 - gate_z)
    grad_c = adjoint * gate_z * (1.0 - gate_c * gate_c)
    grad_r = grad_c * recur[2] * prior * gate_r * (1.0 - gate_r)
    grad_pre = jnp.concatenate([grad_z, grad_r, grad_c], 1).astype(BF16)
    input_grad = jnp.dot(grad_pre, full_weight, preferred_element_type=F32)
    tokens_all = count * inputs.shape[0] * lax.axis_size("seq") * lax.axis_size("rep")
    normal_factor = 1.0 / math.sqrt(tokens_all)
    row_share = lax.psum_scatter(
        lax.dot_general(grad_pre, feats, (((0,), (0,)), ((), ())), preferred_element_type=F32),
        "seq",
        scatter_dimension=0,
        tiled=True,
    )
    weight_grad = (
        lax.psum_scatter(row_share.astype(BF16), "rep", scatter_dimension=1, tiled=True).astype(F32)
        * normal_factor
    )
    stats = jnp.stack(
        [
            grad_z.sum(0),
            grad_r.sum(0),
            grad_c.sum(0),
            (grad_z * prior).sum(0),
            (grad_r * prior).sum(0),
            (grad_c * gate_r * prior).sum(0),
        ]
    )
    param_grad = lax.psum(stats, ("seq", "rep")) * normal_factor
    return (input_grad.astype(BF16)[None], weight_grad, param_grad)


def kernel(
    ns, nr, feats_hbm, weight_hbm, states_hbm, ids_hbm, recur_hbm, bias_hbm, upstream_hbm,
    out_in, out_w, out_p,
    weight, states, ids, recur, bias, upstream,
    pay_src, pay, up_in, tail_src, tail_mid, tail_in, x_all, w_all, prev, ids_col, same_all, up,
    pre, jac, co_z, co_r, co_c, rprior, prior_all,
    scan_a, scan_b, carry, seg_out, seg_in, lam, grads, wg_via, part_out, part_in, part_keep, fin_out, fin_in,
    wg_own, wg_out, wg_end, wg_mid, wg_in, st_out, st_z, st_sum, st_all,
    l_s, x_s, x_r, w_s, w_f, w_r, p_s, p_r, v_s, v_r, e_s, e_r, n_s, n_r, c_s, c_r,
    d_s, d_r, f_s, f_r, g_s, g_e, g_m, g_f, g_r, t_s, t_r, u_s, u_r, h_s, h_r,
):
    T, DI = feats_hbm.shape
    H = states.shape[1]
    nh, nz, nx = 2 * nr, ns // 2, nr // 2
    hb, cw = H // nh, DI // nr
    s, r = lax.axis_index("seq"), lax.axis_index("rep")
    z, y, x, c = s // 2, s % 2, r // 2, r % 2
    q = 2 * r + y
    k = nx * 2 * c + 2 * x + y
    half, per = nz // 2, GATES * nh // nz
    high = z // half
    inner = jnp.logical_or(z == half - 1, z == half)
    end = high * (nz - 1)
    unsent = []

    def place(a, b):
        return {"seq": a, "rep": b}

    def at(plane, j):
        return place(2 * plane + j % 2, 2 * (j // 2 % nx) + j // (2 * nx))

    def column(plane):
        return place(2 * plane + y, r)

    def send(src, dst, ssem, rsem, where):
        pltpu.make_async_remote_copy(
            src_ref=src, dst_ref=dst, send_sem=ssem, recv_sem=rsem,
            device_id=where, device_id_type=pl.DeviceIdType.MESH,
        ).start()

    def local(src, dst, rsem):
        pltpu.make_async_copy(src, dst, rsem).start()

    def landed(dst, sem):
        pltpu.make_async_copy(dst, dst, sem).wait()

    def send_if(allowed, *args):
        pl.when(allowed)(functools.partial(send, *args))

    def send_or_local(src, dst, ssem, rsem, where, here):
        send_if(jnp.logical_not(here), src, dst, ssem, rsem, where)
        pl.when(here)(functools.partial(local, src, dst, rsem))

    def rows(ref, block, count):
        return ref.at[pl.ds(pl.multiple_of(block * count, count), count), :]

    barrier = pltpu.get_barrier_semaphore()

    def greet(where):
        pl.semaphore_signal(barrier, inc=1, device_id=where, device_id_type=pl.DeviceIdType.MESH)

    for j in range(nh):
        pl.when(j != k)(functools.partial(greet, at(z, j)))
    for plane in range(nz):
        pl.when(plane != z)(functools.partial(greet, column(plane)))
    loads = [
        (weight_hbm, weight), (feats_hbm, rows(x_all, q, T)), (states_hbm, states), (ids_hbm, ids),
        (upstream_hbm, upstream), (recur_hbm, recur), (bias_hbm, bias),
    ]
    for n, (src, dst) in enumerate(loads):
        local(src, dst, l_s.at[n])

    def loaded(n):
        landed(loads[n][1], l_s.at[n])

    def piece(g, col):
        return w_all.at[pl.ds(pl.multiple_of(g * hb, hb), hb), col]

    loaded(0)
    pl.semaphore_wait(barrier, nh - 1 + nz - 1)

    mine = pl.ds(pl.multiple_of(r * cw, cw), cw)
    for i in range(GATES):
        b = GATES * s + i
        g, j = b // nh, b % nh
        part = weight.at[i * hb : (i + 1) * hb, :]
        send_or_local(part, piece(g, mine), w_s.at[i], w_r.at[g * nr + r], at(z, j), j == k)
        unsent.append((j != k, part, w_s.at[i]))

    partner = place(s, r + 1 - 2 * c)
    nearest = place(2 * z + (y + c) % 2, 2 * ((x + 1 - c) % nx) + c)
    across = place(2 * z + (y + 1 - c) % 2, 2 * ((x + c) % nx) + c)

    def features(dx, dy, core):
        return 2 * (2 * ((x + dx) % nx) + (c + core) % 2) + (y + dy) % 2

    def share(dx, dy, targets):
        slot = features(dx, dy, 0)
        block = rows(x_all, slot, T)
        for where in targets:
            send(block, block, x_s, x_r.at[slot], where)

    loaded(1)
    share(0, 0, (nearest, across, partner))
    unsent.append((True, x_all.at[0 : (nh - 1) * T, :], x_s))

    loaded(2)
    loaded(3)
    tail_src[0:4, :] = jnp.broadcast_to(states[T - 1 : T, :], (4, H))
    tail_src[4:8, :] = jnp.broadcast_to(ids[0:1, T - 1 : T].astype(F32), (4, H))
    hands_on = jnp.logical_and(y == 1, z < nz - 1)
    takes_over = jnp.logical_and(y == 1, z > 0)
    send_if(hands_on, tail_src, tail_mid, n_s, n_r, column((z + 1) % nz))
    unsent.append((hands_on, tail_src, n_s))
    for j in range(nh):
        pay_src[j, 0:T, :] = states[:, j * hb : (j + 1) * hb].astype(BF16)
        pay_src[j, T:, :] = jnp.broadcast_to(ids[...].astype(F32), (16, hb)).astype(BF16)
    for j in range(nh):
        send_or_local(pay_src.at[j], pay.at[q], p_s, p_r, at(z, j), k == j)
    unsent.append((True, pay.at[0 : nh - 1], p_s))

    def origin(step):
        plane = (z + (1 - 2 * high) * step + nz) % nz
        g = (per * plane - k + nh - 1) // nh
        return plane, g % GATES, jnp.logical_and(g < GATES, nh * g + k < per * (plane + 1))

    order = []
    for n in range(nr):
        chip = (x + n // 2) % nx
        order.append(2 * chip + (c + n) % 2)

    def spread(step, numbers):
        plane, g, found = origin(step)
        outer = jnp.logical_and(found, jnp.logical_not(inner))
        within = jnp.logical_and(found, inner)
        far, near = column(half - high), column(z + 1 - 2 * (z % half))
        for n in numbers:
            block = piece(g, pl.ds(pl.multiple_of(order[n] * cw, cw), cw))
            sem = w_r.at[g * nr + order[n]]
            if step == 0:
                pl.when(found)(functools.partial(landed, block, sem))
                send_if(found, block, block, w_f.at[0], sem, far)
                send_if(within, block, block, w_f.at[0], sem, near)
            else:
                pl.when(within)(functools.partial(landed, block, sem))
                send_if(within, block, block, w_f.at[step], sem, column(end))
        if step == 0:
            for n in numbers:
                block = piece(g, pl.ds(pl.multiple_of(order[n] * cw, cw), cw))
                send_if(outer, block, block, w_f.at[0], w_r.at[g * nr + order[n]], near)
            unsent.append((found, w_all.at[0 : 2 * hb, :], w_f.at[0]))
        elif numbers[-1] == nr - 1:
            unsent.append((within, w_all.at[0:hb, :], w_f.at[step]))

    def relay(dx, dy, targets):
        slot = features(dx, dy, 0)
        landed(rows(x_all, slot, T), x_r.at[slot])
        share(dx, dy, targets)

    spread(0, range(nr))
    pl.when(takes_over)(functools.partial(landed, tail_mid, n_r))
    for j in range(nh):
        part = tail_mid.at[:, j * hb : (j + 1) * hb]
        here = j == k
        send_if(jnp.logical_and(takes_over, j != k), part, tail_in.at[r], e_s, e_r, at(z, j))
        pl.when(jnp.logical_and(takes_over, here))(functools.partial(local, part, tail_in.at[r], e_r))
    unsent.append((takes_over, st_all.at[0 : nh - 1], e_s))
    spread(1, range(nr // 2))
    relay(c, 1 - c, (nearest, partner))
    spread(1, range(nr // 2, nr))
    relay(1 - c, c, (partner,))
    loaded(4)

    def send_upstream(early):
        for j in range(nh):
            part = upstream.at[:, j * hb : (j + 1) * hb]
            over_x, over_y = j // 2 % nx != x, j % 2 != y
            other_link = jnp.where(c == 0, jnp.logical_and(over_y, jnp.logical_not(over_x)), over_x)
            now = jnp.logical_not(other_link) if early else other_link
            send_if(jnp.logical_and(now, j != k), part, up_in.at[q], v_s, v_r, at(z, j))
            if early:
                pl.when(j == k)(functools.partial(local, part, up_in.at[q], v_r))

    unsent.append((True, up_in.at[0 : nh - 1], v_s))
    send_upstream(True)
    spread(2, range(nr))

    stride = T + 8
    landed(pay, p_r)
    pl.when(z > 0)(functools.partial(landed, tail_in, e_r))
    for m in range(nh):
        base = m * stride + 8
        span = slice(m * T, (m + 1) * T)
        prev[base : base + T, :] = pay[m, 0:T, :].astype(F32)
        ids_row = pay[m, T:, :].astype(F32)[0:1, :]
        ids_col[base : base + T, :] = jnp.broadcast_to(ids_row, (hb, T)).T
        if m % 2:
            before = base - stride + T - 1
            prev[base - 1 : base, :] = prev[before : before + 1, :]
            ids_col[base - 1 : base, :] = ids_col[before : before + 1, :]
        else:

            @pl.when(z > 0)
            def _():
                prev[base - 1 : base, :] = tail_in[m // 2, 0:1, :]
                ids_col[base - 1 : base, :] = tail_in[m // 2, 4:5, :]

            @pl.when(z == 0)
            def _():
                prev[base - 1 : base, :] = jnp.zeros((1, hb), F32)
                ids_col[base - 1 : base, :] = jnp.full((1, hb), -1.0, F32)

        same = jnp.where(
            ids_col[base : base + T, :] == ids_col[base - 1 : base - 1 + T, :], 1.0, 0.0
        )
        same_all[span, :] = same
        prior_all[span, :] = prev[base - 1 : base - 1 + T, :] * same

    loaded(5)
    loaded(6)
    (_, g0, found0), (_, g1, _), (_, g2, _), (_, g3, found3) = (origin(step) for step in range(nz))
    own, wide = found0.astype(jnp.int32), found3.astype(jnp.int32)
    early = own * g0 + (1 - own) * g1
    late = wide * g3 + (1 - wide) * g2
    middle = (GATES - early - late) % GATES
    outer = jnp.logical_not(inner)

    def arrived(g, unseen):
        for col in range(nr):
            block = piece(g, slice(col * cw, (col + 1) * cw))
            pl.when(unseen)(functools.partial(landed, block, w_r.at[g * nr + col]))

    def project(span, g):
        return lax.dot_general(
            x_all[span, :], piece(g, slice(None))[...], (((1,), (1,)), ((), ())),
            preferred_element_type=F32,
        )

    def ahead(blocks):
        for m in blocks:
            span = pl.ds(pl.multiple_of(m * T, T), T)
            for g in (early, middle):
                pre[g, span, :] = project(span, g)

    hops = [(0, 0), (0, 1), (1, 0), (1, 1)]
    for dx, dy in hops[:3]:
        m = features(dx, dy, 1)
        landed(rows(x_all, m, T), x_r.at[m])
    arrived(early, jnp.logical_and(jnp.logical_not(found0), outer))
    arrived(middle, outer)
    ahead([features(dx, dy, core) for dx, dy in hops[:3] for core in range(2)])
    send_upstream(False)
    relay(1, 1, (partner,))
    group = pl.ds(pl.multiple_of(k * hb, hb), hb)
    rz, rr, rc = (recur[i : i + 1, group] for i in range(GATES))
    bz, br, bc = (bias[i : i + 1, group] for i in range(GATES))

    def gates(blocks):
        for m in blocks:
            whole = isinstance(m, int)
            span = slice(m * T, (m + 1) * T) if whole else pl.ds(pl.multiple_of(m * T, T), T)
            wide = slice(m * stride, m * stride + T) if whole else pl.ds(pl.multiple_of(m * stride, 8), T)
            last = project(span, late)
            pz, pr, pc = (jnp.where(late == i, last, pre[i, span, :]) for i in range(GATES))
            prior = prior_all[span, :]
            gz = jax.nn.sigmoid(pz + rz * prior + bz)
            gr = jax.nn.sigmoid(pr + rr * prior + br)
            rp = gr * prior
            gc = jnp.tanh(pc + rc * rp + bc)
            az = (gc - prior) * gz * (1.0 - gz)
            ac = gz * (1.0 - gc * gc)
            slope = rp * (1.0 - gr)
            acr = ac * rc
            co_z[span, :] = az
            co_c[span, :] = ac
            co_r[span, :] = acr * slope
            rprior[span, :] = rp
            jac[wide, :] = same_all[span, :] * (1.0 - gz + az * rz + acr * (gr + slope * rr))

    def rest():
        m = features(1, 1, 1)
        landed(rows(x_all, m, T), x_r.at[m])
        ahead([m])

    ahead([features(1, 1, 0)])
    missing = jnp.logical_or(found3, outer)

    @pl.when(c == 1)
    def _():
        arrived(late, missing)
        gates([features(dx, dy, core) for dx, dy in hops[:3] for core in range(2)])
        rest()
        gates([features(1, 1, core) for core in range(2)])

    @pl.when(c == 0)
    def _():
        rest()
        arrived(late, missing)
        gates(range(nh))

    landed(up_in, v_r)
    for m in range(nh):
        up[m * stride : m * stride + T, :] = up_in[m].astype(F32)

    def back(i, state):
        a, b = state
        t = T - 1 - i
        f = jac[pl.ds(t, nh, stride=stride), :]
        b = b + up[pl.ds(t, nh, stride=stride), :]
        scan_a[pl.ds(t, nh, stride=stride), :] = a
        scan_b[pl.ds(t, nh, stride=stride), :] = b
        return f * a, f * b

    a, b = lax.fori_loop(0, T, back, (jnp.ones((nh, hb), F32), jnp.zeros((nh, hb), F32)), unroll=8)
    seg_out[...] = jnp.zeros(seg_out.shape, F32)
    for o in range(nr):
        first, second = slice(2 * o, 2 * o + 1), slice(2 * o + 1, 2 * o + 2)
        seg_out[0, o : o + 1, :] = a[first, :] * a[second, :]
        seg_out[1, o : o + 1, :] = b[first, :] + a[first, :] * b[second, :]
    for plane in range(nz - 1):
        send_if(plane < z, seg_out, seg_in.at[z], c_s, c_r.at[z], at(plane, k))
        unsent.append((z == plane + 1, seg_in.at[0 : plane + 1], c_s))
    carry[...] = jnp.zeros(carry.shape, F32)
    for plane in reversed(range(1, nz)):

        @pl.when(plane > z)
        def _():
            landed(seg_in.at[plane], c_r.at[plane])
            carry[0:nr, :] = seg_in[plane, 1, 0:nr, :] + seg_in[plane, 0, 0:nr, :] * carry[0:nr, :]

    into = carry[0:nr, :]
    carry_rows = []
    for o in range(nr):
        later = into[o : o + 1, :]
        second = slice(2 * o + 1, 2 * o + 2)
        carry_rows += [b[second, :] + a[second, :] * later, later]
    carried = jnp.concatenate(carry_rows, 0)

    for m in range(nh):
        span = slice(m * T, (m + 1) * T)
        padded = slice(m * stride, m * stride + T)
        adj = scan_b[padded, :] + scan_a[padded, :] * carried[m : m + 1, :]
        lam[span, :] = adj
        for g, slope in enumerate((co_z, co_r, co_c)):
            grads[span, g * hb : (g + 1) * hb] = (adj * slope[span, :]).astype(BF16)

    def quarter(col):
        return pl.ds(pl.multiple_of(col * cw, cw), cw)

    away = [2 * ((x + 1 + n // 2) % nx) + n % 2 for n in range(nr)]

    def side(n):
        return pl.ds(pl.multiple_of(2 * ((x + n) % nx) * cw, 2 * cw), 2 * cw)

    def gate_of(step):
        g = high * step + (1 - high) * (GATES - 1 - step)
        return g, (nh * g + k) // per

    def short(hidden):
        g = (per * z - hidden + nh - 1) // nh
        have = jnp.logical_and(g < GATES, nh * g + hidden < per * (z + 1))
        return jnp.logical_and(outer, jnp.logical_not(have))

    other = 2 * nx * c + 2 * ((x + 1) % nx) + y
    lacks, helps = short(k), short(other)
    beside = place(s, 2 * ((x + 1) % nx) + c)
    hub = high + half - 1

    near = inner.astype(jnp.int32)
    turns = (
        (GATES - 1) * (high * near + (1 - high) * (1 - near)),
        (GATES - 1) * (1 - high) * near + 1 - near,
        near + (GATES - 1) * high * (1 - near),
    )

    def statistics():
        sums = [jnp.zeros((1, hb), F32) for _ in range(6)]
        for m in range(nh):
            span = slice(m * T, (m + 1) * T)
            prior = prior_all[span, :]
            adj = lam[span, :]
            grad_z = adj * co_z[span, :]
            grad_r = adj * co_r[span, :]
            grad_c = adj * co_c[span, :]
            terms = (grad_z, grad_r, grad_c, grad_z * prior, grad_r * prior, grad_c * rprior[span, :])
            sums = [total + jnp.sum(term, 0, keepdims=True) for total, term in zip(sums, terms)]
        for i in range(6):
            st_out[i : i + 1, :] = sums[i]
        st_out[6:8, :] = jnp.zeros((2, hb), F32)
        st_z[z] = st_out[...]
        for plane in range(nz):
            send_if(plane != z, st_out, st_z.at[z], t_s, t_r, column(plane))
        unsent.append((True, st_z.at[0 : nz - 1], t_s))

    def weigh(step):
        g = turns[step]
        plane = (nh * g + k) // per
        spans = (side(1), side(0)) if step == 0 else (slice(0, DI),)

        def product(span):
            block = lax.dot_general(
                grads[:, pl.ds(pl.multiple_of(g * hb, hb), hb)], x_all[:, span], (((0,), (0,)), ((), ())),
                preferred_element_type=F32,
            )
            wg_own[g, :, span] = block
            wg_out[g, :, span] = block.astype(BF16)

        product(spans[0])
        outward = jnp.logical_and(inner, plane == end)
        inward = jnp.logical_and(outer, plane != z)
        for n, col in enumerate(away):
            if step == 0 and n == 1:
                give(0)
                statistics()
                product(spans[1])
            part = wg_out.at[g, :, quarter(col)]
            send_if(
                jnp.logical_and(inward, plane != hub), part, wg_end.at[g, :, quarter(col)], g_s.at[g],
                g_e.at[g * nr + col], column(hub),
            )
            send_if(
                outward, part, wg_mid.at[0, :, quarter(col)], g_s.at[g], g_m.at[col], column(end),
            )
        if step == GATES - 1:
            send_if(lacks, wg_out.at[g, :, side(0)], wg_via, g_s.at[g], h_r, beside)
        unsent.append((plane != z, wg_out.at[g], g_s.at[g]))

    def nearby(step):
        g, plane = gate_of(step)
        for n, col in enumerate(away):
            go = jnp.logical_and(outer, plane == hub)
            if step == GATES - 1 and n >= nr // 2:
                go = jnp.logical_and(go, jnp.logical_not(lacks))
            send_if(
                go, wg_out.at[g, :, quarter(col)], wg_end.at[g, :, quarter(col)], g_s.at[g],
                g_e.at[g * nr + col], column(hub),
            )

    def assist():
        g, _ = gate_of(GATES - 1)
        pl.when(helps)(functools.partial(landed, wg_via, h_r))
        for n in range(nr // 2):
            col = 2 * ((x + 1) % nx) + n
            part = wg_via.at[:, n * cw : (n + 1) * cw]
            where = place(2 * hub + y, 2 * ((x + 1) % nx) + c)
            send_if(helps, part, wg_end.at[g, :, quarter(col)], h_s, g_e.at[g * nr + col], where)
        unsent.append((helps, wg_via, h_s))

    chips = [(x + 1, y + 1), (x + 1, y), (x, y + 1), (x, y)]
    lot = (0, 1, 1, 2)

    def tokens(n, core):
        return rows(grads, 2 * (2 * (chips[n][0] % nx) + core) + chips[n][1] % 2, T)[...]

    def give(n):
        part_out[n] = jnp.dot(tokens(n, 1 - c), w_all[...], preferred_element_type=F32).astype(BF16)
        send(part_out.at[n], part_in.at[n], d_s, d_r.at[lot[n]], partner)

    def keep(n):
        part_keep[n] = jnp.dot(tokens(n, c), w_all[...], preferred_element_type=F32)

    def both(n):
        return part_keep[n] + part_in[n].astype(F32)

    parts = [slice(n * T // 2, (n + 1) * T // 2) for n in range(2)]
    scale = 1.0 / math.sqrt(ns * nr * T)

    def gather_stats():
        landed(st_z.at[0 : nz - 1], t_r)
        total = st_z[0]
        for plane in range(1, nz):
            total = total + st_z[plane]
        st_sum[...] = total * scale
        st_all[k] = st_sum[...]
        for j in range(nh):
            send_if(j != k, st_sum, st_all.at[k], u_s, u_r, at(z, j))
        unsent.append((True, st_all.at[0 : nh - 1], u_s))

    def turn(n):
        part = parts[n]
        landed(fin_in.at[0, part], f_r.at[n])
        total = part_keep[2 - c, part] + part_in[2 - c, part].astype(F32) + fin_in[0, part].astype(F32)
        fin_out[2, part] = total.astype(BF16)
        send(fin_out.at[2, part], fin_in.at[2, part], f_s, f_r.at[3 + n], across)

    def hand_on(step, numbers):
        g, plane = gate_of(step)
        passed = jnp.logical_and(inner, jnp.logical_and(plane != z, plane != end))
        far = (plane // half != high) & ((plane == 0) | (plane == nz - 1))
        for col in (away[n] for n in numbers):
            cols = quarter(col)

            @pl.when(passed)
            def _():
                landed(wg_end.at[g, :, cols], g_e.at[g * nr + col])
                wg_out[g, :, cols] = (wg_own[g, :, cols] + wg_end[g, :, cols].astype(F32)).astype(BF16)

            for slot, there in enumerate((jnp.logical_not(far), far)):
                send_if(
                    jnp.logical_and(passed, there), wg_out.at[g, :, cols], wg_mid.at[slot, :, cols],
                    g_s.at[g], g_m.at[slot * nr + col], column(plane),
                )

    weigh(0)
    keep(0)
    weigh(1)
    landed(part_in.at[0], d_r.at[0])
    fin_out[0] = both(0).astype(BF16)
    for n, part in enumerate(parts):
        send(fin_out.at[0, part], fin_in.at[0, part], f_s, f_r.at[n], nearest)
    give(1)
    give(2)
    weigh(2)
    hand_on(0, (0,))
    keep(1)
    keep(2)
    landed(part_in.at[1:3], d_r.at[1])
    fin_out[1] = both(1 + c).astype(BF16)
    send(fin_out.at[1], fin_in.at[1], f_s, f_r.at[2], nearest)
    hand_on(0, (1,))
    give(3)
    keep(3)
    hand_on(0, (2,))
    turn(0)
    hand_on(0, (3,))
    gather_stats()
    turn(1)
    for n in range(GATES):
        nearby(n)
    assist()
    for step in range(1, GATES):
        hand_on(step, range(nr))
    unsent.append((True, part_out, d_s))
    unsent.append((True, fin_out, f_s))

    _, g, found = origin(0)
    b = nh * g + k
    owner, i = b // GATES, b % GATES
    for col in away:
        cols = quarter(col)

        @pl.when(found)
        def _():
            landed(wg_mid.at[0, :, cols], g_m.at[col])
            wg_own[g, :, cols] = wg_own[g, :, cols] + wg_mid[0, :, cols].astype(F32)

        @pl.when(jnp.logical_and(found, inner))
        def _():
            landed(wg_end.at[g, :, cols], g_e.at[g * nr + col])
            wg_own[g, :, cols] = wg_own[g, :, cols] + wg_end[g, :, cols].astype(F32)

        @pl.when(jnp.logical_and(found, outer))
        def _():
            landed(wg_mid.at[1, :, cols], g_m.at[nr + col])
            wg_own[g, :, cols] = wg_own[g, :, cols] + wg_mid[1, :, cols].astype(F32)

        @pl.when(found)
        def _():
            wg_out[g, :, cols] = wg_own[g, :, cols].astype(BF16)

        here = jnp.logical_and(owner == s, r == col)

        @pl.when(jnp.logical_and(found, here))
        def _():
            local(wg_out.at[g, :, cols], wg_in.at[i], g_r.at[i])

        send_if(
            jnp.logical_and(found, jnp.logical_not(here)), wg_out.at[g, :, cols], wg_in.at[i],
            g_f, g_r.at[i], place(owner, col),
        )
    unsent.append((jnp.logical_and(found, owner != s), wg_out.at[0], g_f))
    unsent.append((jnp.logical_and(found, owner == s), wg_out.at[0, :, 0 : (nr - 1) * cw], g_f))

    landed(st_all.at[0 : nh - 1], u_r)
    for j in range(nh):
        out_p[:, j * hb : (j + 1) * hb] = st_all[j, :6, :]

    landed(part_in.at[3], d_r.at[2])
    total = both(3)
    landed(fin_in.at[1], f_r.at[2])
    for n, part in enumerate(parts):
        landed(fin_in.at[2, part], f_r.at[3 + n])
    total = total + fin_in[1].astype(F32) + fin_in[2].astype(F32)
    out_in[...] = total.astype(BF16)

    for i in range(GATES):
        landed(wg_in.at[i], g_r.at[i])
        block = slice(i * hb, (i + 1) * hb)
        out_w[block, :] = wg_in[i].astype(F32) * scale

    for sent, src, sem in unsent:
        if sent is True:
            landed(src, sem)
        else:

            @pl.when(sent)
            def _():
                landed(src, sem)


def flush(in_a, in_b, in_c, out_a, out_b, out_c, sems):
    pairs = [(in_a, out_a), (in_b, out_b), (in_c, out_c)]
    copies = [pltpu.make_async_copy(a, b, sems.at[i]) for i, (a, b) in enumerate(pairs)]
    for copy in copies:
        copy.start()
    for copy in copies:
        copy.wait()


def by_hidden(ns, nr, inputs, weight_t, states, doc_ids, recur, bias, out_grad):
    T, DI = inputs.shape[1:]
    H = states.shape[2]
    nh, nz, nx = 2 * nr, ns // 2, nr // 2
    hb, cw = H // nh, DI // nr
    L = nh * T
    vm = pltpu.VMEM
    scratch = [
        vm(weight_t.shape, BF16),
        vm((T, H), F32),
        vm((1, T), jnp.int32),
        vm((GATES, H), F32),
        vm((GATES, H), F32),
        vm((T, H), BF16),
        vm((nh, T + 16, hb), BF16),
        vm((nh, T + 16, hb), BF16),
        vm((nh, T, hb), BF16),
        vm((8, H), F32),
        vm((8, H), F32),
        vm((nr, 8, hb), F32),
        vm((L, DI), BF16),
        vm((GATES * hb, DI), BF16),
        vm((L + 8 * nh, hb), F32),
        vm((L + 8 * nh, hb), F32),
        vm((L, hb), F32),
        vm((L + 8 * nh, hb), F32),
        vm((GATES, L, hb), F32),
        vm((L + 8 * nh, hb), F32),
        vm((L, hb), F32),
        vm((L, hb), F32),
        vm((L, hb), F32),
        vm((L, hb), F32),
        vm((L, hb), F32),
        vm((L + 8 * nh, hb), F32),
        vm((L + 8 * nh, hb), F32),
        vm((nh, hb), F32),
        vm((2, 8, hb), F32),
        vm((nz, 2, 8, hb), F32),
        vm((L, hb), F32),
        vm((L, GATES * hb), BF16),
        vm((hb, DI // 2), BF16),
        vm((nr, T, DI), BF16),
        vm((nr, T, DI), BF16),
        vm((nr, T, DI), F32),
        vm((3, T, DI), BF16),
        vm((3, T, DI), BF16),
        vm((GATES, hb, DI), F32),
        vm((GATES, hb, DI), BF16),
        vm((GATES, hb, DI), BF16),
        vm((2, hb, DI), BF16),
        vm((GATES, hb, cw), BF16),
        vm((8, hb), F32),
        vm((nz, 8, hb), F32),
        vm((8, hb), F32),
        vm((nh, 8, hb), F32),
    ]
    dma = pltpu.SemaphoreType.DMA
    counts = [
        7, None, nh, GATES, nz - 1, GATES * nr, None, None, None, None, None, None, None, None, None, nz,
        None, 3, None, 5, GATES, GATES * nr, 2 * nr, None, GATES, None, None, None, None, None, None,
    ]
    sems = [dma if n is None else dma((n,)) for n in counts]
    whole = pl.BlockSpec(memory_space=pltpu.VMEM)
    out_in, out_w, out_p = pl.pallas_call(
        functools.partial(kernel, ns, nr),
        out_shape=(
            pltpu.VMEM((T, DI), BF16),
            pltpu.VMEM(weight_t.shape, F32),
            pltpu.VMEM((6, H), F32),
        ),
        in_specs=[pl.BlockSpec(memory_space=pltpu.HBM)] * 7,
        out_specs=(whole,) * 3,
        scratch_shapes=scratch + sems,
        compiler_params=pltpu.CompilerParams(
            collective_id=0, has_side_effects=True, vmem_limit_bytes=56 * 1024 * 1024
        ),
    )(inputs[0], weight_t, states[0], doc_ids, recur, bias, out_grad[0])
    shapes = ((T, DI), BF16), (weight_t.shape, F32), ((6, H), F32)
    out_in, out_w, out_p = pl.pallas_call(
        flush,
        out_shape=tuple(jax.ShapeDtypeStruct(*one) for one in shapes),
        in_specs=[whole] * 3,
        out_specs=(pl.BlockSpec(memory_space=pltpu.HBM),) * 3,
        scratch_shapes=[dma((3,))],
    )(*(pltpu.with_memory_space_constraint(one, pltpu.VMEM) for one in (out_in, out_w, out_p)))
    return out_in[None], out_w, out_p


def fits(ns, nr, inputs, weight_t, states):
    parts, L, DI = inputs.shape
    H = states.shape[2]
    return (
        parts == nr
        and ns == 2 * nr
        and ns % 8 == 0
        and ns == 8
        and L * 2 * nr == H * ns
        and H % (ns * 128) == 0
        and DI % (nr * 128) == 0
        and L % (ns * 128) == 0
        and L * DI <= 1 << 21
    )


def solution(mesh):
    ns, nr = mesh.shape["seq"], mesh.shape["rep"]
    placed = (
        P("rep", "seq", None),
        P("seq", "rep"),
        P("rep", "seq", None),
        P("rep", "seq"),
        P(),
        P(),
        P("rep", "seq", None),
    )

    def run(inputs, weight_t, states, doc_ids, recur, bias, out_grad):
        kernelized = fits(ns, nr, inputs, weight_t, states)
        body = functools.partial(by_hidden, ns, nr) if kernelized else by_tokens
        return jax.shard_map(
            body,
            mesh=mesh,
            in_specs=placed,
            out_specs=(P("rep", "seq", None), P("seq", "rep"), P()),
            check_vma=False,
        )(inputs, weight_t, states, doc_ids, recur, bias, out_grad)

    return run
```

```python
import functools
import math

import jax
import jax.numpy as jnp
from jax import lax
from jax.experimental import pallas as pl
from jax.experimental.pallas import tpu as pltpu
from jax.sharding import PartitionSpec as P

F32 = jnp.float32
BF16 = jnp.bfloat16
GATES = 3


def shifted(block, axis, distance):
    devices = range(lax.axis_size(axis))
    route = [(i - distance, i) for i in devices if i - distance in devices]
    return lax.ppermute(block, axis, route)


def compose(earlier, later):
    return (later[0] * earlier[0], later[1] + later[0] * earlier[1])


def by_tokens(inputs, weight_t, states, doc_ids, recur, bias, out_grad):
    feats = inputs[0]
    hidden_now = states[0]
    ids_float = doc_ids[0].astype(F32)
    count = feats.shape[0]
    width = hidden_now.shape[1]
    columns = lax.all_gather(weight_t, "rep", axis=1, tiled=True)
    contract_last = (((1,), (1,)), ((), ()))
    full_weight = lax.all_gather(columns, "seq", axis=0, tiled=True)
    preact = lax.dot_general(feats, full_weight, contract_last, preferred_element_type=F32)
    tail_state, tail_id = shifted((hidden_now[-1:], ids_float[-1:]), "seq", 1)
    first_same = jnp.where(
        (ids_float[0] == tail_id[0]) & (lax.axis_index("seq") > 0), 1.0, 0.0
    ).astype(F32)
    same = jnp.concatenate([first_same[None], (ids_float[1:] == ids_float[:-1]).astype(F32)])
    prior = jnp.concatenate([tail_state, hidden_now[:-1]], 0) * same[:, None]
    gate_z = jax.nn.sigmoid(preact[:, :width] + recur[0] * prior + bias[0])
    gate_r = jax.nn.sigmoid(preact[:, width : 2 * width] + recur[1] * prior + bias[1])
    gate_c = jnp.tanh(preact[:, 2 * width :] + recur[2] * gate_r * prior + bias[2])
    jacobian = same[:, None] * (
        1.0
        - gate_z
        + (gate_c - prior) * gate_z * (1.0 - gate_z) * recur[0]
        + gate_z
        * (1.0 - gate_c * gate_c)
        * recur[2]
        * (gate_r + prior * gate_r * (1.0 - gate_r) * recur[1])
    )
    upstream = out_grad[0].astype(F32)
    jac_rows, up_rows = (
        lax.all_to_all(jacobian.T, "seq", split_axis=0, concat_axis=1, tiled=True),
        lax.all_to_all(upstream.T, "seq", split_axis=0, concat_axis=1, tiled=True),
    )
    factor = jnp.concatenate([jac_rows[:, 1:], jnp.zeros((jac_rows.shape[0], 1), F32)], 1)
    _, adjoint_rows = lax.associative_scan(compose, (factor, up_rows), reverse=True, axis=1)
    adjoint = lax.all_to_all(adjoint_rows, "seq", split_axis=1, concat_axis=0, tiled=True).T
    grad_z = adjoint * (gate_c - prior) * gate_z * (1.0 - gate_z)
    grad_c = adjoint * gate_z * (1.0 - gate_c * gate_c)
    grad_r = grad_c * recur[2] * prior * gate_r * (1.0 - gate_r)
    grad_pre = jnp.concatenate([grad_z, grad_r, grad_c], 1).astype(BF16)
    input_grad = jnp.dot(grad_pre, full_weight, preferred_element_type=F32)
    tokens_all = count * inputs.shape[0] * lax.axis_size("seq") * lax.axis_size("rep")
    normal_factor = 1.0 / math.sqrt(tokens_all)
    row_share = lax.psum_scatter(
        lax.dot_general(grad_pre, feats, (((0,), (0,)), ((), ())), preferred_element_type=F32),
        "seq",
        scatter_dimension=0,
        tiled=True,
    )
    weight_grad = (
        lax.psum_scatter(row_share.astype(BF16), "rep", scatter_dimension=1, tiled=True).astype(F32)
        * normal_factor
    )
    stats = jnp.stack(
        [
            grad_z.sum(0),
            grad_r.sum(0),
            grad_c.sum(0),
            (grad_z * prior).sum(0),
            (grad_r * prior).sum(0),
            (grad_c * gate_r * prior).sum(0),
        ]
    )
    param_grad = lax.psum(stats, ("seq", "rep")) * normal_factor
    return (input_grad.astype(BF16)[None], weight_grad, param_grad)


def kernel(
    ns, nr, feats_hbm, weight_hbm, states_hbm, ids_hbm, recur_hbm, bias_hbm, upstream_hbm,
    out_in, out_w, out_p,
    weight, states, ids, recur, bias, upstream,
    pay_src, pay, up_in, tail_src, tail_mid, tail_in, x_all, w_all, prev, ids_col, same_all, up,
    pre, jac, co_z, co_r, co_c, rprior, prior_all,
    scan_a, scan_b, carry, seg_out, seg_in, lam, grads, wg_via, part_out, part_in, part_keep, fin_out, fin_in,
    wg_own, wg_out, wg_end, wg_mid, wg_in, st_out, st_z, st_sum, st_all,
    l_s, x_s, x_r, w_s, w_f, w_r, p_s, p_r, v_s, v_r, e_s, e_r, n_s, n_r, c_s, c_r,
    d_s, d_r, f_s, f_r, g_s, g_e, g_m, g_f, g_r, t_s, t_r, u_s, u_r, h_s, h_r,
):
    T, DI = feats_hbm.shape
    H = states.shape[1]
    nh, nz, nx = 2 * nr, ns // 2, nr // 2
    hb, cw = H // nh, DI // nr
    s, r = lax.axis_index("seq"), lax.axis_index("rep")
    z, y, x, c = s // 2, s % 2, r // 2, r % 2
    q = 2 * r + y
    k = nx * 2 * c + 2 * x + y
    half, per = nz // 2, GATES * nh // nz
    high = z // half
    inner = jnp.logical_or(z == half - 1, z == half)
    end = high * (nz - 1)
    unsent = []

    def place(a, b):
        return {"seq": a, "rep": b}

    def at(plane, j):
        return place(2 * plane + j % 2, 2 * (j // 2 % nx) + j // (2 * nx))

    def column(plane):
        return place(2 * plane + y, r)

    def send(src, dst, ssem, rsem, where):
        pltpu.make_async_remote_copy(
            src_ref=src, dst_ref=dst, send_sem=ssem, recv_sem=rsem,
            device_id=where, device_id_type=pl.DeviceIdType.MESH,
        ).start()

    def local(src, dst, rsem):
        pltpu.make_async_copy(src, dst, rsem).start()

    def landed(dst, sem):
        pltpu.make_async_copy(dst, dst, sem).wait()

    def send_if(allowed, *args):
        pl.when(allowed)(functools.partial(send, *args))

    def send_or_local(src, dst, ssem, rsem, where, here):
        send_if(jnp.logical_not(here), src, dst, ssem, rsem, where)
        pl.when(here)(functools.partial(local, src, dst, rsem))

    def rows(ref, block, count):
        return ref.at[pl.ds(pl.multiple_of(block * count, count), count), :]

    barrier = pltpu.get_barrier_semaphore()

    def greet(where):
        pl.semaphore_signal(barrier, inc=1, device_id=where, device_id_type=pl.DeviceIdType.MESH)

    for j in range(nh):
        pl.when(j != k)(functools.partial(greet, at(z, j)))
    for plane in range(nz):
        pl.when(plane != z)(functools.partial(greet, column(plane)))
    loads = [
        (weight_hbm, weight), (feats_hbm, rows(x_all, q, T)), (states_hbm, states), (ids_hbm, ids),
        (upstream_hbm, upstream), (recur_hbm, recur), (bias_hbm, bias),
    ]
    for n, (src, dst) in enumerate(loads):
        local(src, dst, l_s.at[n])

    def loaded(n):
        landed(loads[n][1], l_s.at[n])

    def piece(g, col):
        return w_all.at[pl.ds(pl.multiple_of(g * hb, hb), hb), col]

    loaded(0)
    pl.semaphore_wait(barrier, nh - 1 + nz - 1)

    mine = pl.ds(pl.multiple_of(r * cw, cw), cw)
    kept = jnp.int32(0)
    for i in range(GATES):
        b = GATES * s + i
        g, j = b // nh, b % nh
        part = weight.at[i * hb : (i + 1) * hb, :]
        send_or_local(part, piece(g, mine), w_s, w_r.at[g * nr + r], at(z, j), j == k)
        kept = kept + (j == k).astype(jnp.int32)

    unsent.append((kept == 0, weight, w_s))
    unsent.append((kept == 1, weight.at[0 : (GATES - 1) * hb, :], w_s))
    partner = place(s, r + 1 - 2 * c)
    nearest = place(2 * z + (y + c) % 2, 2 * ((x + 1 - c) % nx) + c)
    across = place(2 * z + (y + 1 - c) % 2, 2 * ((x + c) % nx) + c)

    def features(dx, dy, core):
        return 2 * (2 * ((x + dx) % nx) + (c + core) % 2) + (y + dy) % 2

    def share(dx, dy, targets):
        slot = features(dx, dy, 0)
        block = rows(x_all, slot, T)
        for where in targets:
            send(block, block, x_s, x_r.at[slot], where)

    loaded(1)
    share(0, 0, (nearest, across, partner))
    unsent.append((True, x_all.at[0 : (nh - 1) * T, :], x_s))

    loaded(2)
    loaded(3)
    tail_src[0:4, :] = jnp.broadcast_to(states[T - 1 : T, :], (4, H))
    tail_src[4:8, :] = jnp.broadcast_to(ids[0:1, T - 1 : T].astype(F32), (4, H))
    hands_on = jnp.logical_and(y == 1, z < nz - 1)
    takes_over = jnp.logical_and(y == 1, z > 0)
    send_if(hands_on, tail_src, tail_mid, n_s, n_r, column((z + 1) % nz))
    unsent.append((hands_on, tail_src, n_s))
    for j in range(nh):
        pay_src[j, 0:T, :] = states[:, j * hb : (j + 1) * hb].astype(BF16)
        pay_src[j, T:, :] = jnp.broadcast_to(ids[...].astype(F32), (16, hb)).astype(BF16)
    for j in range(nh):
        send_or_local(pay_src.at[j], pay.at[q], p_s, p_r, at(z, j), k == j)
    unsent.append((True, pay.at[0 : nh - 1], p_s))

    def origin(step):
        plane = (z + (1 - 2 * high) * step + nz) % nz
        g = (per * plane - k + nh - 1) // nh
        return plane, g % GATES, jnp.logical_and(g < GATES, nh * g + k < per * (plane + 1))

    order = []
    for n in range(nr):
        chip = (x + n // 2) % nx
        order.append(2 * chip + (c + n) % 2)

    def spread(step, numbers):
        plane, g, found = origin(step)
        outer = jnp.logical_and(found, jnp.logical_not(inner))
        within = jnp.logical_and(found, inner)
        far, near = column(half - high), column(z + 1 - 2 * (z % half))
        for n in numbers:
            block = piece(g, pl.ds(pl.multiple_of(order[n] * cw, cw), cw))
            sem = w_r.at[g * nr + order[n]]
            if step == 0:
                pl.when(found)(functools.partial(landed, block, sem))
                send_if(found, block, block, w_f.at[0], sem, far)
                send_if(within, block, block, w_f.at[0], sem, near)
            else:
                pl.when(within)(functools.partial(landed, block, sem))
                send_if(within, block, block, w_f.at[step], sem, column(end))
        if step == 0:
            for n in numbers:
                block = piece(g, pl.ds(pl.multiple_of(order[n] * cw, cw), cw))
                send_if(outer, block, block, w_f.at[0], w_r.at[g * nr + order[n]], near)
            unsent.append((found, w_all.at[0 : 2 * hb, :], w_f.at[0]))
        elif numbers[-1] == nr - 1:
            unsent.append((within, w_all.at[0:hb, :], w_f.at[step]))

    def relay(dx, dy, targets):
        slot = features(dx, dy, 0)
        landed(rows(x_all, slot, T), x_r.at[slot])
        share(dx, dy, targets)

    spread(0, range(nr))
    pl.when(takes_over)(functools.partial(landed, tail_mid, n_r))
    for j in range(nh):
        part = tail_mid.at[:, j * hb : (j + 1) * hb]
        here = j == k
        send_if(jnp.logical_and(takes_over, j != k), part, tail_in.at[r], e_s, e_r, at(z, j))
        pl.when(jnp.logical_and(takes_over, here))(functools.partial(local, part, tail_in.at[r], e_r))
    unsent.append((takes_over, st_all.at[0 : nh - 1], e_s))
    spread(1, range(nr // 2))
    relay(c, 1 - c, (nearest, partner))
    spread(1, range(nr // 2, nr))
    relay(1 - c, c, (partner,))
    loaded(4)

    def send_upstream(early):
        for j in range(nh):
            part = upstream.at[:, j * hb : (j + 1) * hb]
            over_x, over_y = j // 2 % nx != x, j % 2 != y
            other_link = jnp.where(c == 0, jnp.logical_and(over_y, jnp.logical_not(over_x)), over_x)
            now = jnp.logical_not(other_link) if early else other_link
            send_if(jnp.logical_and(now, j != k), part, up_in.at[q], v_s, v_r, at(z, j))
            if early:
                pl.when(j == k)(functools.partial(local, part, up_in.at[q], v_r))

    unsent.append((True, up_in.at[0 : nh - 1], v_s))
    send_upstream(True)
    spread(2, range(nr))

    stride = T + 8
    landed(pay, p_r)
    pl.when(z > 0)(functools.partial(landed, tail_in, e_r))
    for m in range(nh):
        base = m * stride + 8
        span = slice(m * T, (m + 1) * T)
        prev[base : base + T, :] = pay[m, 0:T, :].astype(F32)
        ids_row = pay[m, T:, :].astype(F32)[0:1, :]
        ids_col[base : base + T, :] = jnp.broadcast_to(ids_row, (hb, T)).T
        if m % 2:
            before = base - stride + T - 1
            prev[base - 1 : base, :] = prev[before : before + 1, :]
            ids_col[base - 1 : base, :] = ids_col[before : before + 1, :]
        else:

            @pl.when(z > 0)
            def _():
                prev[base - 1 : base, :] = tail_in[m // 2, 0:1, :]
                ids_col[base - 1 : base, :] = tail_in[m // 2, 4:5, :]

            @pl.when(z == 0)
            def _():
                prev[base - 1 : base, :] = jnp.zeros((1, hb), F32)
                ids_col[base - 1 : base, :] = jnp.full((1, hb), -1.0, F32)

        same = jnp.where(
            ids_col[base : base + T, :] == ids_col[base - 1 : base - 1 + T, :], 1.0, 0.0
        )
        same_all[span, :] = same
        prior_all[span, :] = prev[base - 1 : base - 1 + T, :] * same

    loaded(5)
    loaded(6)
    (_, g0, found0), (_, g1, _), (_, g2, _), (_, g3, found3) = (origin(step) for step in range(nz))
    own, wide = found0.astype(jnp.int32), found3.astype(jnp.int32)
    early = own * g0 + (1 - own) * g1
    late = wide * g3 + (1 - wide) * g2
    middle = (GATES - early - late) % GATES
    outer = jnp.logical_not(inner)

    def arrived(g, unseen):
        for col in range(nr):
            block = piece(g, slice(col * cw, (col + 1) * cw))
            pl.when(unseen)(functools.partial(landed, block, w_r.at[g * nr + col]))

    def project(span, g):
        return lax.dot_general(
            x_all[span, :], piece(g, slice(None))[...], (((1,), (1,)), ((), ())),
            preferred_element_type=F32,
        )

    def ahead(blocks):
        for m in blocks:
            span = pl.ds(pl.multiple_of(m * T, T), T)
            for g in (early, middle):
                pre[g, span, :] = project(span, g)

    hops = [(0, 0), (0, 1), (1, 0), (1, 1)]
    for dx, dy in hops[:3]:
        m = features(dx, dy, 1)
        landed(rows(x_all, m, T), x_r.at[m])
    arrived(early, jnp.logical_and(jnp.logical_not(found0), outer))
    arrived(middle, outer)
    ahead([features(dx, dy, core) for dx, dy in hops[:3] for core in range(2)])
    send_upstream(False)
    relay(1, 1, (partner,))
    group = pl.ds(pl.multiple_of(k * hb, hb), hb)
    rz, rr, rc = (recur[i : i + 1, group] for i in range(GATES))
    bz, br, bc = (bias[i : i + 1, group] for i in range(GATES))

    def gates(blocks):
        for m in blocks:
            whole = isinstance(m, int)
            span = slice(m * T, (m + 1) * T) if whole else pl.ds(pl.multiple_of(m * T, T), T)
            wide = slice(m * stride, m * stride + T) if whole else pl.ds(pl.multiple_of(m * stride, 8), T)
            last = project(span, late)
            pz, pr, pc = (jnp.where(late == i, last, pre[i, span, :]) for i in range(GATES))
            prior = prior_all[span, :]
            gz = jax.nn.sigmoid(pz + rz * prior + bz)
            gr = jax.nn.sigmoid(pr + rr * prior + br)
            rp = gr * prior
            gc = jnp.tanh(pc + rc * rp + bc)
            az = (gc - prior) * gz * (1.0 - gz)
            ac = gz * (1.0 - gc * gc)
            slope = rp * (1.0 - gr)
            acr = ac * rc
            co_z[span, :] = az
            co_c[span, :] = ac
            co_r[span, :] = acr * slope
            rprior[span, :] = rp
            jac[wide, :] = same_all[span, :] * (1.0 - gz + az * rz + acr * (gr + slope * rr))

    def rest():
        m = features(1, 1, 1)
        landed(rows(x_all, m, T), x_r.at[m])
        ahead([m])

    ahead([features(1, 1, 0)])
    missing = jnp.logical_or(found3, outer)

    @pl.when(c == 1)
    def _():
        arrived(late, missing)
        gates([features(dx, dy, core) for dx, dy in hops[:3] for core in range(2)])
        rest()
        gates([features(1, 1, core) for core in range(2)])

    @pl.when(c == 0)
    def _():
        rest()
        arrived(late, missing)
        gates(range(nh))

    landed(up_in, v_r)
    for m in range(nh):
        up[m * stride : m * stride + T, :] = up_in[m].astype(F32)

    def back(i, state):
        a, b = state
        t = T - 1 - i
        f = jac[pl.ds(t, nh, stride=stride), :]
        b = b + up[pl.ds(t, nh, stride=stride), :]
        scan_a[pl.ds(t, nh, stride=stride), :] = a
        scan_b[pl.ds(t, nh, stride=stride), :] = b
        return f * a, f * b

    a, b = lax.fori_loop(0, T, back, (jnp.ones((nh, hb), F32), jnp.zeros((nh, hb), F32)), unroll=8)
    seg_out[...] = jnp.zeros(seg_out.shape, F32)
    for o in range(nr):
        first, second = slice(2 * o, 2 * o + 1), slice(2 * o + 1, 2 * o + 2)
        seg_out[0, o : o + 1, :] = a[first, :] * a[second, :]
        seg_out[1, o : o + 1, :] = b[first, :] + a[first, :] * b[second, :]
    for plane in range(nz - 1):
        send_if(plane < z, seg_out, seg_in.at[z], c_s, c_r.at[(z + nz - 1) % nz], at(plane, k))
        unsent.append((z == plane + 1, seg_in.at[0 : plane + 1], c_s))
    carry[...] = jnp.zeros(carry.shape, F32)
    for plane in reversed(range(1, nz)):

        @pl.when(plane > z)
        def _():
            landed(seg_in.at[plane], c_r.at[plane - 1])
            carry[0:nr, :] = seg_in[plane, 1, 0:nr, :] + seg_in[plane, 0, 0:nr, :] * carry[0:nr, :]

    into = carry[0:nr, :]
    carry_rows = []
    for o in range(nr):
        later = into[o : o + 1, :]
        second = slice(2 * o + 1, 2 * o + 2)
        carry_rows += [b[second, :] + a[second, :] * later, later]
    carried = jnp.concatenate(carry_rows, 0)

    for m in range(nh):
        span = slice(m * T, (m + 1) * T)
        padded = slice(m * stride, m * stride + T)
        adj = scan_b[padded, :] + scan_a[padded, :] * carried[m : m + 1, :]
        lam[span, :] = adj
        for g, slope in enumerate((co_z, co_r, co_c)):
            grads[span, g * hb : (g + 1) * hb] = (adj * slope[span, :]).astype(BF16)

    def quarter(col):
        return pl.ds(pl.multiple_of(col * cw, cw), cw)

    away = [2 * ((x + 1 + n // 2) % nx) + n % 2 for n in range(nr)]

    def side(n):
        return pl.ds(pl.multiple_of(2 * ((x + n) % nx) * cw, 2 * cw), 2 * cw)

    def gate_of(step):
        g = high * step + (1 - high) * (GATES - 1 - step)
        return g, (nh * g + k) // per

    def short(hidden):
        g = (per * z - hidden + nh - 1) // nh
        have = jnp.logical_and(g < GATES, nh * g + hidden < per * (z + 1))
        return jnp.logical_and(outer, jnp.logical_not(have))

    other = 2 * nx * c + 2 * ((x + 1) % nx) + y
    lacks, helps = short(k), short(other)
    beside = place(s, 2 * ((x + 1) % nx) + c)
    hub = high + half - 1

    near = inner.astype(jnp.int32)
    turns = (
        (GATES - 1) * (high * near + (1 - high) * (1 - near)),
        (GATES - 1) * (1 - high) * near + 1 - near,
        near + (GATES - 1) * high * (1 - near),
    )

    def statistics():
        sums = [jnp.zeros((1, hb), F32) for _ in range(6)]
        for m in range(nh):
            span = slice(m * T, (m + 1) * T)
            prior = prior_all[span, :]
            adj = lam[span, :]
            grad_z = adj * co_z[span, :]
            grad_r = adj * co_r[span, :]
            grad_c = adj * co_c[span, :]
            terms = (grad_z, grad_r, grad_c, grad_z * prior, grad_r * prior, grad_c * rprior[span, :])
            sums = [total + jnp.sum(term, 0, keepdims=True) for total, term in zip(sums, terms)]
        for i in range(6):
            st_out[i : i + 1, :] = sums[i]
        st_out[6:8, :] = jnp.zeros((2, hb), F32)
        st_z[z] = st_out[...]
        for plane in range(nz):
            send_if(plane != z, st_out, st_z.at[z], t_s, t_r, column(plane))
        unsent.append((True, st_z.at[0 : nz - 1], t_s))

    def weigh(step):
        g = turns[step]
        plane = (nh * g + k) // per
        spans = (side(1), side(0)) if step == 0 else (slice(0, DI),)

        def product(span):
            block = lax.dot_general(
                grads[:, pl.ds(pl.multiple_of(g * hb, hb), hb)], x_all[:, span], (((0,), (0,)), ((), ())),
                preferred_element_type=F32,
            )
            wg_own[g, :, span] = block
            wg_out[g, :, span] = block.astype(BF16)

        product(spans[0])
        outward = jnp.logical_and(inner, plane == end)
        inward = jnp.logical_and(outer, plane != z)
        for n, col in enumerate(away):
            if step == 0 and n == 1:
                give(0)
                statistics()
                product(spans[1])
            part = wg_out.at[g, :, quarter(col)]
            send_if(
                jnp.logical_and(inward, plane != hub), part, wg_end.at[g, :, quarter(col)], g_s,
                g_e.at[g * nr + col], column(hub),
            )
            send_if(
                outward, part, wg_mid.at[0, :, quarter(col)], g_s, g_m.at[col], column(end),
            )
        if step == GATES - 1:
            send_if(lacks, wg_out.at[g, :, side(0)], wg_via, g_s, h_r, beside)

    def nearby(step):
        g, plane = gate_of(step)
        for n, col in enumerate(away):
            go = jnp.logical_and(outer, plane == hub)
            if step == GATES - 1 and n >= nr // 2:
                go = jnp.logical_and(go, jnp.logical_not(lacks))
            send_if(
                go, wg_out.at[g, :, quarter(col)], wg_end.at[g, :, quarter(col)], g_s,
                g_e.at[g * nr + col], column(hub),
            )

    def assist():
        g, _ = gate_of(GATES - 1)
        pl.when(helps)(functools.partial(landed, wg_via, h_r))
        for n in range(nr // 2):
            col = 2 * ((x + 1) % nx) + n
            part = wg_via.at[:, n * cw : (n + 1) * cw]
            where = place(2 * hub + y, 2 * ((x + 1) % nx) + c)
            send_if(helps, part, wg_end.at[g, :, quarter(col)], h_s, g_e.at[g * nr + col], where)
        unsent.append((helps, wg_via, h_s))

    chips = [(x + 1, y + 1), (x + 1, y), (x, y + 1), (x, y)]
    lot = (0, 1, 1, 2)

    def tokens(n, core):
        return rows(grads, 2 * (2 * (chips[n][0] % nx) + core) + chips[n][1] % 2, T)[...]

    def give(n):
        part_out[n] = jnp.dot(tokens(n, 1 - c), w_all[...], preferred_element_type=F32).astype(BF16)
        send(part_out.at[n], part_in.at[n], d_s, d_r.at[lot[n]], partner)

    def keep(n):
        part_keep[n] = jnp.dot(tokens(n, c), w_all[...], preferred_element_type=F32)

    def both(n):
        return part_keep[n] + part_in[n].astype(F32)

    parts = [slice(n * T // 2, (n + 1) * T // 2) for n in range(2)]
    scale = 1.0 / math.sqrt(ns * nr * T)

    def gather_stats():
        landed(st_z.at[0 : nz - 1], t_r)
        total = st_z[0]
        for plane in range(1, nz):
            total = total + st_z[plane]
        st_sum[...] = total * scale
        st_all[k] = st_sum[...]
        for j in range(nh):
            send_if(j != k, st_sum, st_all.at[k], u_s, u_r, at(z, j))
        unsent.append((True, st_all.at[0 : nh - 1], u_s))

    def turn(n):
        part = parts[n]
        landed(fin_in.at[0, part], f_r.at[n])
        total = part_keep[2 - c, part] + part_in[2 - c, part].astype(F32) + fin_in[0, part].astype(F32)
        fin_out[2, part] = total.astype(BF16)
        send(fin_out.at[2, part], fin_in.at[2, part], f_s, f_r.at[3 + n], across)

    def hand_on(step, numbers):
        g, plane = gate_of(step)
        passed = jnp.logical_and(inner, jnp.logical_and(plane != z, plane != end))
        far = (plane // half != high) & ((plane == 0) | (plane == nz - 1))
        for col in (away[n] for n in numbers):
            cols = quarter(col)

            @pl.when(passed)
            def _():
                landed(wg_end.at[g, :, cols], g_e.at[g * nr + col])
                wg_out[g, :, cols] = (wg_own[g, :, cols] + wg_end[g, :, cols].astype(F32)).astype(BF16)

            for slot, there in enumerate((jnp.logical_not(far), far)):
                send_if(
                    jnp.logical_and(passed, there), wg_out.at[g, :, cols], wg_mid.at[slot, :, cols],
                    g_s, g_m.at[slot * nr + col], column(plane),
                )

    weigh(0)
    keep(0)
    weigh(1)
    landed(part_in.at[0], d_r.at[0])
    fin_out[0] = both(0).astype(BF16)
    for n, part in enumerate(parts):
        send(fin_out.at[0, part], fin_in.at[0, part], f_s, f_r.at[n], nearest)
    give(1)
    give(2)
    weigh(2)
    hand_on(0, (0,))
    keep(1)
    keep(2)
    landed(part_in.at[1:3], d_r.at[1])
    fin_out[1] = both(1 + c).astype(BF16)
    send(fin_out.at[1], fin_in.at[1], f_s, f_r.at[2], nearest)
    hand_on(0, (1,))
    give(3)
    keep(3)
    hand_on(0, (2,))
    turn(0)
    hand_on(0, (3,))
    gather_stats()
    turn(1)
    for n in range(GATES):
        nearby(n)
    assist()
    for step in range(1, GATES):
        hand_on(step, range(nr))
    unsent.append((True, part_out, d_s))
    unsent.append((True, fin_out, f_s))

    unsent.append((found0, wg_out.at[0 : GATES - 1], g_s))
    unsent.append((jnp.logical_not(found0), wg_out, g_s))
    _, g, found = origin(0)
    b = nh * g + k
    owner, i = b // GATES, b % GATES
    for col in away:
        cols = quarter(col)

        @pl.when(found)
        def _():
            landed(wg_mid.at[0, :, cols], g_m.at[col])
            wg_own[g, :, cols] = wg_own[g, :, cols] + wg_mid[0, :, cols].astype(F32)

        @pl.when(jnp.logical_and(found, inner))
        def _():
            landed(wg_end.at[g, :, cols], g_e.at[g * nr + col])
            wg_own[g, :, cols] = wg_own[g, :, cols] + wg_end[g, :, cols].astype(F32)

        @pl.when(jnp.logical_and(found, outer))
        def _():
            landed(wg_mid.at[1, :, cols], g_m.at[nr + col])
            wg_own[g, :, cols] = wg_own[g, :, cols] + wg_mid[1, :, cols].astype(F32)

        @pl.when(found)
        def _():
            wg_out[g, :, cols] = wg_own[g, :, cols].astype(BF16)

        here = jnp.logical_and(owner == s, r == col)

        @pl.when(jnp.logical_and(found, here))
        def _():
            local(wg_out.at[g, :, cols], wg_in.at[i], g_r)

        send_if(
            jnp.logical_and(found, jnp.logical_not(here)), wg_out.at[g, :, cols], wg_in.at[i],
            g_f, g_r, place(owner, col),
        )
    unsent.append((jnp.logical_and(found, owner != s), wg_out.at[0], g_f))
    unsent.append((jnp.logical_and(found, owner == s), wg_out.at[0, :, 0 : (nr - 1) * cw], g_f))

    landed(st_all.at[0 : nh - 1], u_r)
    for j in range(nh):
        out_p[:, j * hb : (j + 1) * hb] = st_all[j, :6, :]

    landed(part_in.at[3], d_r.at[2])
    total = both(3)
    landed(fin_in.at[1], f_r.at[2])
    for n, part in enumerate(parts):
        landed(fin_in.at[2, part], f_r.at[3 + n])
    total = total + fin_in[1].astype(F32) + fin_in[2].astype(F32)
    out_in[...] = total.astype(BF16)

    landed(wg_in, g_r)
    for i in range(GATES):
        block = slice(i * hb, (i + 1) * hb)
        out_w[block, :] = wg_in[i].astype(F32) * scale

    for sent, src, sem in unsent:
        if sent is True:
            landed(src, sem)
        else:

            @pl.when(sent)
            def _():
                landed(src, sem)


def flush(in_a, in_b, in_c, out_a, out_b, out_c, sems):
    pairs = [(in_a, out_a), (in_b, out_b), (in_c, out_c)]
    copies = [pltpu.make_async_copy(a, b, sems.at[i]) for i, (a, b) in enumerate(pairs)]
    for copy in copies:
        copy.start()
    for copy in copies:
        copy.wait()


def by_hidden(ns, nr, inputs, weight_t, states, doc_ids, recur, bias, out_grad):
    T, DI = inputs.shape[1:]
    H = states.shape[2]
    nh, nz, nx = 2 * nr, ns // 2, nr // 2
    hb, cw = H // nh, DI // nr
    L = nh * T
    vm = pltpu.VMEM
    scratch = [
        vm(weight_t.shape, BF16),
        vm((T, H), F32),
        vm((1, T), jnp.int32),
        vm((GATES, H), F32),
        vm((GATES, H), F32),
        vm((T, H), BF16),
        vm((nh, T + 16, hb), BF16),
        vm((nh, T + 16, hb), BF16),
        vm((nh, T, hb), BF16),
        vm((8, H), F32),
        vm((8, H), F32),
        vm((nr, 8, hb), F32),
        vm((L, DI), BF16),
        vm((GATES * hb, DI), BF16),
        vm((L + 8 * nh, hb), F32),
        vm((L + 8 * nh, hb), F32),
        vm((L, hb), F32),
        vm((L + 8 * nh, hb), F32),
        vm((GATES, L, hb), F32),
        vm((L + 8 * nh, hb), F32),
        vm((L, hb), F32),
        vm((L, hb), F32),
        vm((L, hb), F32),
        vm((L, hb), F32),
        vm((L, hb), F32),
        vm((L + 8 * nh, hb), F32),
        vm((L + 8 * nh, hb), F32),
        vm((nh, hb), F32),
        vm((2, 8, hb), F32),
        vm((nz, 2, 8, hb), F32),
        vm((L, hb), F32),
        vm((L, GATES * hb), BF16),
        vm((hb, DI // 2), BF16),
        vm((nr, T, DI), BF16),
        vm((nr, T, DI), BF16),
        vm((nr, T, DI), F32),
        vm((3, T, DI), BF16),
        vm((3, T, DI), BF16),
        vm((GATES, hb, DI), F32),
        vm((GATES, hb, DI), BF16),
        vm((GATES, hb, DI), BF16),
        vm((2, hb, DI), BF16),
        vm((GATES, hb, cw), BF16),
        vm((8, hb), F32),
        vm((nz, 8, hb), F32),
        vm((8, hb), F32),
        vm((nh, 8, hb), F32),
    ]
    dma = pltpu.SemaphoreType.DMA
    counts = [
        7, None, nh, None, nz - 1, GATES * nr, None, None, None, None, None, None, None, None, None, nz - 1,
        None, 3, None, 5, None, GATES * nr, 2 * nr, None, None, None, None, None, None, None, None,
    ]
    sems = [dma if n is None else dma((n,)) for n in counts]
    whole = pl.BlockSpec(memory_space=pltpu.VMEM)
    out_in, out_w, out_p = pl.pallas_call(
        functools.partial(kernel, ns, nr),
        out_shape=(
            pltpu.VMEM((T, DI), BF16),
            pltpu.VMEM(weight_t.shape, F32),
            pltpu.VMEM((6, H), F32),
        ),
        in_specs=[pl.BlockSpec(memory_space=pltpu.HBM)] * 7,
        out_specs=(whole,) * 3,
        scratch_shapes=scratch + sems,
        compiler_params=pltpu.CompilerParams(
            collective_id=0, has_side_effects=True, vmem_limit_bytes=56 * 1024 * 1024
        ),
    )(inputs[0], weight_t, states[0], doc_ids, recur, bias, out_grad[0])
    shapes = ((T, DI), BF16), (weight_t.shape, F32), ((6, H), F32)
    out_in, out_w, out_p = pl.pallas_call(
        flush,
        out_shape=tuple(jax.ShapeDtypeStruct(*one) for one in shapes),
        in_specs=[whole] * 3,
        out_specs=(pl.BlockSpec(memory_space=pltpu.HBM),) * 3,
        scratch_shapes=[dma((3,))],
    )(*(pltpu.with_memory_space_constraint(one, pltpu.VMEM) for one in (out_in, out_w, out_p)))
    return out_in[None], out_w, out_p


def fits(ns, nr, inputs, weight_t, states):
    parts, L, DI = inputs.shape
    H = states.shape[2]
    return (
        parts == nr
        and ns == 2 * nr
        and ns % 8 == 0
        and ns == 8
        and L * 2 * nr == H * ns
        and H % (ns * 128) == 0
        and DI % (nr * 128) == 0
        and L % (ns * 128) == 0
        and L * DI <= 1 << 21
    )


def solution(mesh):
    ns, nr = mesh.shape["seq"], mesh.shape["rep"]
    placed = (
        P("rep", "seq", None),
        P("seq", "rep"),
        P("rep", "seq", None),
        P("rep", "seq"),
        P(),
        P(),
        P("rep", "seq", None),
    )

    def run(inputs, weight_t, states, doc_ids, recur, bias, out_grad):
        kernelized = fits(ns, nr, inputs, weight_t, states)
        body = functools.partial(by_hidden, ns, nr) if kernelized else by_tokens
        return jax.shard_map(
            body,
            mesh=mesh,
            in_specs=placed,
            out_specs=(P("rep", "seq", None), P("seq", "rep"), P()),
            check_vma=False,
        )(inputs, weight_t, states, doc_ids, recur, bias, out_grad)

    return run
```
